16 devices in a mesh: tp: 2 (over z), ep: 8 (over y, x, core).
Axes of the slice: x: 2, y: 2, z: 2, core: 2. Of those that a mesh axis runs over, the one named last changes fastest.
Arguments:
- act_in: bfloat16 [16384, 1024], P('ep')
- w_router: float32 [1024, 32], replicated
- choice_one: int32 [16384], P('ep')
- choice_two: int32 [16384], P('ep')
- w_gelu: bfloat16 [32, 1024, 512], P('ep', None, 'tp')
- w_lin: bfloat16 [32, 1024, 512], P('ep', None, 'tp')
- w_out: bfloat16 [32, 512, 1024], P('ep', 'tp')
- grad_out: bfloat16 [16384, 1024], P('ep')
Outputs:
- output 1: bfloat16 [16384, 1024], P('ep')
- output 2: bfloat16 [16384, 1024], P('ep')
- output 3: float32 [32, 1024, 512], P('ep', None, 'tp')
- output 4: float32 [32, 1024, 512], P('ep', None, 'tp')
- output 5: float32 [32, 512, 1024], P('ep', 'tp')
- output 6: float32 [1024, 32], replicated
All inputs are finite; a program needn't handle non-finite values.
Results may differ from the reference program's by a relative error of at most 0.00998415.
Values are sent between devices in bfloat16 or wider.
A program may use at most 1 GiB of HBM per device.

```python
import jax
import jax.numpy as jnp
from jax import lax

D = 1024
FF = 512
EXPERTS = 32
TOKENS = 2048
EP_SIZE = 8
TP_SIZE = 2
ALL_TOKENS = EP_SIZE * TOKENS
SLOT_CAP = 2 * TOKENS // EXPERTS
PIECE_W = FF // TP_SIZE
EXP_ROWS = EP_SIZE * SLOT_CAP
ALL_SLOTS = EXPERTS * SLOT_CAP
GELU_COEF = 0.7978845608028654


def gelu_parts(pre_act):
    inner_arg = GELU_COEF * (pre_act + 0.044715 * pre_act * pre_act * pre_act)
    tanh_val = jnp.tanh(inner_arg)
    gelu_val = 0.5 * pre_act * (1.0 + tanh_val)
    gelu_slope = 0.5 * (1.0 + tanh_val) + 0.5 * pre_act * (1.0 - tanh_val * tanh_val) * GELU_COEF * (1.0 + 0.134145 * pre_act * pre_act)
    return gelu_val, gelu_slope


def draw_choices(base_key):
    key_a, key_b, key_c, key_d = jax.random.split(base_key, 4)
    draws_a = jax.random.randint(key_a, (ALL_TOKENS,), 0, EXPERTS, dtype=jnp.int32)
    draws_b = jax.random.randint(key_b, (ALL_TOKENS,), 0, EXPERTS, dtype=jnp.int32)
    skewed = ((draws_a + 1) * (draws_b + 1) - 1) // EXPERTS
    shifts = jax.random.randint(key_c, (EP_SIZE, 1), 0, EXPERTS, dtype=jnp.int32)
    first_ids = ((skewed.reshape(EP_SIZE, TOKENS) + shifts) % EXPERTS).reshape(ALL_TOKENS)
    first_ids = jnp.concatenate([jnp.arange(EXPERTS, dtype=jnp.int32), first_ids[EXPERTS:]])
    hop_ids = jax.random.randint(key_d, (ALL_TOKENS,), 1, EXPERTS, dtype=jnp.int32)
    second_ids = (first_ids + hop_ids) % EXPERTS
    return first_ids.astype(jnp.int32), second_ids.astype(jnp.int32)


def setup_inputs(seed: int = 0) -> dict:
    key_list = jax.random.split(jax.random.key(seed), 7)
    in_scale = D ** -0.5
    out_scale = FF ** -0.5
    act_in = jax.random.normal(key_list[0], (ALL_TOKENS, D), jnp.float32).astype(jnp.bfloat16)
    w_router = 0.5 * in_scale * jax.random.normal(key_list[1], (D, EXPERTS), jnp.float32)
    choice_one, choice_two = draw_choices(key_list[2])
    w_gelu = (in_scale * jax.random.normal(key_list[3], (EXPERTS, D, FF), jnp.float32)).astype(jnp.bfloat16)
    w_lin = (in_scale * jax.random.normal(key_list[4], (EXPERTS, D, FF), jnp.float32)).astype(jnp.bfloat16)
    w_out = (out_scale * jax.random.normal(key_list[5], (EXPERTS, FF, D), jnp.float32)).astype(jnp.bfloat16)
    grad_out = jax.random.normal(key_list[6], (ALL_TOKENS, D), jnp.float32).astype(jnp.bfloat16)
    return {"act_in": act_in, "w_router": w_router, "choice_one": choice_one, "choice_two": choice_two, "w_gelu": w_gelu, "w_lin": w_lin, "w_out": w_out, "grad_out": grad_out}


def route_shard(x_rows, w_router, first_ids, second_ids):
    logits = jnp.dot(x_rows.astype(jnp.float32), w_router)
    router_prob = jax.nn.softmax(logits, axis=-1)
    expert_ids = jnp.arange(EXPERTS, dtype=jnp.int32)
    hot_one = (first_ids[:, None] == expert_ids[None, :]).astype(jnp.int32)
    hot_two = (second_ids[:, None] == expert_ids[None, :]).astype(jnp.int32)
    prob_one = jnp.sum(router_prob * hot_one, axis=-1)
    prob_two = jnp.sum(router_prob * hot_two, axis=-1)
    fill_one = jnp.sum(hot_one, axis=0)
    pos_one = jnp.sum((jnp.cumsum(hot_one, axis=0) - hot_one) * hot_one, axis=-1)
    pos_two = jnp.sum((jnp.cumsum(hot_two, axis=0) - hot_two + fill_one[None, :]) * hot_two, axis=-1)
    slot_one = jnp.where(pos_one < SLOT_CAP, first_ids * SLOT_CAP + pos_one, ALL_SLOTS)
    slot_two = jnp.where(pos_two < SLOT_CAP, second_ids * SLOT_CAP + pos_two, ALL_SLOTS)
    gate_sum = prob_one + prob_two
    return (router_prob, hot_one, hot_two, prob_one, prob_two, prob_one / gate_sum, prob_two / gate_sum, slot_one, slot_two)


def fill_slots(slot_one, slot_two, gate_one, gate_two):
    token_rows = jnp.arange(TOKENS, dtype=jnp.int32)
    source = jnp.full((ALL_SLOTS,), TOKENS, jnp.int32).at[slot_one].set(token_rows, mode="drop").at[slot_two].set(token_rows, mode="drop")
    weight = jnp.zeros((ALL_SLOTS,), jnp.float32).at[slot_one].set(gate_one, mode="drop").at[slot_two].set(gate_two, mode="drop")
    return source, weight


def dispatch_shard(shard_args, w_router):
    x_rows, first_ids, second_ids, dy_rows = shard_args
    routed = route_shard(x_rows, w_router, first_ids, second_ids)
    source, weight = fill_slots(routed[7], routed[8], routed[5], routed[6])
    disp_rows = jnp.take(x_rows, source, axis=0, mode="fill", fill_value=0)
    dout_rows = (weight[:, None] * jnp.take(dy_rows, source, axis=0, mode="fill", fill_value=0).astype(jnp.float32)).astype(jnp.bfloat16)
    return disp_rows.reshape(EXPERTS, SLOT_CAP, D), dout_rows.reshape(EXPERTS, SLOT_CAP, D)


def expert_pass(expert_args):
    disp_rows, dout_rows, w_a, w_b, w_c = expert_args
    pre_a = jnp.dot(disp_rows, w_a, preferred_element_type=jnp.float32)
    pre_b = jnp.dot(disp_rows, w_b, preferred_element_type=jnp.float32)
    gelu_val, gelu_slope = gelu_parts(pre_a)
    hidden = (gelu_val * pre_b).astype(jnp.bfloat16)
    part_out = jnp.einsum("rkf,kfd->krd", hidden.reshape(EXP_ROWS, TP_SIZE, PIECE_W).astype(jnp.float32), w_c.reshape(TP_SIZE, PIECE_W, D).astype(jnp.float32))
    merged = jnp.sum(part_out.astype(jnp.bfloat16).astype(jnp.float32), axis=0).astype(jnp.bfloat16)
    grad_hidden = jnp.dot(dout_rows, w_c.T, preferred_element_type=jnp.float32)
    grad_a = (grad_hidden * pre_b * gelu_slope).astype(jnp.bfloat16)
    grad_b = (grad_hidden * gelu_val).astype(jnp.bfloat16)
    grad_wc = jnp.dot(hidden.T, dout_rows, preferred_element_type=jnp.float32)
    grad_wa = jnp.dot(disp_rows.T, grad_a, preferred_element_type=jnp.float32)
    grad_wb = jnp.dot(disp_rows.T, grad_b, preferred_element_type=jnp.float32)
    part_in = jnp.einsum("rkf,dkf->krd", grad_a.reshape(EXP_ROWS, TP_SIZE, PIECE_W).astype(jnp.float32), w_a.reshape(D, TP_SIZE, PIECE_W).astype(jnp.float32)) + jnp.einsum("rkf,dkf->krd", grad_b.reshape(EXP_ROWS, TP_SIZE, PIECE_W).astype(jnp.float32), w_b.reshape(D, TP_SIZE, PIECE_W).astype(jnp.float32))
    grad_disp = jnp.sum(part_in.astype(jnp.bfloat16).astype(jnp.float32), axis=0).astype(jnp.bfloat16)
    return merged, grad_disp, grad_wa, grad_wb, grad_wc


def combine_shard(shard_args, w_router):
    x_rows, first_ids, second_ids, dy_rows, merged_rows, grad_rows = shard_args
    (router_prob, hot_one, hot_two, prob_one, prob_two, gate_one, gate_two, slot_one, slot_two) = route_shard(x_rows, w_router, first_ids, second_ids)
    out_one = jnp.take(merged_rows, slot_one, axis=0, mode="fill", fill_value=0).astype(jnp.float32)
    out_two = jnp.take(merged_rows, slot_two, axis=0, mode="fill", fill_value=0).astype(jnp.float32)
    act_out = (gate_one[:, None] * out_one + gate_two[:, None] * out_two).astype(jnp.bfloat16)
    dy_f32 = dy_rows.astype(jnp.float32)
    dgate_one = jnp.sum(dy_f32 * out_one, axis=-1)
    dgate_two = jnp.sum(dy_f32 * out_two, axis=-1)
    shared = dgate_one * gate_one + dgate_two * gate_two
    gate_sum = prob_one + prob_two
    dprob_one = (dgate_one - shared) / gate_sum
    dprob_two = (dgate_two - shared) / gate_sum
    centre = dprob_one * prob_one + dprob_two * prob_two
    grad_logits = router_prob * (dprob_one[:, None] * hot_one + dprob_two[:, None] * hot_two - centre[:, None])
    back_one = jnp.take(grad_rows, slot_one, axis=0, mode="fill", fill_value=0).astype(jnp.float32)
    back_two = jnp.take(grad_rows, slot_two, axis=0, mode="fill", fill_value=0).astype(jnp.float32)
    grad_in = (back_one + back_two + jnp.dot(grad_logits, w_router.T)).astype(jnp.bfloat16)
    return act_out, grad_in, grad_logits


def reference(act_in, w_router, choice_one, choice_two, w_gelu, w_lin, w_out, grad_out):
    x_shards = act_in.reshape(EP_SIZE, TOKENS, D)
    dy_shards = grad_out.reshape(EP_SIZE, TOKENS, D)
    first_sh = choice_one.reshape(EP_SIZE, TOKENS)
    second_sh = choice_two.reshape(EP_SIZE, TOKENS)

    def dispatch_step(shard_args):
        return dispatch_shard(shard_args, w_router)

    def combine_step(shard_args):
        return combine_shard(shard_args, w_router)

    disp_all, dout_all = lax.map(dispatch_step, (x_shards, first_sh, second_sh, dy_shards))
    disp_exp = disp_all.transpose(1, 0, 2, 3).reshape(EXPERTS, EXP_ROWS, D)
    dout_exp = dout_all.transpose(1, 0, 2, 3).reshape(EXPERTS, EXP_ROWS, D)
    merged, grad_disp, grad_gelu, grad_lin, grad_wout = lax.map(expert_pass, (disp_exp, dout_exp, w_gelu, w_lin, w_out))
    merged_tok = merged.reshape(EXPERTS, EP_SIZE, SLOT_CAP, D).transpose(1, 0, 2, 3).reshape(EP_SIZE, ALL_SLOTS, D)
    grad_tok = grad_disp.reshape(EXPERTS, EP_SIZE, SLOT_CAP, D).transpose(1, 0, 2, 3).reshape(EP_SIZE, ALL_SLOTS, D)
    act_out, grad_in, grad_logits = lax.map(combine_step, (x_shards, first_sh, second_sh, dy_shards, merged_tok, grad_tok))
    grad_router = jnp.einsum("td,te->de", act_in.astype(jnp.float32), grad_logits.reshape(ALL_TOKENS, EXPERTS))
    return (act_out.reshape(ALL_TOKENS, D), grad_in.reshape(ALL_TOKENS, D), grad_gelu, grad_lin, grad_wout, grad_router)
```

```python
import functools

import jax
import jax.numpy as jnp
from jax import lax
from jax.experimental import pallas as pl
from jax.experimental.pallas import tpu as pltpu
from jax.sharding import PartitionSpec as P


GELU_COEF = 0.7978845608028654
F32 = jnp.float32
BF16 = jnp.bfloat16
NT = (((1,), (1,)), ((), ()))
TN = (((0,), (0,)), ((), ()))
TILE = 256


def gelu_parts(pre_act):
    inner_arg = GELU_COEF * (pre_act + 0.044715 * pre_act * pre_act * pre_act)
    tanh_val = jnp.tanh(inner_arg)
    gelu_val = 0.5 * pre_act * (1.0 + tanh_val)
    gelu_slope = 0.5 * (1.0 + tanh_val) + 0.5 * pre_act * (1.0 - tanh_val * tanh_val) * GELU_COEF * (1.0 + 0.134145 * pre_act * pre_act)
    return gelu_val, gelu_slope


def split3(val):
    high = val.astype(BF16)
    rest = val - high.astype(F32)
    mid = rest.astype(BF16)
    return high, mid, (rest - mid.astype(F32)).astype(BF16)


def route_kernel(me_ref, x_ref, wt_ref, ids_ref, rows_ref, prob_ref, *, slot_cap, own_experts):
    n_experts, n_tokens = prob_ref.shape
    pieces = jnp.concatenate(split3(wt_ref[...]), axis=0)
    raw = lax.dot_general(pieces, x_ref[...], NT, preferred_element_type=F32)
    logits = raw[:n_experts] + raw[n_experts:2 * n_experts] + raw[2 * n_experts:]
    expo = jnp.exp(logits - jnp.max(logits, axis=0, keepdims=True))
    prob = expo / jnp.sum(expo, axis=0, keepdims=True)
    prob_ref[...] = prob
    expert = lax.broadcasted_iota(jnp.int32, (n_experts, n_tokens), 0)
    id_one, id_two = ids_ref[0:1, :], ids_ref[1:2, :]
    hot_one = jnp.where(id_one == expert, 1.0, 0.0)
    hot_two = jnp.where(id_two == expert, 1.0, 0.0)
    hots = jnp.concatenate([hot_one, hot_two], axis=0)
    before = lax.broadcasted_iota(jnp.int32, (TILE, TILE), 0) < lax.broadcasted_iota(jnp.int32, (TILE, TILE), 1)
    tri = jnp.where(before, 1.0, 0.0).astype(BF16)
    run = jnp.zeros((2 * n_experts, 1), F32)
    counts = []
    for b in range(n_tokens // TILE):
        part = hots[:, b * TILE:(b + 1) * TILE]
        counts.append(jnp.dot(part.astype(BF16), tri, preferred_element_type=F32) + run)
        run = run + jnp.sum(part, axis=1, keepdims=True)
    count = jnp.concatenate(counts, axis=1)
    pos_one = jnp.sum(count[:n_experts] * hot_one, axis=0, keepdims=True)
    pos_two = jnp.sum((count[n_experts:] + run[:n_experts]) * hot_two, axis=0, keepdims=True)
    prob_one = jnp.sum(prob * hot_one, axis=0, keepdims=True)
    prob_two = jnp.sum(prob * hot_two, axis=0, keepdims=True)
    turn = me_ref[0] * (own_experts * slot_cap)

    def slot_of(ids, pos):
        place = pos.astype(jnp.int32)
        slot = jnp.where(place < slot_cap, ids * slot_cap + place, n_experts * slot_cap)
        return jnp.bitwise_xor(slot, turn).astype(F32)

    gate_sum = prob_one + prob_two
    rows_ref[...] = jnp.concatenate(
        [slot_of(id_one, pos_one), slot_of(id_two, pos_two), prob_one / gate_sum, prob_two / gate_sum, prob_one, prob_two, jnp.zeros((10, n_tokens), F32)],
        axis=0)


def gather_kernel(rows_ref, src_ref, *outs, first, per, scaled):
    step = pl.program_id(0)
    n_tokens = src_ref.shape[0]
    slot = (first * per + step) * TILE + lax.broadcasted_iota(jnp.int32, (TILE, n_tokens), 0)
    slot = slot.astype(F32)
    hit_one = rows_ref[0:1, :] == slot
    hit_two = rows_ref[1:2, :] == slot
    pick = jnp.where(jnp.logical_or(hit_one, hit_two), 1.0, 0.0).astype(BF16)
    val = jnp.dot(pick, src_ref[...], preferred_element_type=F32)
    if scaled:
        gate = jnp.where(hit_one, rows_ref[2:3, :], 0.0) + jnp.where(hit_two, rows_ref[3:4, :], 0.0)
        val = jnp.sum(gate, axis=1, keepdims=True) * val
    val = val.astype(BF16)
    for i, out in enumerate(outs):
        @pl.when(step // per == i)
        def _(out=out):
            out[...] = val


def forward_kernel(z_ref, *refs, n_src, cols):
    xs = refs[:n_src]
    wa, wb, wc, wa2, wb2, wc2 = refs[n_src:n_src + 6]
    outs = refs[n_src + 6:2 * n_src + 6]
    gv_ref, sv_ref, h_ref = refs[2 * n_src + 6:2 * n_src + 9]
    cap = xs[0].shape[1]
    width = wa.shape[2]
    col = pl.ds(pl.multiple_of(z_ref[0] * cols, cols), cols)
    for j in range(n_src // 2):
        x = jnp.concatenate([xs[2 * j][0], xs[2 * j + 1][0]], axis=0)
        rows = slice(2 * j * cap, 2 * (j + 1) * cap)
        total = None
        for k, (a_ref, b_ref, c_ref) in enumerate(((wa, wb, wc), (wa2, wb2, wc2))):
            pre_a = jnp.dot(x, a_ref[0], preferred_element_type=F32)
            pre_b = jnp.dot(x, b_ref[0], preferred_element_type=F32)
            gelu_val, gelu_slope = gelu_parts(pre_a)
            hidden = (gelu_val * pre_b).astype(BF16)
            gv_ref[0, rows, k * width:(k + 1) * width] = gelu_val
            sv_ref[0, rows, k * width:(k + 1) * width] = pre_b * gelu_slope
            if k == 0:
                h_ref[0, rows, :] = hidden
            part = jnp.dot(hidden, c_ref[0, :, col], preferred_element_type=F32).astype(BF16).astype(F32)
            total = part if total is None else total + part
        total = total.astype(BF16)
        outs[2 * j][0] = total[:cap]
        outs[2 * j + 1][0] = total[cap:]


def backward_kernel(z_ref, *refs, n_src, cols, n_chunk):
    dos = refs[:n_src]
    gv_ref, sv_ref, wa, wb, wc, wa2, wb2, wc2 = refs[n_src:n_src + 8]
    outs = refs[n_src + 8:n_src + 8 + n_chunk * n_src]
    da_ref, db_ref = refs[n_src + 8 + n_chunk * n_src:]
    cap = dos[0].shape[1]
    width = wa.shape[2]
    row = pl.ds(pl.multiple_of(z_ref[0] * cols, cols), cols)
    for j in range(n_src // 2):
        dout = jnp.concatenate([dos[2 * j][0], dos[2 * j + 1][0]], axis=0)
        rows = slice(2 * j * cap, 2 * (j + 1) * cap)
        total = None
        for k, (a_ref, b_ref, c_ref) in enumerate(((wa, wb, wc), (wa2, wb2, wc2))):
            dhid = lax.dot_general(dout, c_ref[0], NT, preferred_element_type=F32)
            grad_a = (dhid * sv_ref[0, rows, k * width:(k + 1) * width]).astype(BF16)
            grad_b = (dhid * gv_ref[0, rows, k * width:(k + 1) * width]).astype(BF16)
            if k == 0:
                da_ref[0, rows, :] = grad_a
                db_ref[0, rows, :] = grad_b
            part = lax.dot_general(grad_a, a_ref[0, row, :], NT, preferred_element_type=F32)
            part = part + lax.dot_general(grad_b, b_ref[0, row, :], NT, preferred_element_type=F32)
            part = part.astype(BF16).astype(F32)
            total = part if total is None else total + part
        total = total.astype(BF16)
        wide = cols // n_chunk
        for c in range(n_chunk):
            outs[c * n_src + 2 * j][0] = total[:cap, c * wide:(c + 1) * wide]
            outs[c * n_src + 2 * j + 1][0] = total[cap:, c * wide:(c + 1) * wide]


def weight_grad_kernel(*refs, n_src):
    xs, dos = refs[:n_src], refs[n_src:2 * n_src]
    h_ref, da_ref, db_ref, ga_ref, gb_ref, gc_ref = refs[2 * n_src:]
    x = jnp.concatenate([r[0] for r in xs], axis=0)
    dout = jnp.concatenate([r[0] for r in dos], axis=0)
    ga_ref[0] = lax.dot_general(x, da_ref[0], TN, preferred_element_type=F32)
    gb_ref[0] = lax.dot_general(x, db_ref[0], TN, preferred_element_type=F32)
    gc_ref[0] = lax.dot_general(h_ref[0], dout, TN, preferred_element_type=F32)


def combine_out_kernel(z_ref, cols_ref, dy_ref, *refs, n_src):
    srcs = refs[:n_src]
    y_ref, dg_ref, all_ref = refs[n_src:]
    per = srcs[0].shape[0]

    @pl.when(pl.program_id(0) == 0)
    def _():
        for d in range(n_src):
            all_ref[d * per:(d + 1) * per, :] = srcs[d][...]

    slot = lax.broadcasted_iota(jnp.int32, (TILE, n_src * per), 1).astype(F32)
    rows = all_ref[...]
    dy = dy_ref[...].astype(F32)
    acc = None
    dgs = []
    for k in range(2):
        pick = jnp.where(cols_ref[:, k:k + 1] == slot, 1.0, 0.0).astype(BF16)
        out = jnp.dot(pick, rows, preferred_element_type=F32)
        part = cols_ref[:, 2 + k:3 + k] * out
        acc = part if acc is None else acc + part
        dgs.append(jnp.sum(dy * out, axis=1, keepdims=True))
    y_ref[...] = acc.astype(BF16)
    wide = jnp.concatenate([dgs[0], dgs[1], jnp.zeros((TILE, 126), F32)], axis=1)
    dg_ref[...] = wide.T[:8, :]


def logit_grad_kernel(z_ref, rows_ref, prob_ref, ids_ref, dga_ref, dgb_ref, x_ref, dl_ref, dw_ref):
    n_experts, n_tokens = prob_ref.shape
    dgate = dga_ref[0:2, :] + dgb_ref[0:2, :]
    dg_one, dg_two = dgate[0:1], dgate[1:2]
    gate_one, gate_two = rows_ref[2:3, :], rows_ref[3:4, :]
    prob_one, prob_two = rows_ref[4:5, :], rows_ref[5:6, :]
    shared = dg_one * gate_one + dg_two * gate_two
    gate_sum = prob_one + prob_two
    dp_one = (dg_one - shared) / gate_sum
    dp_two = (dg_two - shared) / gate_sum
    centre = dp_one * prob_one + dp_two * prob_two
    expert = lax.broadcasted_iota(jnp.int32, (n_experts, n_tokens), 0)
    inner = jnp.where(ids_ref[0:1, :] == expert, dp_one, 0.0) + jnp.where(ids_ref[1:2, :] == expert, dp_two, 0.0) - centre
    high, mid, low = split3(prob_ref[...] * inner)
    dl_ref[...] = jnp.concatenate([high, high, mid, high, low, mid], axis=0)
    raw = jnp.dot(jnp.concatenate([high, mid, low], axis=0), x_ref[...], preferred_element_type=F32)
    dw_ref[...] = raw[:n_experts] + raw[n_experts:2 * n_experts] + raw[2 * n_experts:]


def combine_in_kernel(z_ref, cols_ref, dl_ref, wt_ref, *refs, n_src):
    srcs = refs[:n_src]
    dx_ref, all_ref = refs[n_src:]
    per = srcs[0].shape[0]

    @pl.when(pl.program_id(0) == 0)
    def _():
        for d in range(n_src):
            all_ref[d * per:(d + 1) * per, :] = srcs[d][...]

    slot = lax.broadcasted_iota(jnp.int32, (TILE, n_src * per), 1).astype(F32)
    hit = jnp.logical_or(cols_ref[:, 0:1] == slot, cols_ref[:, 1:2] == slot)
    acc = jnp.dot(jnp.where(hit, 1.0, 0.0).astype(BF16), all_ref[...], preferred_element_type=F32)
    high, mid, low = split3(wt_ref[...])
    weights = jnp.concatenate([high, mid, high, low, high, mid], axis=0)
    back = lax.dot_general(dl_ref[...], weights, TN, preferred_element_type=F32)
    dx_ref[...] = (acc + back).astype(BF16)


def cost(flops, nbytes, trans=0):
    return pl.CostEstimate(flops=int(flops), bytes_accessed=int(nbytes), transcendentals=int(trans))


def solution(mesh):
    tp_size = mesh.shape["tp"]
    n_src = mesh.shape["ep"]
    n_chunk = 2

    def local_step(x_rows, w_router, first_ids, second_ids, w_gelu, w_lin, w_out, dy_rows):
        n_tokens, model = x_rows.shape
        n_experts = w_router.shape[1]
        own, width = w_gelu.shape[0], w_gelu.shape[2]
        slot_cap = 2 * n_tokens // n_experts
        block = own * slot_cap
        cols = model // tp_size
        rows_all = n_src * slot_cap
        sds = jax.ShapeDtypeStruct
        me = lax.axis_index("ep").astype(jnp.int32).reshape(1)
        z = lax.axis_index("tp").astype(jnp.int32).reshape(1)
        swap = [(i, tp_size - 1 - i) for i in range(tp_size)]

        def across(val):
            return lax.ppermute(val, "tp", swap)

        def to_peer(val, d):
            return val if d == 0 else lax.ppermute(val, "ep", [(i, i ^ d) for i in range(n_src)])

        wa2, wb2, wc2 = across(w_gelu), across(w_lin), across(w_out)
        wt = w_router.T
        ids = jnp.stack([first_ids, second_ids])
        rows, prob = pl.pallas_call(
            functools.partial(route_kernel, slot_cap=slot_cap, own_experts=own),
            in_specs=[pl.BlockSpec(memory_space=pltpu.SMEM)] + [pl.BlockSpec(memory_space=pltpu.VMEM)] * 3,
            out_shape=(sds((16, n_tokens), F32), sds((n_experts, n_tokens), F32)),
            cost_estimate=cost(2 * 96 * n_tokens * model, 2 * n_tokens * model, n_experts * n_tokens),
            name="route",
        )(me, x_rows, wt, ids)
        token_cols = rows.T

        per = block // TILE

        def gather(src, first, count, scaled):
            def out_map(g, i):
                return (jnp.clip(g - i * per, 0, per - 1), 0)

            return pl.pallas_call(
                functools.partial(gather_kernel, first=first, per=per, scaled=scaled),
                grid=(count * per,),
                in_specs=[pl.BlockSpec((16, n_tokens), lambda g: (0, 0)), pl.BlockSpec((n_tokens, model), lambda g: (0, 0))],
                out_specs=[pl.BlockSpec((TILE, model), functools.partial(out_map, i=i)) for i in range(count)],
                out_shape=[sds((block, model), BF16)] * count,
                cost_estimate=cost(2 * count * block * n_tokens * model, 2 * (n_tokens + count * block) * model),
                name="gather",
            )(rows, src)

        half = n_src // 2
        order = list(range(half, n_src, 2)) + list(range(half + 1, n_src, 2)) + list(range(2, half)) + [1, 0]

        def dispatch(src, scaled):
            late = gather(src, half, half, scaled)
            early = gather(src, 0, half, scaled)
            mine = list(early) + list(late)
            got = [None] * n_src
            for d in order:
                got[d] = to_peer(mine[d], d).reshape(own, slot_cap, model)
            return got

        xs = dispatch(x_rows, False)
        dos = dispatch(dy_rows, True)

        def row_spec(wide):
            return pl.BlockSpec((1, slot_cap, wide), lambda e, *_: (e, 0, 0))

        def whole(a, b):
            return pl.BlockSpec((1, a, b), lambda e, *_: (e, 0, 0))

        w_specs = [whole(model, width), whole(model, width), whole(width, model)] * 2
        full = tp_size * width
        fwd = pl.pallas_call(
            functools.partial(forward_kernel, n_src=n_src, cols=cols),
            grid_spec=pltpu.PrefetchScalarGridSpec(
                num_scalar_prefetch=1, grid=(own,),
                in_specs=[row_spec(model)] * n_src + w_specs,
                out_specs=[row_spec(cols)] * n_src + [whole(rows_all, full), whole(rows_all, full), whole(rows_all, width)]),
            out_shape=[sds((own, slot_cap, cols), BF16)] * n_src + [sds((own, rows_all, full), F32)] * 2 + [sds((own, rows_all, width), BF16)],
            cost_estimate=cost(2 * own * rows_all * full * (2 * model + cols), 50e6, own * rows_all * full),
            name="forward",
        )(z, *xs, w_gelu, w_lin, w_out, wa2, wb2, wc2)
        outs, gv, sv, hidden = fwd[:n_src], fwd[n_src], fwd[n_src + 1], fwd[n_src + 2]
        back_out = [None] * n_src
        for d in order:
            back_out[d] = to_peer(outs[d], d).reshape(block, cols)

        wide = cols // n_chunk
        bwd = pl.pallas_call(
            functools.partial(backward_kernel, n_src=n_src, cols=cols, n_chunk=n_chunk),
            grid_spec=pltpu.PrefetchScalarGridSpec(
                num_scalar_prefetch=1, grid=(own,),
                in_specs=[row_spec(model)] * n_src + [whole(rows_all, full)] * 2 + w_specs,
                out_specs=[row_spec(wide)] * (n_src * n_chunk) + [whole(rows_all, width)] * 2),
            out_shape=[sds((own, slot_cap, wide), BF16)] * (n_src * n_chunk) + [sds((own, rows_all, width), BF16)] * 2,
            cost_estimate=cost(2 * own * rows_all * full * (model + 2 * cols), 50e6),
            name="backward",
        )(z, *dos, gv, sv, w_gelu, w_lin, w_out, wa2, wb2, wc2)
        grad_a, grad_b = bwd[n_src * n_chunk:]
        back_in = []
        for c in range(n_chunk):
            got = [None] * n_src
            for d in order:
                got[d] = to_peer(bwd[c * n_src + d], d).reshape(block, wide)
            back_in.append(got)

        grad_wa, grad_wb, grad_wc = pl.pallas_call(
            functools.partial(weight_grad_kernel, n_src=n_src),
            grid=(own,),
            in_specs=[row_spec(model)] * (2 * n_src) + [whole(rows_all, width)] * 3,
            out_specs=[whole(model, width), whole(model, width), whole(width, model)],
            out_shape=[sds((own, model, width), F32)] * 2 + [sds((own, width, model), F32)],
            cost_estimate=cost(6 * own * rows_all * width * model, 40e6),
            name="weight_grad",
        )(*xs, *dos, hidden, grad_a, grad_b)

        def resident(a, b):
            return pl.BlockSpec((a, b), lambda i, *_: (0, 0))

        y_half, dg_mine = pl.pallas_call(
            functools.partial(combine_out_kernel, n_src=n_src),
            grid_spec=pltpu.PrefetchScalarGridSpec(
                num_scalar_prefetch=1, grid=(n_tokens // TILE,),
                in_specs=[pl.BlockSpec((TILE, 16), lambda i, z: (i, 0)), pl.BlockSpec((TILE, cols), lambda i, z: (i, z[0]))] + [resident(block, cols)] * n_src,
                out_specs=[pl.BlockSpec((TILE, cols), lambda i, z: (i, 0)), pl.BlockSpec((8, TILE), lambda i, z: (0, i))],
                scratch_shapes=[pltpu.VMEM((n_src * block, cols), BF16)]),
            out_shape=[sds((n_tokens, cols), BF16), sds((8, n_tokens), F32)],
            cost_estimate=cost(4 * n_tokens * n_src * block * cols, 12e6),
            name="combine_out",
        )(z, token_cols, dy_rows, *back_out)
        y_other = across(y_half)
        dg_other = across(dg_mine)

        dl, dw = pl.pallas_call(
            logit_grad_kernel,
            grid_spec=pltpu.PrefetchScalarGridSpec(
                num_scalar_prefetch=1, grid=(1,),
                in_specs=[resident(16, n_tokens), resident(n_experts, n_tokens), resident(2, n_tokens), resident(8, n_tokens), resident(8, n_tokens), pl.BlockSpec((n_tokens, cols), lambda i, z: (0, z[0]))],
                out_specs=[resident(6 * n_experts, n_tokens), resident(n_experts, cols)]),
            out_shape=[sds((6 * n_experts, n_tokens), BF16), sds((n_experts, cols), F32)],
            cost_estimate=cost(2 * 96 * n_tokens * cols, 4e6),
            name="logit_grad",
        )(z, rows, prob, ids, dg_mine, dg_other, x_rows)

        def combine_in(c):
            return pl.pallas_call(
                functools.partial(combine_in_kernel, n_src=n_src),
                grid_spec=pltpu.PrefetchScalarGridSpec(
                    num_scalar_prefetch=1, grid=(n_tokens // TILE,),
                    in_specs=[pl.BlockSpec((TILE, 16), lambda i, z: (i, 0)), pl.BlockSpec((6 * n_experts, TILE), lambda i, z: (0, i)), pl.BlockSpec((n_experts, wide), lambda i, z: (0, z[0] * n_chunk + c))] + [resident(block, wide)] * n_src,
                    out_specs=pl.BlockSpec((TILE, wide), lambda i, z: (i, 0)),
                    scratch_shapes=[pltpu.VMEM((n_src * block, wide), BF16)]),
                out_shape=sds((n_tokens, wide), BF16),
                cost_estimate=cost(2 * n_tokens * n_src * block * wide, 6e6),
                name="combine_in",
            )(z, token_cols, dl, wt, *back_in[c])

        dx_mine = [combine_in(c) for c in range(n_chunk)]
        dx_other = [across(v) for v in dx_mine]
        bit = 1
        while bit < n_src:
            dw = dw + to_peer(dw, bit)
            bit *= 2
        dw_other = across(dw)
        low = z[0] == 0

        def join(mine, other, axis):
            return jnp.where(low, jnp.concatenate(mine + other, axis=axis), jnp.concatenate(other + mine, axis=axis))

        act_out = join([y_half], [y_other], 1)
        grad_in = join(dx_mine, dx_other, 1)
        grad_router = join([dw], [dw_other], 1).T
        return act_out, grad_in, grad_wa, grad_wb, grad_wc, grad_router

    return jax.shard_map(local_step, mesh=mesh, in_specs=(P("ep", None), P(), P("ep"), P("ep"), P("ep", None, "tp"), P("ep", None, "tp"), P("ep", "tp", None), P("ep", None)), out_specs=(P("ep", None), P("ep", None), P("ep", None, "tp"), P("ep", None, "tp"), P("ep", "tp", None), P()), check_vma=False)
```

```python
import functools

import jax
import jax.numpy as jnp
from jax import lax
from jax.experimental import pallas as pl
from jax.experimental.pallas import tpu as pltpu
from jax.sharding import PartitionSpec as P


GELU_COEF = 0.7978845608028654
F32 = jnp.float32
BF16 = jnp.bfloat16
NT = (((1,), (1,)), ((), ()))
TN = (((0,), (0,)), ((), ()))
TILE = 256


def gelu_parts(pre_act):
    inner_arg = GELU_COEF * (pre_act + 0.044715 * pre_act * pre_act * pre_act)
    tanh_val = jnp.tanh(inner_arg)
    gelu_val = 0.5 * pre_act * (1.0 + tanh_val)
    gelu_slope = 0.5 * (1.0 + tanh_val) + 0.5 * pre_act * (1.0 - tanh_val * tanh_val) * GELU_COEF * (1.0 + 0.134145 * pre_act * pre_act)
    return gelu_val, gelu_slope


def split3(val):
    high = val.astype(BF16)
    rest = val - high.astype(F32)
    mid = rest.astype(BF16)
    return high, mid, (rest - mid.astype(F32)).astype(BF16)


def route_kernel(me_ref, x_ref, wt_ref, ids_ref, rows_ref, prob_ref, *, slot_cap, own_experts):
    n_experts, n_tokens = prob_ref.shape
    pieces = jnp.concatenate(split3(wt_ref[...]), axis=0)
    raw = lax.dot_general(pieces, x_ref[...], NT, preferred_element_type=F32)
    logits = raw[:n_experts] + raw[n_experts:2 * n_experts] + raw[2 * n_experts:]
    expo = jnp.exp(logits - jnp.max(logits, axis=0, keepdims=True))
    prob = expo / jnp.sum(expo, axis=0, keepdims=True)
    prob_ref[...] = prob
    expert = lax.broadcasted_iota(jnp.int32, (n_experts, n_tokens), 0)
    id_one, id_two = ids_ref[0:1, :], ids_ref[1:2, :]
    hot_one = jnp.where(id_one == expert, 1.0, 0.0)
    hot_two = jnp.where(id_two == expert, 1.0, 0.0)
    hots = jnp.concatenate([hot_one, hot_two], axis=0)
    before = lax.broadcasted_iota(jnp.int32, (TILE, TILE), 0) < lax.broadcasted_iota(jnp.int32, (TILE, TILE), 1)
    tri = jnp.where(before, 1.0, 0.0).astype(BF16)
    run = jnp.zeros((2 * n_experts, 1), F32)
    counts = []
    for b in range(n_tokens // TILE):
        part = hots[:, b * TILE:(b + 1) * TILE]
        counts.append(jnp.dot(part.astype(BF16), tri, preferred_element_type=F32) + run)
        run = run + jnp.sum(part, axis=1, keepdims=True)
    count = jnp.concatenate(counts, axis=1)
    pos_one = jnp.sum(count[:n_experts] * hot_one, axis=0, keepdims=True)
    pos_two = jnp.sum((count[n_experts:] + run[:n_experts]) * hot_two, axis=0, keepdims=True)
    prob_one = jnp.sum(prob * hot_one, axis=0, keepdims=True)
    prob_two = jnp.sum(prob * hot_two, axis=0, keepdims=True)
    turn = me_ref[0] * (own_experts * slot_cap)

    def slot_of(ids, pos):
        place = pos.astype(jnp.int32)
        slot = jnp.where(place < slot_cap, ids * slot_cap + place, n_experts * slot_cap)
        return jnp.bitwise_xor(slot, turn).astype(F32)

    gate_sum = prob_one + prob_two
    rows_ref[...] = jnp.concatenate(
        [slot_of(id_one, pos_one), slot_of(id_two, pos_two), prob_one / gate_sum, prob_two / gate_sum, prob_one, prob_two, jnp.zeros((10, n_tokens), F32)],
        axis=0)


def gather_kernel(z_ref, rows_ref, src_ref, *outs, peers, per, scaled):
    step = pl.program_id(0)
    n_tokens = src_ref.shape[0]
    peer = sum(jnp.where(step // per == i, d, 0) for i, d in enumerate(peers))
    slot = (peer * per + step % per) * TILE + lax.broadcasted_iota(jnp.int32, (TILE, n_tokens), 0)
    slot = slot.astype(F32)
    hit_one = rows_ref[0:1, :] == slot
    hit_two = rows_ref[1:2, :] == slot
    pick = jnp.where(jnp.logical_or(hit_one, hit_two), 1.0, 0.0).astype(BF16)
    val = jnp.dot(pick, src_ref[...], preferred_element_type=F32)
    if scaled:
        gate = jnp.where(hit_one, rows_ref[2:3, :], 0.0) + jnp.where(hit_two, rows_ref[3:4, :], 0.0)
        val = jnp.sum(gate, axis=1, keepdims=True) * val
    val = val.astype(BF16)
    for i, out in enumerate(outs):
        @pl.when(step // per == i)
        def _(out=out):
            out[...] = val


def forward_own_kernel(z_ref, *refs, n_src, cols):
    xs = refs[:n_src]
    wa, wb, wc, gv_ref, sv_ref, h_ref, part_ref = refs[n_src:]
    cap = xs[0].shape[1]
    col = pl.ds(pl.multiple_of(z_ref[0] * cols, cols), cols)
    for j in range(n_src // 2):
        x = jnp.concatenate([xs[2 * j][0], xs[2 * j + 1][0]], axis=0)
        rows = slice(2 * j * cap, 2 * (j + 1) * cap)
        pre_a = jnp.dot(x, wa[0], preferred_element_type=F32)
        pre_b = jnp.dot(x, wb[0], preferred_element_type=F32)
        gelu_val, gelu_slope = gelu_parts(pre_a)
        hidden = (gelu_val * pre_b).astype(BF16)
        gv_ref[0, rows, :] = gelu_val
        sv_ref[0, rows, :] = pre_b * gelu_slope
        h_ref[0, rows, :] = hidden
        part_ref[0, rows, :] = jnp.dot(hidden, wc[0, :, col], preferred_element_type=F32).astype(BF16)


def forward_other_kernel(*refs, n_src, n_chunk):
    xs = refs[:n_src]
    part_ref, wa, wb, wc = refs[n_src:n_src + 4]
    outs = refs[n_src + 4:n_src + 4 + n_chunk * n_src]
    gv_ref, sv_ref = refs[n_src + 4 + n_chunk * n_src:]
    cap = xs[0].shape[1]
    wide = outs[0].shape[2]
    for j in range(n_src // 2):
        x = jnp.concatenate([xs[2 * j][0], xs[2 * j + 1][0]], axis=0)
        rows = slice(2 * j * cap, 2 * (j + 1) * cap)
        pre_a = jnp.dot(x, wa[0], preferred_element_type=F32)
        pre_b = jnp.dot(x, wb[0], preferred_element_type=F32)
        gelu_val, gelu_slope = gelu_parts(pre_a)
        hidden = (gelu_val * pre_b).astype(BF16)
        gv_ref[0, rows, :] = gelu_val
        sv_ref[0, rows, :] = pre_b * gelu_slope
        part = jnp.dot(hidden, wc[0], preferred_element_type=F32).astype(BF16).astype(F32)
        total = (part_ref[0, rows, :].astype(F32) + part).astype(BF16)
        for c in range(n_chunk):
            outs[c * n_src + 2 * j][0] = total[:cap, c * wide:(c + 1) * wide]
            outs[c * n_src + 2 * j + 1][0] = total[cap:, c * wide:(c + 1) * wide]


def put_rows(z, rows, ref, dest):
    if len(ref) == 1:
        dest[rows, :] = ref[0][0]
        return
    cols = ref[0].shape[2]
    dest[rows, pl.ds(pl.multiple_of(z * cols, cols), cols)] = ref[0][0]
    dest[rows, pl.ds(pl.multiple_of((1 - z) * cols, cols), cols)] = ref[1][0]


def group_refs(refs, widths):
    groups, at = [], 0
    for w in widths:
        groups.append(refs[at:at + w])
        at += w
    return groups, refs[at:]


def backward_kernel(z_ref, *refs, widths, cols, n_chunk):
    dos, refs = group_refs(refs, widths)
    n_src = len(widths)
    gv_ref, sv_ref, gv2_ref, sv2_ref, wa, wb, wc, wa2, wb2, wcz, wcn = refs[:11]
    outs = refs[11:11 + n_chunk * n_src]
    da_ref, db_ref, do_ref = refs[11 + n_chunk * n_src:]
    cap = dos[0][0].shape[1]
    z = z_ref[0]
    near = pl.ds(pl.multiple_of(z * cols, cols), cols)
    far = pl.ds(pl.multiple_of((1 - z) * cols, cols), cols)
    wide = cols // n_chunk
    for j in range(n_src // 2):
        rows = slice(2 * j * cap, 2 * (j + 1) * cap)
        put_rows(z, slice(2 * j * cap, (2 * j + 1) * cap), dos[2 * j], do_ref)
        put_rows(z, slice((2 * j + 1) * cap, 2 * (j + 1) * cap), dos[2 * j + 1], do_ref)
        total = None
        for k, (a_ref, b_ref, s_ref, g_ref) in enumerate(((wa, wb, sv_ref, gv_ref), (wa2, wb2, sv2_ref, gv2_ref))):
            if k == 0:
                dhid = lax.dot_general(do_ref[rows, :], wc[0], NT, preferred_element_type=F32)
            else:
                dhid = lax.dot_general(do_ref[rows, near], wcz[0], NT, preferred_element_type=F32)
                dhid = dhid + lax.dot_general(do_ref[rows, far], wcn[0], NT, preferred_element_type=F32)
            grad_a = (dhid * s_ref[0, rows, :]).astype(BF16)
            grad_b = (dhid * g_ref[0, rows, :]).astype(BF16)
            if k == 0:
                da_ref[0, rows, :] = grad_a
                db_ref[0, rows, :] = grad_b
            part = lax.dot_general(grad_a, a_ref[0, near, :], NT, preferred_element_type=F32)
            part = part + lax.dot_general(grad_b, b_ref[0, near, :], NT, preferred_element_type=F32)
            part = part.astype(BF16).astype(F32)
            total = part if total is None else total + part
        total = total.astype(BF16)
        for c in range(n_chunk):
            outs[c * n_src + 2 * j][0] = total[:cap, c * wide:(c + 1) * wide]
            outs[c * n_src + 2 * j + 1][0] = total[cap:, c * wide:(c + 1) * wide]


def weight_grad_kernel(z_ref, *refs, n_src, widths):
    xs = refs[:n_src]
    dos, refs = group_refs(refs[n_src:], widths)
    h_ref, da_ref, da2_ref, db_ref, db2_ref, ga_ref, gb_ref, gc_ref, do_ref = refs
    cap = xs[0].shape[1]
    for i, ref in enumerate(dos):
        put_rows(z_ref[0], slice(i * cap, (i + 1) * cap), ref, do_ref)
    x = jnp.concatenate([r[0] for r in xs], axis=0)
    grad_a = jnp.concatenate([da_ref[0], da2_ref[0]], axis=0)
    grad_b = jnp.concatenate([db_ref[0], db2_ref[0]], axis=0)
    ga_ref[0] = lax.dot_general(x, grad_a, TN, preferred_element_type=F32)
    gb_ref[0] = lax.dot_general(x, grad_b, TN, preferred_element_type=F32)
    gc_ref[0] = lax.dot_general(h_ref[0], do_ref[...], TN, preferred_element_type=F32)


def slot_picks(cols_ref):
    lane = lax.broadcasted_iota(jnp.int32, (TILE, 128), 1).astype(F32)
    picks = []
    for k in range(2):
        slot = cols_ref[:, k:k + 1]
        blk = jnp.floor(slot * (1.0 / 128.0))
        hot = jnp.where(slot - 128.0 * blk == lane, 1.0, 0.0).astype(BF16)
        picks.append((jnp.broadcast_to(blk, (TILE, 128)).astype(BF16), hot))
    return picks


def stack_rows(srcs, all_ref):
    per = srcs[0].shape[0]

    @pl.when(pl.program_id(0) == 0)
    def _():
        for d, src in enumerate(srcs):
            all_ref[d * per:(d + 1) * per, :] = src[...]


def combine_out_kernel(z_ref, cols_ref, dy_ref, *refs, n_src):
    srcs = refs[:n_src]
    y_ref, dg_ref, all_ref = refs[n_src:]
    stack_rows(srcs, all_ref)
    n_slots = all_ref.shape[0]
    zero = jnp.zeros((TILE, 128), BF16)
    pick = jnp.concatenate(
        [jnp.concatenate([jnp.where(blk == jnp.asarray(b, BF16), hot, zero) for b in range(n_slots // 128)], axis=1) for blk, hot in slot_picks(cols_ref)],
        axis=0)
    both = jnp.dot(pick, all_ref[...], preferred_element_type=F32)
    dy = dy_ref[...].astype(F32)
    one, two = both[:TILE], both[TILE:]
    y_ref[...] = (cols_ref[:, 2:3] * one + cols_ref[:, 3:4] * two).astype(BF16)
    dg_one = jnp.sum(dy * one, axis=1, keepdims=True)
    dg_two = jnp.sum(dy * two, axis=1, keepdims=True)
    wide = jnp.concatenate([dg_one, dg_two, jnp.zeros((TILE, 126), F32)], axis=1)
    dg_ref[...] = wide.T[:8, :]


def logit_grad_kernel(z_ref, rows_ref, prob_ref, ids_ref, x_ref, *refs, n_chunk):
    dgs, (dl_ref, dw_ref) = refs[:2 * n_chunk], refs[2 * n_chunk:]
    n_experts, n_tokens = prob_ref.shape
    mine = sum(r[0:2, :] for r in dgs[:n_chunk])
    other = sum(r[0:2, :] for r in dgs[n_chunk:])
    dgate = mine + other
    dg_one, dg_two = dgate[0:1], dgate[1:2]
    gate_one, gate_two = rows_ref[2:3, :], rows_ref[3:4, :]
    prob_one, prob_two = rows_ref[4:5, :], rows_ref[5:6, :]
    shared = dg_one * gate_one + dg_two * gate_two
    gate_sum = prob_one + prob_two
    dp_one = (dg_one - shared) / gate_sum
    dp_two = (dg_two - shared) / gate_sum
    centre = dp_one * prob_one + dp_two * prob_two
    expert = lax.broadcasted_iota(jnp.int32, (n_experts, n_tokens), 0)
    inner = jnp.where(ids_ref[0:1, :] == expert, dp_one, 0.0) + jnp.where(ids_ref[1:2, :] == expert, dp_two, 0.0) - centre
    high, mid, low = split3(prob_ref[...] * inner)
    dl_ref[...] = jnp.concatenate([high, high, mid, high, low, mid], axis=0)
    raw = jnp.dot(jnp.concatenate([high, mid, low], axis=0), x_ref[...], preferred_element_type=F32)
    dw_ref[...] = raw[:n_experts] + raw[n_experts:2 * n_experts] + raw[2 * n_experts:]


def combine_in_kernel(z_ref, cols_ref, dl_ref, wt_ref, *refs, n_src):
    srcs = refs[:n_src]
    dx_ref, all_ref = refs[n_src:]
    stack_rows(srcs, all_ref)
    n_slots = all_ref.shape[0]
    (blk_one, hot_one), (blk_two, hot_two) = slot_picks(cols_ref)
    zero = jnp.zeros((TILE, 128), BF16)
    parts = []
    for b in range(n_slots // 128):
        this = jnp.asarray(b, BF16)
        parts.append(jnp.where(blk_one == this, hot_one, jnp.where(blk_two == this, hot_two, zero)))
    acc = jnp.dot(jnp.concatenate(parts, axis=1), all_ref[...], preferred_element_type=F32)
    high, mid, low = split3(wt_ref[...])
    weights = jnp.concatenate([high, mid, high, low, high, mid], axis=0)
    back = lax.dot_general(dl_ref[...], weights, TN, preferred_element_type=F32)
    dx_ref[...] = (acc + back).astype(BF16)


def place_kernel(z_ref, *refs):
    pieces, out = refs[:-1], refs[-1]
    n_chunk = len(pieces) // 2
    wide = pieces[0].shape[1]
    for side in range(2):
        base = jnp.where(side == 0, z_ref[0], 1 - z_ref[0]) * (n_chunk * wide)
        for c in range(n_chunk):
            out[:, pl.ds(pl.multiple_of(base + c * wide, wide), wide)] = pieces[side * n_chunk + c][...]


def cost(flops, nbytes, trans=0):
    return pl.CostEstimate(flops=int(flops), bytes_accessed=int(nbytes), transcendentals=int(trans))


def solution(mesh):
    tp_size = mesh.shape["tp"]
    n_src = mesh.shape["ep"]
    n_chunk = 2
    diag = [n_src - 2, n_src - 1]
    early = diag + [2, 4, 0, 1]
    late = [3, 5]
    src_order = early + late

    def local_step(x_rows, w_router, first_ids, second_ids, w_gelu, w_lin, w_out, dy_rows):
        n_tokens, model = x_rows.shape
        n_experts = w_router.shape[1]
        own, width = w_gelu.shape[0], w_gelu.shape[2]
        slot_cap = 2 * n_tokens // n_experts
        block = own * slot_cap
        cols = model // tp_size
        wide = cols // n_chunk
        rows_all = n_src * slot_cap
        rows_early = len(early) * slot_cap
        rows_late = len(late) * slot_cap
        sds = jax.ShapeDtypeStruct
        me = lax.axis_index("ep").astype(jnp.int32).reshape(1)
        z = lax.axis_index("tp").astype(jnp.int32).reshape(1)
        swap = [(i, tp_size - 1 - i) for i in range(tp_size)]

        def across(val):
            return lax.ppermute(val, "tp", swap)

        def to_peer(val, d):
            if d == 0:
                return val
            return lax.ppermute(val, "ep", [(i, i ^ d) for i in range(n_src)])

        def call(kernel, grid, in_specs, out_specs, out_shape, estimate, args, scratch=()):
            return pl.pallas_call(
                kernel,
                grid_spec=pltpu.PrefetchScalarGridSpec(num_scalar_prefetch=1, grid=grid, in_specs=in_specs, out_specs=out_specs, scratch_shapes=list(scratch)),
                out_shape=out_shape, cost_estimate=estimate)(z, *args)

        wa2, wb2 = across(w_gelu), across(w_lin)
        wt = w_router.T
        ids = jnp.stack([first_ids, second_ids])
        rows, prob = pl.pallas_call(
            functools.partial(route_kernel, slot_cap=slot_cap, own_experts=own),
            in_specs=[pl.BlockSpec(memory_space=pltpu.SMEM)] + [pl.BlockSpec(memory_space=pltpu.VMEM)] * 3,
            out_shape=(sds((16, n_tokens), F32), sds((n_experts, n_tokens), F32)),
            cost_estimate=cost(2 * 96 * n_tokens * model, 2 * n_tokens * model, n_experts * n_tokens),
            name="route",
        )(me, x_rows, wt, ids)
        token_cols = rows.T
        wcz = across(lax.dynamic_slice_in_dim(w_out, (1 - z[0]) * cols, cols, 2))
        wcn = across(lax.dynamic_slice_in_dim(w_out, z[0] * cols, cols, 2))

        per = block // TILE

        def gather(src, peers, scaled, part=False):
            width_out = cols if part else model

            def out_map(g, z, i):
                return (jnp.clip(g - i * per, 0, per - 1), 0)

            def src_map(g, z):
                return (0, z[0] if part else 0)

            return call(
                functools.partial(gather_kernel, peers=peers, per=per, scaled=scaled), (len(peers) * per,),
                [pl.BlockSpec((16, n_tokens), lambda g, z: (0, 0)), pl.BlockSpec((n_tokens, width_out), src_map)],
                [pl.BlockSpec((TILE, width_out), functools.partial(out_map, i=i)) for i in range(len(peers))],
                [sds((block, width_out), BF16)] * len(peers),
                cost(2 * len(peers) * block * n_tokens * width_out, 2 * (n_tokens + len(peers) * block) * width_out),
                (rows, src))

        xs, dos = [None] * n_src, [None] * n_src
        for peers in ([6], [4, 2], [7, 5, 3], [1, 0]):
            for d, val in zip(peers, gather(x_rows, peers, False)):
                xs[d] = to_peer(val, d).reshape(own, slot_cap, model)
        for d, val in zip(diag, gather(dy_rows, diag, True, part=True)):
            mine = to_peer(val, d)
            dos[d] = tuple(v.reshape(own, slot_cap, cols) for v in (mine, across(mine)))
        for peers in ([4, 2], [1, 0], [5, 3]):
            for d, val in zip(peers, gather(dy_rows, peers, True)):
                dos[d] = (to_peer(val, d).reshape(own, slot_cap, model),)
        xs = [xs[d] for d in src_order]

        def whole(a, b, at=0):
            return pl.BlockSpec((1, a, b), lambda e, *_: (e, at, 0))

        act_specs = [whole(rows_all, width)] * 3
        act_shapes = [sds((own, rows_all, width), F32)] * 2 + [sds((own, rows_all, width), BF16)]
        gv, sv, hidden, part = call(
            functools.partial(forward_own_kernel, n_src=n_src, cols=cols), (own,),
            [whole(slot_cap, model)] * n_src + [whole(model, width)] * 2 + [whole(width, model)],
            act_specs + [whole(rows_all, cols)], act_shapes + [sds((own, rows_all, cols), BF16)],
            cost(2 * own * rows_all * width * (2 * model + cols), 32e6, own * rows_all * width),
            (*xs, w_gelu, w_lin, w_out))
        fwd = pl.pallas_call(
            functools.partial(forward_other_kernel, n_src=n_src, n_chunk=n_chunk), grid=(own,),
            in_specs=[whole(slot_cap, model)] * n_src + [whole(rows_all, cols)] + [whole(model, width)] * 2 + [whole(width, cols)],
            out_specs=[whole(slot_cap, wide)] * (n_src * n_chunk) + act_specs[:2],
            out_shape=[sds((own, slot_cap, wide), BF16)] * (n_src * n_chunk) + act_shapes[:2],
            cost_estimate=cost(2 * own * rows_all * width * (2 * model + cols), 32e6, own * rows_all * width),
            name="k_fwd_other")(*xs, part, wa2, wb2, wcz)
        gv2, sv2 = fwd[n_chunk * n_src:]
        back_out = []
        for c in range(n_chunk):
            got = [None] * n_src
            for i, d in enumerate(src_order):
                got[d] = to_peer(fwd[c * n_src + i], d).reshape(block, wide)
            back_out.append(got)

        def backward(peers, at):
            n_rows = len(peers) * slot_cap
            args = [v for d in peers for v in dos[d]]
            saved = [whole(n_rows, width, at)] * 4
            return call(
                functools.partial(backward_kernel, widths=[len(dos[d]) for d in peers], cols=cols, n_chunk=n_chunk), (own,),
                [whole(slot_cap, v.shape[2]) for v in args] + saved + [whole(model, width)] * 2 + [whole(width, model)] + [whole(model, width)] * 2 + [whole(width, cols)] * 2,
                [whole(slot_cap, wide)] * (len(peers) * n_chunk) + [whole(n_rows, width)] * 2,
                [sds((own, slot_cap, wide), BF16)] * (len(peers) * n_chunk) + [sds((own, n_rows, width), BF16)] * 2,
                cost(4 * own * n_rows * width * (model + 2 * cols), 6e3 * own * n_rows),
                (*args, gv, sv, gv2, sv2, w_gelu, w_lin, w_out, wa2, wb2, wcz, wcn),
                [pltpu.VMEM((n_rows, model), BF16)])

        bwd_a = backward(early, 0)
        bwd_b = backward(late, rows_early // rows_late)
        back_in = []
        for c in range(n_chunk):
            got = [None] * n_src
            for peers, vals in ((early, bwd_a), (late, bwd_b)):
                for i, d in enumerate(peers):
                    got[d] = to_peer(vals[c * len(peers) + i], d).reshape(block, wide)
            back_in.append(got)

        all_dos = [v for d in src_order for v in dos[d]]
        grad_wa, grad_wb, grad_wc = call(
            functools.partial(weight_grad_kernel, n_src=n_src, widths=[len(dos[d]) for d in src_order]), (own,),
            [whole(slot_cap, model)] * n_src + [whole(slot_cap, v.shape[2]) for v in all_dos] + [whole(rows_all, width)] + [whole(rows_early, width), whole(rows_late, width)] * 2,
            [whole(model, width), whole(model, width), whole(width, model)],
            [sds((own, model, width), F32)] * 2 + [sds((own, width, model), F32)],
            cost(6 * own * rows_all * width * model, 40e6),
            (*xs, *all_dos, hidden, bwd_a[-2], bwd_b[-2], bwd_a[-1], bwd_b[-1]),
            [pltpu.VMEM((rows_all, model), BF16)])

        def resident(a, b):
            return pl.BlockSpec((a, b), lambda i, *_: (0, 0))

        def tiles(b, col=None):
            return pl.BlockSpec((TILE, b), lambda i, z: (i, 0 if col is None else z[0] * n_chunk + col))

        n_tiles = (n_tokens // TILE,)
        stacked = [pltpu.VMEM((n_src * block, wide), BF16)]
        y_mine, y_other, dg_mine, dg_other = [], [], [], []
        for c in range(n_chunk):
            y, dg = call(
                functools.partial(combine_out_kernel, n_src=n_src), n_tiles,
                [tiles(16), tiles(wide, c)] + [resident(block, wide)] * n_src,
                [tiles(wide), pl.BlockSpec((8, TILE), lambda i, z: (0, i))],
                [sds((n_tokens, wide), BF16), sds((8, n_tokens), F32)],
                cost(4 * n_tokens * n_src * block * wide, 6e6),
                (token_cols, dy_rows, *back_out[c]), stacked)
            y_mine.append(y)
            dg_mine.append(dg)
            dg_other.append(across(dg))
            y_other.append(across(y))

        dl, dw = call(
            functools.partial(logit_grad_kernel, n_chunk=n_chunk), (1,),
            [resident(16, n_tokens), resident(n_experts, n_tokens), resident(2, n_tokens), pl.BlockSpec((n_tokens, cols), lambda i, z: (0, z[0]))] + [resident(8, n_tokens)] * (2 * n_chunk),
            [resident(6 * n_experts, n_tokens), resident(n_experts, cols)],
            [sds((6 * n_experts, n_tokens), BF16), sds((n_experts, cols), F32)],
            cost(2 * 96 * n_tokens * cols, 4e6),
            (rows, prob, ids, x_rows, *dg_mine, *dg_other))

        dx_mine, dx_other = [], []
        for c in range(n_chunk):
            dx = call(
                functools.partial(combine_in_kernel, n_src=n_src), n_tiles,
                [tiles(16), pl.BlockSpec((6 * n_experts, TILE), lambda i, z: (0, i)), pl.BlockSpec((n_experts, wide), lambda i, z: (0, z[0] * n_chunk + c))] + [resident(block, wide)] * n_src,
                tiles(wide), sds((n_tokens, wide), BF16),
                cost(2 * n_tokens * n_src * block * wide, 6e6),
                (token_cols, dl, wt, *back_in[c]), stacked)
            dx_mine.append(dx)
            dx_other.append(across(dx))
        bit = 1
        while bit < n_src:
            dw = dw + to_peer(dw, bit)
            bit *= 2
        dw_other = across(dw)

        def place(pieces):
            return call(place_kernel, n_tiles, [tiles(wide)] * len(pieces), tiles(model), sds((n_tokens, model), BF16), cost(1e6, 8e6), pieces)

        act_out = place(y_mine + y_other)
        grad_in = place(dx_mine + dx_other)
        grad_router = jnp.where(z[0] == 0, jnp.concatenate([dw, dw_other], axis=1), jnp.concatenate([dw_other, dw], axis=1)).T
        return act_out, grad_in, grad_wa, grad_wb, grad_wc, grad_router

    return jax.shard_map(local_step, mesh=mesh, in_specs=(P("ep", None), P(), P("ep"), P("ep"), P("ep", None, "tp"), P("ep", None, "tp"), P("ep", "tp", None), P("ep", None)), out_specs=(P("ep", None), P("ep", None), P("ep", None, "tp"), P("ep", None, "tp"), P("ep", "tp", None), P()), check_vma=False)
```

```python
import functools

import jax
import jax.numpy as jnp
from jax import lax
from jax.experimental import pallas as pl
from jax.experimental.pallas import tpu as pltpu
from jax.sharding import PartitionSpec as P


GELU_COEF = 0.7978845608028654
F32 = jnp.float32
BF16 = jnp.bfloat16
NT = (((1,), (1,)), ((), ()))
TN = (((0,), (0,)), ((), ()))
TILE = 256
GATHER_TILE = 256
GROUP = 2
TOKEN_TILE = 512


def gelu_parts(pre_act):
    inner_arg = GELU_COEF * (pre_act + 0.044715 * pre_act * pre_act * pre_act)
    tanh_val = jnp.tanh(inner_arg)
    gelu_val = 0.5 * pre_act * (1.0 + tanh_val)
    gelu_slope = 0.5 * (1.0 + tanh_val) + 0.5 * pre_act * (1.0 - tanh_val * tanh_val) * GELU_COEF * (1.0 + 0.134145 * pre_act * pre_act)
    return gelu_val, gelu_slope


def split3(val):
    high = val.astype(BF16)
    rest = val - high.astype(F32)
    mid = rest.astype(BF16)
    return high, mid, (rest - mid.astype(F32)).astype(BF16)


def route_kernel(me_ref, x_ref, wt_ref, one_ref, two_ref, rows_ref, prob_ref, first_ref, *, slot_cap, own_experts, peer):
    n_experts, n_tokens = prob_ref.shape
    pieces = jnp.concatenate(split3(wt_ref[...]), axis=0)
    raw = lax.dot_general(pieces, x_ref[...], NT, preferred_element_type=F32)
    logits = raw[:n_experts] + raw[n_experts:2 * n_experts] + raw[2 * n_experts:]
    expo = jnp.exp(logits - jnp.max(logits, axis=0, keepdims=True))
    prob = expo / jnp.sum(expo, axis=0, keepdims=True)
    prob_ref[...] = prob
    expert = lax.broadcasted_iota(jnp.int32, (n_experts, n_tokens), 0)
    id_one, id_two = one_ref[...], two_ref[...]
    hot_one = jnp.where(id_one == expert, 1.0, 0.0)
    hot_two = jnp.where(id_two == expert, 1.0, 0.0)
    hots = jnp.concatenate([hot_one, hot_two], axis=0)
    before = lax.broadcasted_iota(jnp.int32, (TILE, TILE), 0) < lax.broadcasted_iota(jnp.int32, (TILE, TILE), 1)
    tri = jnp.where(before, 1.0, 0.0).astype(BF16)
    run = jnp.zeros((2 * n_experts, 1), F32)
    counts = []
    for b in range(n_tokens // TILE):
        part = hots[:, b * TILE:(b + 1) * TILE]
        counts.append(jnp.dot(part.astype(BF16), tri, preferred_element_type=F32) + run)
        run = run + jnp.sum(part, axis=1, keepdims=True)
    count = jnp.concatenate(counts, axis=1)
    pos_one = jnp.sum(count[:n_experts] * hot_one, axis=0, keepdims=True)
    pos_two = jnp.sum((count[n_experts:] + run[:n_experts]) * hot_two, axis=0, keepdims=True)
    prob_one = jnp.sum(prob * hot_one, axis=0, keepdims=True)
    prob_two = jnp.sum(prob * hot_two, axis=0, keepdims=True)
    turn = me_ref[0] * (own_experts * slot_cap)

    def slot_of(ids, pos):
        place = pos.astype(jnp.int32)
        slot = jnp.where(place < slot_cap, ids * slot_cap + place, n_experts * slot_cap)
        return jnp.bitwise_xor(slot, turn).astype(F32)

    gate_sum = prob_one + prob_two
    slot_one, slot_two = slot_of(id_one, pos_one), slot_of(id_two, pos_two)
    block = first_ref.shape[0]
    slot = (peer * block + lax.broadcasted_iota(jnp.int32, (block, n_tokens), 0)).astype(F32)
    hit = jnp.logical_or(slot_one == slot, slot_two == slot)
    first_ref[...] = jnp.dot(jnp.where(hit, 1.0, 0.0).astype(BF16), x_ref[...], preferred_element_type=F32).astype(BF16)
    rows_ref[...] = jnp.concatenate(
        [slot_one, slot_two, prob_one / gate_sum, prob_two / gate_sum, prob_one, prob_two, jnp.zeros((10, n_tokens), F32)],
        axis=0)


def gather_kernel(z_ref, rows_ref, src_ref, *outs, peers, per, scaled):
    step = pl.program_id(0)
    n_tokens = src_ref.shape[0]
    peer = sum(jnp.where(step // per == i, d, 0) for i, d in enumerate(peers))
    slot = (peer * per + step % per) * GATHER_TILE + lax.broadcasted_iota(jnp.int32, (GATHER_TILE, n_tokens), 0)
    slot = slot.astype(F32)
    hit_one = rows_ref[0:1, :] == slot
    hit_two = rows_ref[1:2, :] == slot
    pick = jnp.where(jnp.logical_or(hit_one, hit_two), 1.0, 0.0).astype(BF16)
    val = jnp.dot(pick, src_ref[...], preferred_element_type=F32)
    if scaled:
        gate = jnp.where(hit_one, rows_ref[2:3, :], 0.0) + jnp.where(hit_two, rows_ref[3:4, :], 0.0)
        val = jnp.sum(gate, axis=1, keepdims=True) * val
    val = val.astype(BF16)
    for i, out in enumerate(outs):
        @pl.when(step // per == i)
        def _(out=out):
            out[...] = val


def forward_own_kernel(z_ref, *refs, n_src, cols):
    xs = refs[:n_src]
    wa, wb, wc, gv_ref, sv_ref, h_ref, part_ref = refs[n_src:]
    cap = xs[0].shape[1]
    col = pl.ds(pl.multiple_of(z_ref[0] * cols, cols), cols)
    group = GROUP
    for first in range(0, n_src, group):
        x = jnp.concatenate([r[0] for r in xs[first:first + group]], axis=0)
        rows = slice(first * cap, (first + group) * cap)
        pre_a = jnp.dot(x, wa[0], preferred_element_type=F32)
        pre_b = jnp.dot(x, wb[0], preferred_element_type=F32)
        gelu_val, gelu_slope = gelu_parts(pre_a)
        hidden = (gelu_val * pre_b).astype(BF16)
        gv_ref[0, rows, :] = gelu_val
        sv_ref[0, rows, :] = pre_b * gelu_slope
        h_ref[0, rows, :] = hidden
        part_ref[0, rows, :] = jnp.dot(hidden, wc[0, :, col], preferred_element_type=F32).astype(BF16)


def forward_other_kernel(*refs, n_src, n_chunk):
    xs = refs[:n_src]
    part_ref, part2_ref, wa, wb, wc = refs[n_src:n_src + 5]
    outs = refs[n_src + 5:n_src + 5 + n_chunk * n_src]
    gv_ref, sv_ref = refs[n_src + 5 + n_chunk * n_src:]
    parts = jnp.concatenate([part_ref[0], part2_ref[0]], axis=0)
    cap = xs[0].shape[1]
    wide = outs[0].shape[2]
    group = GROUP
    for first in range(0, n_src, GROUP):
        x = jnp.concatenate([r[0] for r in xs[first:first + GROUP]], axis=0)
        rows = slice(first * cap, (first + GROUP) * cap)
        pre_a = jnp.dot(x, wa[0], preferred_element_type=F32)
        pre_b = jnp.dot(x, wb[0], preferred_element_type=F32)
        gelu_val, gelu_slope = gelu_parts(pre_a)
        hidden = (gelu_val * pre_b).astype(BF16)
        gv_ref[0, rows, :] = gelu_val
        sv_ref[0, rows, :] = pre_b * gelu_slope
        part = jnp.dot(hidden, wc[0], preferred_element_type=F32).astype(BF16).astype(F32)
        total = (parts[rows].astype(F32) + part).astype(BF16)
        for c in range(n_chunk):
            for i in range(group):
                outs[c * n_src + first + i][0] = total[i * cap:(i + 1) * cap, c * wide:(c + 1) * wide]


def put_rows(z, rows, ref, dest):
    if len(ref) == 1:
        dest[rows, :] = ref[0][0]
        return
    cols = ref[0].shape[2]
    dest[rows, pl.ds(pl.multiple_of(z * cols, cols), cols)] = ref[0][0]
    dest[rows, pl.ds(pl.multiple_of((1 - z) * cols, cols), cols)] = ref[1][0]


def group_refs(refs, widths):
    groups, at = [], 0
    for w in widths:
        groups.append(refs[at:at + w])
        at += w
    return groups, refs[at:]


def backward_kernel(z_ref, *refs, widths, saved_widths, cols, n_chunk):
    dos, refs = group_refs(refs, widths)
    n_src = len(widths)
    saved, refs = group_refs(refs, saved_widths)
    wa, wb, wc, wa2, wb2, wcz, wcn = refs[:7]
    outs = refs[7:7 + n_chunk * n_src]
    da_ref, db_ref, do_ref = refs[7 + n_chunk * n_src:]
    gv, sv, gv2, sv2 = [jnp.concatenate([r[0] for r in group], axis=0) if len(group) > 1 else group[0][0] for group in saved]
    cap = dos[0][0].shape[1]
    z = z_ref[0]
    near = pl.ds(pl.multiple_of(z * cols, cols), cols)
    far = pl.ds(pl.multiple_of((1 - z) * cols, cols), cols)
    wide = cols // n_chunk
    group = GROUP
    for first in range(0, n_src, group):
        rows = slice(first * cap, (first + group) * cap)
        for i in range(first, first + group):
            put_rows(z, slice(i * cap, (i + 1) * cap), dos[i], do_ref)
        total = None
        for k, (a_ref, b_ref, slope, gelu) in enumerate(((wa, wb, sv, gv), (wa2, wb2, sv2, gv2))):
            if k == 0:
                dhid = lax.dot_general(do_ref[rows, :], wc[0], NT, preferred_element_type=F32)
            else:
                dhid = lax.dot_general(do_ref[rows, near], wcz[0], NT, preferred_element_type=F32)
                dhid = dhid + lax.dot_general(do_ref[rows, far], wcn[0], NT, preferred_element_type=F32)
            grad_a = (dhid * slope[rows]).astype(BF16)
            grad_b = (dhid * gelu[rows]).astype(BF16)
            if k == 0:
                da_ref[0, rows, :] = grad_a
                db_ref[0, rows, :] = grad_b
            part = lax.dot_general(grad_a, a_ref[0, near, :], NT, preferred_element_type=F32)
            part = part + lax.dot_general(grad_b, b_ref[0, near, :], NT, preferred_element_type=F32)
            part = part.astype(BF16).astype(F32)
            total = part if total is None else total + part
        total = total.astype(BF16)
        for c in range(n_chunk):
            for i in range(group):
                outs[c * n_src + first + i][0] = total[i * cap:(i + 1) * cap, c * wide:(c + 1) * wide]


def weight_grad_kernel(z_ref, *refs, n_src, widths):
    xs = refs[:n_src]
    dos, refs = group_refs(refs[n_src:], widths)
    h_ref, h2_ref, da_ref, da2_ref, db_ref, db2_ref, ga_ref, gb_ref, gc_ref, do_ref = refs
    cap = xs[0].shape[1]
    for i, ref in enumerate(dos):
        put_rows(z_ref[0], slice(i * cap, (i + 1) * cap), ref, do_ref)
    x = jnp.concatenate([r[0] for r in xs], axis=0)
    grad_a = jnp.concatenate([da_ref[0], da2_ref[0]], axis=0)
    grad_b = jnp.concatenate([db_ref[0], db2_ref[0]], axis=0)
    ga_ref[0] = lax.dot_general(x, grad_a, TN, preferred_element_type=F32)
    gb_ref[0] = lax.dot_general(x, grad_b, TN, preferred_element_type=F32)
    gc_ref[0] = lax.dot_general(jnp.concatenate([h_ref[0], h2_ref[0]], axis=0), do_ref[...], TN, preferred_element_type=F32)


def slot_picks(cols_ref):
    lane = lax.broadcasted_iota(jnp.int32, (TOKEN_TILE, 128), 1).astype(F32)
    picks = []
    for k in range(2):
        slot = cols_ref[:, k:k + 1]
        blk = jnp.floor(slot * (1.0 / 128.0))
        hot = jnp.where(slot - 128.0 * blk == lane, 1.0, 0.0).astype(BF16)
        picks.append((jnp.broadcast_to(blk, (TOKEN_TILE, 128)).astype(BF16), hot))
    return picks


def combine_out_kernel(z_ref, cols_ref, dy_ref, *refs, n_src):
    srcs = refs[:n_src]
    y_ref, dg_ref = refs[n_src:]
    blocks = srcs[0].shape[0] // 128
    picks = slot_picks(cols_ref)
    zero = jnp.zeros((TOKEN_TILE, 128), BF16)
    both = None
    for d in range(n_src):
        pick = jnp.concatenate(
            [jnp.concatenate([jnp.where(blk == jnp.asarray(d * blocks + b, BF16), hot, zero) for b in range(blocks)], axis=1) for blk, hot in picks], axis=0)
        part = jnp.dot(pick, srcs[d][...], preferred_element_type=F32)
        both = part if both is None else both + part
    dy = dy_ref[...].astype(F32)
    one, two = both[:TOKEN_TILE], both[TOKEN_TILE:]
    y_ref[...] = (cols_ref[:, 2:3] * one + cols_ref[:, 3:4] * two).astype(BF16)
    dg_one = jnp.sum(dy * one, axis=1, keepdims=True)
    dg_two = jnp.sum(dy * two, axis=1, keepdims=True)
    wide = jnp.concatenate([dg_one, dg_two, jnp.zeros((TOKEN_TILE, 126), F32)], axis=1)
    dg_ref[...] = wide.T[:8, :]


def logit_grad_kernel(z_ref, rows_ref, prob_ref, one_ref, two_ref, x_ref, *refs, n_chunk):
    dgs, (dl_ref, dw_ref) = refs[:2 * n_chunk], refs[2 * n_chunk:]
    n_experts, n_tokens = prob_ref.shape
    mine = sum(r[0:2, :] for r in dgs[:n_chunk])
    other = sum(r[0:2, :] for r in dgs[n_chunk:])
    dgate = mine + other
    dg_one, dg_two = dgate[0:1], dgate[1:2]
    gate_one, gate_two = rows_ref[2:3, :], rows_ref[3:4, :]
    prob_one, prob_two = rows_ref[4:5, :], rows_ref[5:6, :]
    shared = dg_one * gate_one + dg_two * gate_two
    gate_sum = prob_one + prob_two
    dp_one = (dg_one - shared) / gate_sum
    dp_two = (dg_two - shared) / gate_sum
    centre = dp_one * prob_one + dp_two * prob_two
    expert = lax.broadcasted_iota(jnp.int32, (n_experts, n_tokens), 0)
    inner = jnp.where(one_ref[...] == expert, dp_one, 0.0) + jnp.where(two_ref[...] == expert, dp_two, 0.0) - centre
    high, mid, low = split3(prob_ref[...] * inner)
    dl_ref[...] = jnp.concatenate([high, high, mid, high, low, mid], axis=0)
    raw = jnp.dot(jnp.concatenate([high, mid, low], axis=0), x_ref[...], preferred_element_type=F32)
    dw_ref[...] = raw[:n_experts] + raw[n_experts:2 * n_experts] + raw[2 * n_experts:]


def combine_in_kernel(z_ref, cols_ref, dl_ref, wt_ref, *refs, n_src):
    srcs, dx_ref = refs[:n_src], refs[n_src]
    blocks = srcs[0].shape[0] // 128
    (blk_one, hot_one), (blk_two, hot_two) = slot_picks(cols_ref)
    zero = jnp.zeros((TOKEN_TILE, 128), BF16)
    acc = None
    for d in range(n_src):
        parts = []
        for b in range(blocks):
            this = jnp.asarray(d * blocks + b, BF16)
            parts.append(jnp.where(blk_one == this, hot_one, jnp.where(blk_two == this, hot_two, zero)))
        part = jnp.dot(jnp.concatenate(parts, axis=1), srcs[d][...], preferred_element_type=F32)
        acc = part if acc is None else acc + part
    high, mid, low = split3(wt_ref[...])
    weights = jnp.concatenate([high, mid, high, low, high, mid], axis=0)
    back = lax.dot_general(dl_ref[...], weights, TN, preferred_element_type=F32)
    dx_ref[...] = (acc + back).astype(BF16)


def place_kernel(z_ref, *refs):
    pieces, out = refs[:-1], refs[-1]
    n_chunk = len(pieces) // 2
    wide = pieces[0].shape[1]
    for side in range(2):
        @pl.when(pl.program_id(1) == side)
        def _(side=side):
            for c in range(n_chunk):
                out[:, c * wide:(c + 1) * wide] = pieces[side * n_chunk + c][...]


def place_last_kernel(z_ref, kept_ref, piece_ref, out_ref):
    out_ref[...] = piece_ref[...]


def cost(flops, nbytes, trans=0):
    return pl.CostEstimate(flops=int(flops), bytes_accessed=int(nbytes), transcendentals=int(trans))


def solution(mesh):
    tp_size = mesh.shape["tp"]
    n_src = mesh.shape["ep"]
    n_chunk = 2
    diag = [n_src - 2, n_src - 1]
    early = diag + [0, 1]
    late = [2, 4, 3, 5]
    src_order = early + late
    first_peer = 6

    def local_step(x_rows, w_router, first_ids, second_ids, w_gelu, w_lin, w_out, dy_rows):
        n_tokens, model = x_rows.shape
        n_experts = w_router.shape[1]
        own, width = w_gelu.shape[0], w_gelu.shape[2]
        slot_cap = 2 * n_tokens // n_experts
        block = own * slot_cap
        cols = model // tp_size
        wide = cols // n_chunk
        rows_all = n_src * slot_cap
        rows_early = len(early) * slot_cap
        rows_late = len(late) * slot_cap
        sds = jax.ShapeDtypeStruct
        me = lax.axis_index("ep").astype(jnp.int32).reshape(1)
        z = lax.axis_index("tp").astype(jnp.int32).reshape(1)
        swap = [(i, tp_size - 1 - i) for i in range(tp_size)]

        def across(val):
            return lax.ppermute(val, "tp", swap)

        def to_peer(val, d):
            if d == 0:
                return val
            return lax.ppermute(val, "ep", [(i, i ^ d) for i in range(n_src)])

        def call(kernel, grid, in_specs, out_specs, out_shape, estimate, args, scratch=()):
            return pl.pallas_call(
                kernel,
                grid_spec=pltpu.PrefetchScalarGridSpec(num_scalar_prefetch=1, grid=grid, in_specs=in_specs, out_specs=out_specs, scratch_shapes=list(scratch)),
                out_shape=out_shape, cost_estimate=estimate)(z, *args)

        wa2, wb2 = across(w_gelu), across(w_lin)
        wt = w_router.T
        id_one, id_two = first_ids.reshape(1, n_tokens), second_ids.reshape(1, n_tokens)
        rows, prob, first_x = pl.pallas_call(
            functools.partial(route_kernel, slot_cap=slot_cap, own_experts=own, peer=first_peer),
            in_specs=[pl.BlockSpec(memory_space=pltpu.SMEM)] + [pl.BlockSpec(memory_space=pltpu.VMEM)] * 4,
            out_shape=(sds((16, n_tokens), F32), sds((n_experts, n_tokens), F32), sds((block, model), BF16)),
            cost_estimate=cost(2 * 96 * n_tokens * model, 2 * n_tokens * model, n_experts * n_tokens),
            name="route",
        )(me, x_rows, wt, id_one, id_two)
        token_cols = rows.T
        wcz = across(lax.dynamic_slice_in_dim(w_out, (1 - z[0]) * cols, cols, 2))
        wcn = across(lax.dynamic_slice_in_dim(w_out, z[0] * cols, cols, 2))

        per = block // GATHER_TILE

        def gather(src, peers, scaled, part=False):
            width_out = cols if part else model

            def out_map(g, z, i):
                return (jnp.clip(g - i * per, 0, per - 1), 0)

            def src_map(g, z):
                return (0, z[0] if part else 0)

            return call(
                functools.partial(gather_kernel, peers=peers, per=per, scaled=scaled), (len(peers) * per,),
                [pl.BlockSpec((16, n_tokens), lambda g, z: (0, 0)), pl.BlockSpec((n_tokens, width_out), src_map)],
                [pl.BlockSpec((GATHER_TILE, width_out), functools.partial(out_map, i=i)) for i in range(len(peers))],
                [sds((block, width_out), BF16)] * len(peers),
                cost(2 * len(peers) * block * n_tokens * width_out, 2 * (n_tokens + len(peers) * block) * width_out),
                (rows, src))

        xs, dos = [None] * n_src, [None] * n_src
        xs[first_peer] = to_peer(first_x, first_peer).reshape(own, slot_cap, model)
        for peers in ([4, 2], [7, 1, 0], [5, 3]):
            for d, val in zip(peers, gather(x_rows, peers, False)):
                xs[d] = to_peer(val, d).reshape(own, slot_cap, model)
        for peers in (diag, [4, 2]):
            for d, val in zip(peers, gather(dy_rows, peers, True, part=True)):
                mine = to_peer(val, d)
                dos[d] = tuple(v.reshape(own, slot_cap, cols) for v in (mine, across(mine)))
        for peers in ([1, 0], [5, 3]):
            for d, val in zip(peers, gather(dy_rows, peers, True)):
                dos[d] = (to_peer(val, d).reshape(own, slot_cap, model),)
        xs = [xs[d] for d in src_order]

        def whole(a, b, at=0):
            return pl.BlockSpec((1, a, b), lambda e, *_: (e, at, 0))

        def forward_own(lo, hi):
            n_rows = (hi - lo) * slot_cap
            return call(
                functools.partial(forward_own_kernel, n_src=hi - lo, cols=cols), (own,),
                [whole(slot_cap, model)] * (hi - lo) + [whole(model, width)] * 2 + [whole(width, model)],
                [whole(n_rows, width)] * 3 + [whole(n_rows, cols)],
                [sds((own, n_rows, width), F32)] * 2 + [sds((own, n_rows, width), BF16), sds((own, n_rows, cols), BF16)],
                cost(2 * own * n_rows * width * (2 * model + cols), 8e3 * own * n_rows, own * n_rows * width),
                (*xs[lo:hi], w_gelu, w_lin, w_out))

        cuts = (0, n_src - 2, n_src)
        own_parts = [forward_own(cuts[i], cuts[i + 1]) for i in range(2)]
        part_rows = [(cuts[i + 1] - cuts[i]) * slot_cap for i in range(2)]
        fwd = pl.pallas_call(
            functools.partial(forward_other_kernel, n_src=n_src, n_chunk=n_chunk), grid=(own,),
            in_specs=[whole(slot_cap, model)] * n_src + [whole(r, cols) for r in part_rows] + [whole(model, width)] * 2 + [whole(width, cols)],
            out_specs=[whole(slot_cap, wide)] * (n_src * n_chunk) + [whole(rows_all, width)] * 2,
            out_shape=[sds((own, slot_cap, wide), BF16)] * (n_src * n_chunk) + [sds((own, rows_all, width), F32)] * 2,
            cost_estimate=cost(2 * own * rows_all * width * (2 * model + cols), 32e6, own * rows_all * width),
            name="k_fwd_other")(*xs, own_parts[0][3], own_parts[1][3], wa2, wb2, wcz)
        gv2, sv2 = fwd[n_chunk * n_src:]
        back_out = []
        for c in range(n_chunk):
            got = [None] * n_src
            for i, d in enumerate(src_order):
                got[d] = to_peer(fwd[c * n_src + i], d).reshape(block, wide)
            back_out.append(got)

        def backward(peers, at):
            n_rows = len(peers) * slot_cap
            lo, hi = at * slot_cap, at * slot_cap + n_rows
            args = [v for d in peers for v in dos[d]]
            saved, specs, counts = [], [], []
            for source in ([p[0] for p in own_parts], [p[1] for p in own_parts], [gv2], [sv2]):
                base, n = 0, 0
                for arr in source:
                    rows_in = arr.shape[1]
                    a, b = max(lo, base), min(hi, base + rows_in)
                    if a < b:
                        step = b - a
                        saved.append(arr)
                        specs.append(whole(step, width, (a - base) // step))
                        n += 1
                    base += rows_in
                counts.append(n)
            return call(
                functools.partial(backward_kernel, widths=[len(dos[d]) for d in peers], saved_widths=counts, cols=cols, n_chunk=n_chunk), (own,),
                [whole(slot_cap, v.shape[2]) for v in args] + specs + [whole(model, width)] * 2 + [whole(width, model)] + [whole(model, width)] * 2 + [whole(width, cols)] * 2,
                [whole(slot_cap, wide)] * (len(peers) * n_chunk) + [whole(n_rows, width)] * 2,
                [sds((own, slot_cap, wide), BF16)] * (len(peers) * n_chunk) + [sds((own, n_rows, width), BF16)] * 2,
                cost(4 * own * n_rows * width * (model + 2 * cols), 6e3 * own * n_rows),
                (*args, *saved, w_gelu, w_lin, w_out, wa2, wb2, wcz, wcn),
                [pltpu.VMEM((n_rows, model), BF16)])

        bwd_a = backward(early, 0)
        bwd_b = backward(late, len(early))
        back_in = []
        for c in range(n_chunk):
            got = [None] * n_src
            for peers, vals in ((early, bwd_a), (late, bwd_b)):
                for i, d in enumerate(peers):
                    got[d] = to_peer(vals[c * len(peers) + i], d).reshape(block, wide)
            back_in.append(got)

        all_dos = [v for d in src_order for v in dos[d]]
        grad_wa, grad_wb, grad_wc = call(
            functools.partial(weight_grad_kernel, n_src=n_src, widths=[len(dos[d]) for d in src_order]), (own,),
            [whole(slot_cap, model)] * n_src + [whole(slot_cap, v.shape[2]) for v in all_dos] + [whole(r, width) for r in part_rows] + [whole(rows_early, width), whole(rows_late, width)] * 2,
            [whole(model, width), whole(model, width), whole(width, model)],
            [sds((own, model, width), F32)] * 2 + [sds((own, width, model), F32)],
            cost(6 * own * rows_all * width * model, 40e6),
            (*xs, *all_dos, own_parts[0][2], own_parts[1][2], bwd_a[-2], bwd_b[-2], bwd_a[-1], bwd_b[-1]),
            [pltpu.VMEM((rows_all, model), BF16)])

        def resident(a, b):
            return pl.BlockSpec((a, b), lambda i, *_: (0, 0))

        def tiles(b, col=None):
            return pl.BlockSpec((TOKEN_TILE, b), lambda i, z: (i, 0 if col is None else z[0] * n_chunk + col))

        n_tiles = (n_tokens // TOKEN_TILE,)
        y_mine, y_other, dg_mine, dg_other = [], [], [], []
        for c in range(n_chunk):
            y, dg = call(
                functools.partial(combine_out_kernel, n_src=n_src), n_tiles,
                [tiles(16), tiles(wide, c)] + [resident(block, wide)] * n_src,
                [tiles(wide), pl.BlockSpec((8, TOKEN_TILE), lambda i, z: (0, i))],
                [sds((n_tokens, wide), BF16), sds((8, n_tokens), F32)],
                cost(4 * n_tokens * n_src * block * wide, 6e6),
                (token_cols, dy_rows, *back_out[c]))
            y_mine.append(y)
            dg_mine.append(dg)
            dg_other.append(across(dg))
            y_other.append(across(y))

        dl, dw = call(
            functools.partial(logit_grad_kernel, n_chunk=n_chunk), (1,),
            [resident(16, n_tokens), resident(n_experts, n_tokens), resident(1, n_tokens), resident(1, n_tokens), pl.BlockSpec((n_tokens, cols), lambda i, z: (0, z[0]))] + [resident(8, n_tokens)] * (2 * n_chunk),
            [resident(6 * n_experts, n_tokens), resident(n_experts, cols)],
            [sds((6 * n_experts, n_tokens), BF16), sds((n_experts, cols), F32)],
            cost(2 * 96 * n_tokens * cols, 4e6),
            (rows, prob, id_one, id_two, x_rows, *dg_mine, *dg_other))

        dx_mine, dx_other = [], []
        for c in range(n_chunk):
            dx = call(
                functools.partial(combine_in_kernel, n_src=n_src), n_tiles,
                [tiles(16), pl.BlockSpec((6 * n_experts, TOKEN_TILE), lambda i, z: (0, i)), pl.BlockSpec((n_experts, wide), lambda i, z: (0, z[0] * n_chunk + c))] + [resident(block, wide)] * n_src,
                tiles(wide), sds((n_tokens, wide), BF16),
                cost(2 * n_tokens * n_src * block * wide, 6e6),
                (token_cols, dl, wt, *back_in[c]))
            dx_mine.append(dx)
            dx_other.append(across(dx))
        bit = 1
        while bit < n_src:
            dw = dw + to_peer(dw, bit)
            bit *= 2
        dw_other = across(dw)

        def place(pieces):
            return call(
                place_kernel, (2, 2), [pl.BlockSpec((n_tokens // 2, wide), lambda i, h, z: (i, 0))] * len(pieces),
                pl.BlockSpec((n_tokens // 2, cols), lambda i, h, z: (i, z[0] + h - 2 * h * z[0])),
                sds((n_tokens, model), BF16), cost(1e6, 8e6), pieces)

        act_out = place(y_mine + y_other)
        first_dx = place(dx_mine + dx_other[:-1] + dx_mine[-1:])
        grad_in = pl.pallas_call(
            place_last_kernel,
            grid_spec=pltpu.PrefetchScalarGridSpec(
                num_scalar_prefetch=1, grid=(2,),
                in_specs=[pl.BlockSpec(memory_space=pl.ANY), pl.BlockSpec((n_tokens // 2, wide), lambda i, z: (i, 0))],
                out_specs=pl.BlockSpec((n_tokens // 2, wide), lambda i, z: (i, (1 - z[0]) * n_chunk + n_chunk - 1))),
            out_shape=sds((n_tokens, model), BF16), input_output_aliases={1: 0},
            cost_estimate=cost(1e6, 2e6), name="k_place_dx1")(z, first_dx, dx_other[-1])
        grad_router = jnp.where(z[0] == 0, jnp.concatenate([dw, dw_other], axis=1), jnp.concatenate([dw_other, dw], axis=1)).T
        return act_out, grad_in, grad_wa, grad_wb, grad_wc, grad_router

    return jax.shard_map(local_step, mesh=mesh, in_specs=(P("ep", None), P(), P("ep"), P("ep"), P("ep", None, "tp"), P("ep", None, "tp"), P("ep", "tp", None), P("ep", None)), out_specs=(P("ep", None), P("ep", None), P("ep", None, "tp"), P("ep", None, "tp"), P("ep", "tp", None), P()), check_vma=False)
```

```python
import functools

import jax
import jax.numpy as jnp
from jax import lax
from jax.experimental import pallas as pl
from jax.experimental.pallas import tpu as pltpu
from jax.sharding import PartitionSpec as P


GELU_COEF = 0.7978845608028654
F32 = jnp.float32
BF16 = jnp.bfloat16
NT = (((1,), (1,)), ((), ()))
TN = (((0,), (0,)), ((), ()))
TILE = 256
GATHER_TILE = 256
GROUP = 2
TOKEN_TILE = 512


def gelu_parts(pre_act):
    inner_arg = GELU_COEF * (pre_act + 0.044715 * pre_act * pre_act * pre_act)
    tanh_val = jnp.tanh(inner_arg)
    gelu_val = 0.5 * pre_act * (1.0 + tanh_val)
    gelu_slope = 0.5 * (1.0 + tanh_val) + 0.5 * pre_act * (1.0 - tanh_val * tanh_val) * GELU_COEF * (1.0 + 0.134145 * pre_act * pre_act)
    return gelu_val, gelu_slope


def split3(val):
    high = val.astype(BF16)
    rest = val - high.astype(F32)
    mid = rest.astype(BF16)
    return high, mid, (rest - mid.astype(F32)).astype(BF16)


def route_kernel(me_ref, x_ref, wt_ref, one_ref, two_ref, rows_ref, prob_ref, first_ref, *, slot_cap, own_experts, peer):
    n_experts, n_tokens = prob_ref.shape
    pieces = jnp.concatenate(split3(wt_ref[...]), axis=0)
    raw = lax.dot_general(pieces, x_ref[...], NT, preferred_element_type=F32)
    logits = raw[:n_experts] + raw[n_experts:2 * n_experts] + raw[2 * n_experts:]
    expo = jnp.exp(logits - jnp.max(logits, axis=0, keepdims=True))
    prob = expo / jnp.sum(expo, axis=0, keepdims=True)
    prob_ref[...] = prob
    expert = lax.broadcasted_iota(jnp.int32, (n_experts, n_tokens), 0)
    id_one, id_two = one_ref[...], two_ref[...]
    hot_one = jnp.where(id_one == expert, 1.0, 0.0)
    hot_two = jnp.where(id_two == expert, 1.0, 0.0)
    hots = jnp.concatenate([hot_one, hot_two], axis=0)
    before = lax.broadcasted_iota(jnp.int32, (TILE, TILE), 0) < lax.broadcasted_iota(jnp.int32, (TILE, TILE), 1)
    tri = jnp.where(before, 1.0, 0.0).astype(BF16)
    run = jnp.zeros((2 * n_experts, 1), F32)
    counts = []
    for b in range(n_tokens // TILE):
        part = hots[:, b * TILE:(b + 1) * TILE]
        counts.append(jnp.dot(part.astype(BF16), tri, preferred_element_type=F32) + run)
        run = run + jnp.sum(part, axis=1, keepdims=True)
    count = jnp.concatenate(counts, axis=1)
    pos_one = jnp.sum(count[:n_experts] * hot_one, axis=0, keepdims=True)
    pos_two = jnp.sum((count[n_experts:] + run[:n_experts]) * hot_two, axis=0, keepdims=True)
    prob_one = jnp.sum(prob * hot_one, axis=0, keepdims=True)
    prob_two = jnp.sum(prob * hot_two, axis=0, keepdims=True)
    turn = me_ref[0] * (own_experts * slot_cap)

    def slot_of(ids, pos):
        place = pos.astype(jnp.int32)
        slot = jnp.where(place < slot_cap, ids * slot_cap + place, n_experts * slot_cap)
        return jnp.bitwise_xor(slot, turn).astype(F32)

    gate_sum = prob_one + prob_two
    slot_one, slot_two = slot_of(id_one, pos_one), slot_of(id_two, pos_two)
    block = first_ref.shape[0]
    slot = (peer * block + lax.broadcasted_iota(jnp.int32, (block, n_tokens), 0)).astype(F32)
    hit = jnp.logical_or(slot_one == slot, slot_two == slot)
    first_ref[...] = jnp.dot(jnp.where(hit, 1.0, 0.0).astype(BF16), x_ref[...], preferred_element_type=F32).astype(BF16)
    rows_ref[...] = jnp.concatenate(
        [slot_one, slot_two, prob_one / gate_sum, prob_two / gate_sum, prob_one, prob_two, jnp.zeros((10, n_tokens), F32)],
        axis=0)


def gather_kernel(z_ref, rows_ref, src_ref, *outs, peers, per, scaled):
    step = pl.program_id(0)
    n_tokens = src_ref.shape[0]
    peer = sum(jnp.where(step // per == i, d, 0) for i, d in enumerate(peers))
    slot = (peer * per + step % per) * GATHER_TILE + lax.broadcasted_iota(jnp.int32, (GATHER_TILE, n_tokens), 0)
    slot = slot.astype(F32)
    hit_one = rows_ref[0:1, :] == slot
    hit_two = rows_ref[1:2, :] == slot
    pick = jnp.where(jnp.logical_or(hit_one, hit_two), 1.0, 0.0).astype(BF16)
    val = jnp.dot(pick, src_ref[...], preferred_element_type=F32)
    if scaled:
        gate = jnp.where(hit_one, rows_ref[2:3, :], 0.0) + jnp.where(hit_two, rows_ref[3:4, :], 0.0)
        val = jnp.sum(gate, axis=1, keepdims=True) * val
    val = val.astype(BF16)
    for i, out in enumerate(outs):
        @pl.when(step // per == i)
        def _(out=out):
            out[...] = val


def forward_own_kernel(z_ref, *refs, n_src, cols):
    xs = refs[:n_src]
    wa, wb, wc, gv_ref, sv_ref, h_ref, part_ref = refs[n_src:]
    cap = xs[0].shape[1]
    col = pl.ds(pl.multiple_of(z_ref[0] * cols, cols), cols)
    group = GROUP
    for first in range(0, n_src, group):
        x = jnp.concatenate([r[0] for r in xs[first:first + group]], axis=0)
        rows = slice(first * cap, (first + group) * cap)
        pre_a = jnp.dot(x, wa[0], preferred_element_type=F32)
        pre_b = jnp.dot(x, wb[0], preferred_element_type=F32)
        gelu_val, gelu_slope = gelu_parts(pre_a)
        hidden = (gelu_val * pre_b).astype(BF16)
        gv_ref[0, rows, :] = gelu_val
        sv_ref[0, rows, :] = pre_b * gelu_slope
        h_ref[0, rows, :] = hidden
        part_ref[0, rows, :] = jnp.dot(hidden, wc[0, :, col], preferred_element_type=F32).astype(BF16)


def forward_other_kernel(*refs, n_src, n_chunk):
    xs = refs[:n_src]
    part_ref, part2_ref, wa, wb, wc = refs[n_src:n_src + 5]
    outs = refs[n_src + 5:n_src + 5 + n_chunk * n_src]
    gv_ref, sv_ref = refs[n_src + 5 + n_chunk * n_src:]
    parts = jnp.concatenate([part_ref[0], part2_ref[0]], axis=0)
    cap = xs[0].shape[1]
    wide = outs[0].shape[2]
    group = GROUP
    for first in range(0, n_src, GROUP):
        x = jnp.concatenate([r[0] for r in xs[first:first + GROUP]], axis=0)
        rows = slice(first * cap, (first + GROUP) * cap)
        pre_a = jnp.dot(x, wa[0], preferred_element_type=F32)
        pre_b = jnp.dot(x, wb[0], preferred_element_type=F32)
        gelu_val, gelu_slope = gelu_parts(pre_a)
        hidden = (gelu_val * pre_b).astype(BF16)
        gv_ref[0, rows, :] = gelu_val
        sv_ref[0, rows, :] = pre_b * gelu_slope
        part = jnp.dot(hidden, wc[0], preferred_element_type=F32).astype(BF16).astype(F32)
        total = (parts[rows].astype(F32) + part).astype(BF16)
        for c in range(n_chunk):
            for i in range(group):
                outs[c * n_src + first + i][0] = total[i * cap:(i + 1) * cap, c * wide:(c + 1) * wide]


def put_rows(z, rows, ref, dest):
    if len(ref) == 1:
        dest[rows, :] = ref[0][0]
        return
    cols = ref[0].shape[2]
    dest[rows, pl.ds(pl.multiple_of(z * cols, cols), cols)] = ref[0][0]
    dest[rows, pl.ds(pl.multiple_of((1 - z) * cols, cols), cols)] = ref[1][0]


def group_refs(refs, widths):
    groups, at = [], 0
    for w in widths:
        groups.append(refs[at:at + w])
        at += w
    return groups, refs[at:]


def backward_kernel(z_ref, *refs, widths, saved_widths, cols, n_chunk):
    dos, refs = group_refs(refs, widths)
    n_src = len(widths)
    saved, refs = group_refs(refs, saved_widths)
    wa, wb, wc, wa2, wb2, wcz, wcn = refs[:7]
    outs = refs[7:7 + n_chunk * n_src]
    da_ref, db_ref, do_ref = refs[7 + n_chunk * n_src:]
    gv, sv, gv2, sv2 = [jnp.concatenate([r[0] for r in group], axis=0) if len(group) > 1 else group[0][0] for group in saved]
    cap = dos[0][0].shape[1]
    z = z_ref[0]
    near = pl.ds(pl.multiple_of(z * cols, cols), cols)
    far = pl.ds(pl.multiple_of((1 - z) * cols, cols), cols)
    wide = cols // n_chunk
    head = pl.ds(pl.multiple_of(z * cols, cols), wide)
    shared = (slice(wide, cols), slice(cols + wide, 2 * cols))
    group = GROUP
    for first in range(0, n_src, group):
        rows = slice(first * cap, (first + group) * cap)
        for i in range(first, first + group):
            put_rows(z, slice(i * cap, (i + 1) * cap), dos[i], do_ref)
        totals = [None, None]
        for k, (a_ref, b_ref, slope, gelu) in enumerate(((wa, wb, sv, gv), (wa2, wb2, sv2, gv2))):
            if k == 0:
                dhid = lax.dot_general(do_ref[rows, :], wc[0], NT, preferred_element_type=F32)
            else:
                dhid = lax.dot_general(do_ref[rows, near], wcz[0], NT, preferred_element_type=F32)
                dhid = dhid + lax.dot_general(do_ref[rows, far], wcn[0], NT, preferred_element_type=F32)
            grad_a = (dhid * slope[rows]).astype(BF16)
            grad_b = (dhid * gelu[rows]).astype(BF16)
            if k == 0:
                da_ref[0, rows, :] = grad_a
                db_ref[0, rows, :] = grad_b
            for c, picks in enumerate(((head,), shared)):
                parts = [lax.dot_general(grad_a, a_ref[0, p, :], NT, preferred_element_type=F32) + lax.dot_general(grad_b, b_ref[0, p, :], NT, preferred_element_type=F32) for p in picks]
                part = jnp.concatenate(parts, axis=1).astype(BF16).astype(F32)
                totals[c] = part if k == 0 else totals[c] + part
        for c in range(2):
            total = totals[c].astype(BF16)
            for i in range(group):
                outs[c * n_src + first + i][0] = total[i * cap:(i + 1) * cap]


def weight_grad_kernel(z_ref, *refs, n_src, widths):
    xs = refs[:n_src]
    dos, refs = group_refs(refs[n_src:], widths)
    h_ref, h2_ref, da_ref, da2_ref, db_ref, db2_ref, ga_ref, gb_ref, gc_ref, do_ref = refs
    cap = xs[0].shape[1]
    for i, ref in enumerate(dos):
        put_rows(z_ref[0], slice(i * cap, (i + 1) * cap), ref, do_ref)
    x = jnp.concatenate([r[0] for r in xs], axis=0)
    grad_a = jnp.concatenate([da_ref[0], da2_ref[0]], axis=0)
    grad_b = jnp.concatenate([db_ref[0], db2_ref[0]], axis=0)
    ga_ref[0] = lax.dot_general(x, grad_a, TN, preferred_element_type=F32)
    gb_ref[0] = lax.dot_general(x, grad_b, TN, preferred_element_type=F32)
    gc_ref[0] = lax.dot_general(jnp.concatenate([h_ref[0], h2_ref[0]], axis=0), do_ref[...], TN, preferred_element_type=F32)


def slot_picks(cols_ref):
    lane = lax.broadcasted_iota(jnp.int32, (TOKEN_TILE, 128), 1).astype(F32)
    picks = []
    for k in range(2):
        slot = cols_ref[:, k:k + 1]
        blk = jnp.floor(slot * (1.0 / 128.0))
        hot = jnp.where(slot - 128.0 * blk == lane, 1.0, 0.0).astype(BF16)
        picks.append((jnp.broadcast_to(blk, (TOKEN_TILE, 128)).astype(BF16), hot))
    return picks


def combine_out_kernel(z_ref, cols_ref, dy_ref, *refs, n_src):
    srcs = refs[:n_src]
    y_ref, dg_ref = refs[n_src:]
    blocks = srcs[0].shape[0] // 128
    picks = slot_picks(cols_ref)
    zero = jnp.zeros((TOKEN_TILE, 128), BF16)
    both = None
    for d in range(n_src):
        pick = jnp.concatenate(
            [jnp.concatenate([jnp.where(blk == jnp.asarray(d * blocks + b, BF16), hot, zero) for b in range(blocks)], axis=1) for blk, hot in picks], axis=0)
        part = jnp.dot(pick, srcs[d][...], preferred_element_type=F32)
        both = part if both is None else both + part
    dy = dy_ref[...].astype(F32)
    one, two = both[:TOKEN_TILE], both[TOKEN_TILE:]
    y_ref[...] = (cols_ref[:, 2:3] * one + cols_ref[:, 3:4] * two).astype(BF16)
    dg_one = jnp.sum(dy * one, axis=1, keepdims=True)
    dg_two = jnp.sum(dy * two, axis=1, keepdims=True)
    wide = jnp.concatenate([dg_one, dg_two, jnp.zeros((TOKEN_TILE, 126), F32)], axis=1)
    dg_ref[...] = wide.T[:8, :]


def logit_grad_kernel(z_ref, rows_ref, prob_ref, one_ref, two_ref, x_ref, dga_ref, dgb_ref, dl_ref, dw_ref):
    n_experts, n_tokens = prob_ref.shape
    dgate = dga_ref[0:2, :] + dgb_ref[0:2, :]
    dg_one, dg_two = dgate[0:1], dgate[1:2]
    gate_one, gate_two = rows_ref[2:3, :], rows_ref[3:4, :]
    prob_one, prob_two = rows_ref[4:5, :], rows_ref[5:6, :]
    shared = dg_one * gate_one + dg_two * gate_two
    gate_sum = prob_one + prob_two
    dp_one = (dg_one - shared) / gate_sum
    dp_two = (dg_two - shared) / gate_sum
    centre = dp_one * prob_one + dp_two * prob_two
    expert = lax.broadcasted_iota(jnp.int32, (n_experts, n_tokens), 0)
    inner = jnp.where(one_ref[...] == expert, dp_one, 0.0) + jnp.where(two_ref[...] == expert, dp_two, 0.0) - centre
    high, mid, low = split3(prob_ref[...] * inner)
    dl_ref[...] = jnp.concatenate([high, high, mid, high, low, mid], axis=0)
    raw = jnp.dot(jnp.concatenate([high, mid, low], axis=0), x_ref[...], preferred_element_type=F32)
    dw_ref[...] = raw[:n_experts] + raw[n_experts:2 * n_experts] + raw[2 * n_experts:]


def combine_in_kernel(z_ref, cols_ref, dl_ref, *refs, n_src, last):
    n_w = 2 if last else 1
    wts, refs = refs[:n_w], refs[n_w:]
    srcs, refs = refs[:n_src], refs[n_src:]
    blocks = srcs[0].shape[0] // 128
    (blk_one, hot_one), (blk_two, hot_two) = slot_picks(cols_ref)
    zero = jnp.zeros((TOKEN_TILE, 128), BF16)
    acc = None
    for d in range(n_src):
        parts = []
        for b in range(blocks):
            this = jnp.asarray(d * blocks + b, BF16)
            parts.append(jnp.where(blk_one == this, hot_one, jnp.where(blk_two == this, hot_two, zero)))
        part = jnp.dot(jnp.concatenate(parts, axis=1), srcs[d][...], preferred_element_type=F32)
        acc = part if acc is None else acc + part
    high, mid, low = split3(jnp.concatenate([w[...] for w in wts], axis=1))
    weights = jnp.concatenate([high, mid, high, low, high, mid], axis=0)
    back = lax.dot_general(dl_ref[...], weights, TN, preferred_element_type=F32)
    res = (acc + back).astype(BF16)
    if not last:
        refs[0][...] = res
        return
    mine, other, dx_ref = refs
    wide = mine.shape[1]
    low_side = z_ref[0] == 0
    dx_ref[:, :wide] = jnp.where(low_side, mine[...], other[...])
    dx_ref[:, wide:2 * wide] = res[:, :wide]
    dx_ref[:, 2 * wide:3 * wide] = jnp.where(low_side, other[...], mine[...])
    dx_ref[:, 3 * wide:] = res[:, wide:]


def sum_kernel(z_ref, *refs):
    parts, out = [r[...] for r in refs[:-1]], refs[-1]
    while len(parts) > 1:
        parts = [parts[i] + parts[i + 1] for i in range(0, len(parts), 2)]
    out[...] = parts[0]


def cost(flops, nbytes, trans=0):
    return pl.CostEstimate(flops=int(flops), bytes_accessed=int(nbytes), transcendentals=int(trans))


def solution(mesh):
    tp_size = mesh.shape["tp"]
    n_src = mesh.shape["ep"]
    n_chunk = 2
    all_vmem = pltpu.CompilerParams(vmem_limit_bytes=67043328)
    diag = [n_src - 2, n_src - 1]
    early = diag + [0, 1]
    late = [2, 4, 3, 5]
    src_order = early + late
    first_peer = 6

    def local_step(x_rows, w_router, first_ids, second_ids, w_gelu, w_lin, w_out, dy_rows):
        n_tokens, model = x_rows.shape
        n_experts = w_router.shape[1]
        own, width = w_gelu.shape[0], w_gelu.shape[2]
        slot_cap = 2 * n_tokens // n_experts
        block = own * slot_cap
        cols = model // tp_size
        wide = cols // n_chunk
        rows_all = n_src * slot_cap
        rows_early = len(early) * slot_cap
        rows_late = len(late) * slot_cap
        sds = jax.ShapeDtypeStruct
        me = lax.axis_index("ep").astype(jnp.int32).reshape(1)
        z = lax.axis_index("tp").astype(jnp.int32).reshape(1)
        swap = [(i, tp_size - 1 - i) for i in range(tp_size)]

        def across(val):
            return lax.ppermute(val, "tp", swap)

        def to_peer(val, d):
            if d == 0:
                return val
            return lax.ppermute(val, "ep", [(i, i ^ d) for i in range(n_src)])

        def call(kernel, grid, in_specs, out_specs, out_shape, estimate, args, scratch=()):
            return pl.pallas_call(
                kernel,
                grid_spec=pltpu.PrefetchScalarGridSpec(num_scalar_prefetch=1, grid=grid, in_specs=in_specs, out_specs=out_specs, scratch_shapes=list(scratch)),
                out_shape=out_shape, cost_estimate=estimate, compiler_params=all_vmem)(z, *args)

        wa2, wb2 = across(w_gelu), across(w_lin)
        wt = w_router.T
        id_one, id_two = first_ids.reshape(1, n_tokens), second_ids.reshape(1, n_tokens)
        rows, prob, first_x = pl.pallas_call(
            functools.partial(route_kernel, slot_cap=slot_cap, own_experts=own, peer=first_peer),
            in_specs=[pl.BlockSpec(memory_space=pltpu.SMEM)] + [pl.BlockSpec(memory_space=pltpu.VMEM)] * 4,
            out_shape=(sds((16, n_tokens), F32), sds((n_experts, n_tokens), F32), sds((block, model), BF16)),
            cost_estimate=cost(2 * 96 * n_tokens * model, 2 * n_tokens * model, n_experts * n_tokens),
            compiler_params=all_vmem, name="route",
        )(me, x_rows, wt, id_one, id_two)
        token_cols = rows.T
        wcz = across(lax.dynamic_slice_in_dim(w_out, (1 - z[0]) * cols, cols, 2))
        wcn = across(lax.dynamic_slice_in_dim(w_out, z[0] * cols, cols, 2))

        per = block // GATHER_TILE

        def gather(src, peers, scaled, part=False):
            width_out = cols if part else model

            def out_map(g, z, i):
                return (jnp.clip(g - i * per, 0, per - 1), 0)

            def src_map(g, z):
                return (0, z[0] if part else 0)

            return call(
                functools.partial(gather_kernel, peers=peers, per=per, scaled=scaled), (len(peers) * per,),
                [pl.BlockSpec((16, n_tokens), lambda g, z: (0, 0)), pl.BlockSpec((n_tokens, width_out), src_map)],
                [pl.BlockSpec((GATHER_TILE, width_out), functools.partial(out_map, i=i)) for i in range(len(peers))],
                [sds((block, width_out), BF16)] * len(peers),
                cost(2 * len(peers) * block * n_tokens * width_out, 2 * (n_tokens + len(peers) * block) * width_out),
                (rows, src))

        xs, dos = [None] * n_src, [None] * n_src
        xs[first_peer] = to_peer(first_x, first_peer).reshape(own, slot_cap, model)
        for peers in ([4, 2], [7, 1, 0], [5, 3]):
            for d, val in zip(peers, gather(x_rows, peers, False)):
                xs[d] = to_peer(val, d).reshape(own, slot_cap, model)
        for peers in (diag, [4, 2]):
            for d, val in zip(peers, gather(dy_rows, peers, True, part=True)):
                mine = to_peer(val, d)
                dos[d] = tuple(v.reshape(own, slot_cap, cols) for v in (mine, across(mine)))
        for peers in ([1, 0], [5, 3]):
            for d, val in zip(peers, gather(dy_rows, peers, True)):
                dos[d] = (to_peer(val, d).reshape(own, slot_cap, model),)
        xs = [xs[d] for d in src_order]

        def whole(a, b, at=0):
            return pl.BlockSpec((1, a, b), lambda e, *_: (e, at, 0))

        def forward_own(lo, hi):
            n_rows = (hi - lo) * slot_cap
            return call(
                functools.partial(forward_own_kernel, n_src=hi - lo, cols=cols), (own,),
                [whole(slot_cap, model)] * (hi - lo) + [whole(model, width)] * 2 + [whole(width, model)],
                [whole(n_rows, width)] * 3 + [whole(n_rows, cols)],
                [sds((own, n_rows, width), F32)] * 2 + [sds((own, n_rows, width), BF16), sds((own, n_rows, cols), BF16)],
                cost(2 * own * n_rows * width * (2 * model + cols), 8e3 * own * n_rows, own * n_rows * width),
                (*xs[lo:hi], w_gelu, w_lin, w_out))

        cuts = (0, n_src - 2, n_src)
        own_parts = [forward_own(cuts[i], cuts[i + 1]) for i in range(2)]
        part_rows = [(cuts[i + 1] - cuts[i]) * slot_cap for i in range(2)]
        fwd = pl.pallas_call(
            functools.partial(forward_other_kernel, n_src=n_src, n_chunk=1), grid=(own,),
            in_specs=[whole(slot_cap, model)] * n_src + [whole(r, cols) for r in part_rows] + [whole(model, width)] * 2 + [whole(width, cols)],
            out_specs=[whole(slot_cap, cols)] * n_src + [whole(rows_all, width)] * 2,
            out_shape=[sds((own, slot_cap, cols), BF16)] * n_src + [sds((own, rows_all, width), F32)] * 2,
            cost_estimate=cost(2 * own * rows_all * width * (2 * model + cols), 32e6, own * rows_all * width),
            compiler_params=all_vmem, name="k_fwd_other")(*xs, own_parts[0][3], own_parts[1][3], wa2, wb2, wcz)
        gv2, sv2 = fwd[n_src:]
        back_out = [None] * n_src
        for i, d in enumerate(src_order):
            back_out[d] = to_peer(fwd[i], d).reshape(block, cols)

        dx_widths = (wide, 2 * wide)

        def backward(peers, at):
            n_rows = len(peers) * slot_cap
            lo, hi = at * slot_cap, at * slot_cap + n_rows
            args = [v for d in peers for v in dos[d]]
            saved, specs, counts = [], [], []
            for source in ([p[0] for p in own_parts], [p[1] for p in own_parts], [gv2], [sv2]):
                base, n = 0, 0
                for arr in source:
                    rows_in = arr.shape[1]
                    a, b = max(lo, base), min(hi, base + rows_in)
                    if a < b:
                        step = b - a
                        saved.append(arr)
                        specs.append(whole(step, width, (a - base) // step))
                        n += 1
                    base += rows_in
                counts.append(n)
            return call(
                functools.partial(backward_kernel, widths=[len(dos[d]) for d in peers], saved_widths=counts, cols=cols, n_chunk=n_chunk), (own,),
                [whole(slot_cap, v.shape[2]) for v in args] + specs + [whole(model, width)] * 2 + [whole(width, model)] + [whole(model, width)] * 2 + [whole(width, cols)] * 2,
                [whole(slot_cap, w) for w in dx_widths for _ in peers] + [whole(n_rows, width)] * 2,
                [sds((own, slot_cap, w), BF16) for w in dx_widths for _ in peers] + [sds((own, n_rows, width), BF16)] * 2,
                cost(4 * own * n_rows * width * (model + 2 * cols), 6e3 * own * n_rows),
                (*args, *saved, w_gelu, w_lin, w_out, wa2, wb2, wcz, wcn),
                [pltpu.VMEM((n_rows, model), BF16)])

        bwd_a = backward(early, 0)
        bwd_b = backward(late, len(early))
        back_in = []
        for c in range(n_chunk):
            got = [None] * n_src
            for peers, vals in ((early, bwd_a), (late, bwd_b)):
                for i, d in enumerate(peers):
                    got[d] = to_peer(vals[c * len(peers) + i], d).reshape(block, dx_widths[c])
            back_in.append(got)

        all_dos = [v for d in src_order for v in dos[d]]
        grad_wa, grad_wb, grad_wc = call(
            functools.partial(weight_grad_kernel, n_src=n_src, widths=[len(dos[d]) for d in src_order]), (own,),
            [whole(slot_cap, model)] * n_src + [whole(slot_cap, v.shape[2]) for v in all_dos] + [whole(r, width) for r in part_rows] + [whole(rows_early, width), whole(rows_late, width)] * 2,
            [whole(model, width), whole(model, width), whole(width, model)],
            [sds((own, model, width), F32)] * 2 + [sds((own, width, model), F32)],
            cost(6 * own * rows_all * width * model, 40e6),
            (*xs, *all_dos, own_parts[0][2], own_parts[1][2], bwd_a[-2], bwd_b[-2], bwd_a[-1], bwd_b[-1]),
            [pltpu.VMEM((rows_all, model), BF16)])

        def resident(a, b):
            return pl.BlockSpec((a, b), lambda i, *_: (0, 0))

        def tiles(b, col=None):
            return pl.BlockSpec((TOKEN_TILE, b), lambda i, z: (i, 0 if col is None else z[0] * n_chunk + col))

        n_tiles = (n_tokens // TOKEN_TILE,)
        y_mine, dg_mine = call(
            functools.partial(combine_out_kernel, n_src=n_src), n_tiles,
            [tiles(16), pl.BlockSpec((TOKEN_TILE, cols), lambda i, z: (i, z[0]))] + [resident(block, cols)] * n_src,
            [tiles(cols), pl.BlockSpec((8, TOKEN_TILE), lambda i, z: (0, i))],
            [sds((n_tokens, cols), BF16), sds((8, n_tokens), F32)],
            cost(4 * n_tokens * n_src * block * cols, 12e6),
            (token_cols, dy_rows, *back_out))
        dg_other = across(dg_mine)
        y_other = across(y_mine)

        dl, dw = call(
            logit_grad_kernel, (1,),
            [resident(16, n_tokens), resident(n_experts, n_tokens), resident(1, n_tokens), resident(1, n_tokens), pl.BlockSpec((n_tokens, cols), lambda i, z: (0, z[0]))] + [resident(8, n_tokens)] * 2,
            [resident(6 * n_experts, n_tokens), resident(n_experts, cols)],
            [sds((6 * n_experts, n_tokens), BF16), sds((n_experts, cols), F32)],
            cost(2 * 96 * n_tokens * cols, 4e6),
            (rows, prob, id_one, id_two, x_rows, dg_mine, dg_other))

        def combine_in(last, extra, srcs):
            quarters = [(lambda i, z: (0, 1)), (lambda i, z: (0, 3))] if last else [lambda i, z: (0, z[0] * n_chunk)]
            return call(
                functools.partial(combine_in_kernel, n_src=n_src, last=last), n_tiles,
                [tiles(16), pl.BlockSpec((6 * n_experts, TOKEN_TILE), lambda i, z: (0, i))] + [pl.BlockSpec((n_experts, wide), q) for q in quarters]
                + [resident(block, v.shape[1]) for v in srcs] + [tiles(wide)] * len(extra),
                tiles(model if last else wide), sds((n_tokens, model if last else wide), BF16),
                cost(2 * n_tokens * n_src * block * srcs[0].shape[1], 8e6),
                (token_cols, dl, *([wt] * len(quarters)), *srcs, *extra))

        dx_mine = combine_in(False, (), back_in[0])
        dx_other = across(dx_mine)
        grad_in = combine_in(True, (dx_mine, dx_other), back_in[1])

        def add_all(parts):
            return call(sum_kernel, (1,), [resident(n_experts, cols)] * len(parts), resident(n_experts, cols), sds((n_experts, cols), F32), cost(1e6, 4e5), parts)

        dw = add_all((dw, to_peer(dw, 2), to_peer(dw, 4), to_peer(dw, 6)))
        dw = add_all((dw, to_peer(dw, 1)))
        dw_other = across(dw)

        lower = z[0] == 0

        def join(mine, other):
            return jnp.where(lower, jnp.concatenate([mine, other], axis=1), jnp.concatenate([other, mine], axis=1))

        act_out = join(y_mine, y_other)
        grad_router = join(dw, dw_other).T
        return act_out, grad_in, grad_wa, grad_wb, grad_wc, grad_router

    return jax.shard_map(local_step, mesh=mesh, in_specs=(P("ep", None), P(), P("ep"), P("ep"), P("ep", None, "tp"), P("ep", None, "tp"), P("ep", "tp", None), P("ep", None)), out_specs=(P("ep", None), P("ep", None), P("ep", None, "tp"), P("ep", None, "tp"), P("ep", "tp", None), P()), check_vma=False)
```

```python
import functools

import jax
import jax.numpy as jnp
from jax import lax
from jax.experimental import pallas as pl
from jax.experimental.pallas import tpu as pltpu
from jax.sharding import PartitionSpec as P


GELU_COEF = 0.7978845608028654
F32 = jnp.float32
BF16 = jnp.bfloat16
NT = (((1,), (1,)), ((), ()))
TN = (((0,), (0,)), ((), ()))
TILE = 256
GATHER_TILE = 256
GROUP = 2
TOKEN_TILE = 512


def gelu_parts(pre_act):
    inner_arg = GELU_COEF * (pre_act + 0.044715 * pre_act * pre_act * pre_act)
    tanh_val = jnp.tanh(inner_arg)
    gelu_val = 0.5 * pre_act * (1.0 + tanh_val)
    gelu_slope = 0.5 * (1.0 + tanh_val) + 0.5 * pre_act * (1.0 - tanh_val * tanh_val) * GELU_COEF * (1.0 + 0.134145 * pre_act * pre_act)
    return gelu_val, gelu_slope


def split3(val):
    high = val.astype(BF16)
    rest = val - high.astype(F32)
    mid = rest.astype(BF16)
    return high, mid, (rest - mid.astype(F32)).astype(BF16)


def slots_kernel(me_ref, x_ref, one_ref, two_ref, slots_ref, first_ref, *, slot_cap, own_experts, n_experts, peer):
    n_tokens = x_ref.shape[0]
    expert = lax.broadcasted_iota(jnp.int32, (n_experts, n_tokens), 0)
    id_one, id_two = one_ref[...], two_ref[...]
    hot_one = jnp.where(id_one == expert, 1.0, 0.0)
    hot_two = jnp.where(id_two == expert, 1.0, 0.0)
    hots = jnp.concatenate([hot_one, hot_two], axis=0)
    before = lax.broadcasted_iota(jnp.int32, (TILE, TILE), 0) < lax.broadcasted_iota(jnp.int32, (TILE, TILE), 1)
    tri = jnp.where(before, 1.0, 0.0).astype(BF16)
    run = jnp.zeros((2 * n_experts, 1), F32)
    counts = []
    for b in range(n_tokens // TILE):
        part = hots[:, b * TILE:(b + 1) * TILE]
        counts.append(jnp.dot(part.astype(BF16), tri, preferred_element_type=F32) + run)
        run = run + jnp.sum(part, axis=1, keepdims=True)
    count = jnp.concatenate(counts, axis=1)
    pos_one = jnp.sum(count[:n_experts] * hot_one, axis=0, keepdims=True)
    pos_two = jnp.sum((count[n_experts:] + run[:n_experts]) * hot_two, axis=0, keepdims=True)
    turn = me_ref[0] * (own_experts * slot_cap)

    def slot_of(ids, pos):
        place = pos.astype(jnp.int32)
        slot = jnp.where(place < slot_cap, ids * slot_cap + place, n_experts * slot_cap)
        return jnp.bitwise_xor(slot, turn).astype(F32)

    slot_one, slot_two = slot_of(id_one, pos_one), slot_of(id_two, pos_two)
    slots_ref[...] = jnp.concatenate([slot_one, slot_two, jnp.zeros((6, n_tokens), F32)], axis=0)
    block = first_ref.shape[0]
    slot = (peer * block + lax.broadcasted_iota(jnp.int32, (block, n_tokens), 0)).astype(F32)
    hit = jnp.logical_or(slot_one == slot, slot_two == slot)
    first_ref[...] = jnp.dot(jnp.where(hit, 1.0, 0.0).astype(BF16), x_ref[...], preferred_element_type=F32).astype(BF16)


def route_kernel(x_ref, wt_ref, one_ref, two_ref, slots_ref, rows_ref, prob_ref):
    n_experts, n_tokens = prob_ref.shape
    pieces = jnp.concatenate(split3(wt_ref[...]), axis=0)
    raw = lax.dot_general(pieces, x_ref[...], NT, preferred_element_type=F32)
    logits = raw[:n_experts] + raw[n_experts:2 * n_experts] + raw[2 * n_experts:]
    expo = jnp.exp(logits - jnp.max(logits, axis=0, keepdims=True))
    prob = expo / jnp.sum(expo, axis=0, keepdims=True)
    prob_ref[...] = prob
    expert = lax.broadcasted_iota(jnp.int32, (n_experts, n_tokens), 0)
    prob_one = jnp.sum(jnp.where(one_ref[...] == expert, prob, 0.0), axis=0, keepdims=True)
    prob_two = jnp.sum(jnp.where(two_ref[...] == expert, prob, 0.0), axis=0, keepdims=True)
    gate_sum = prob_one + prob_two
    rows_ref[...] = jnp.concatenate(
        [slots_ref[0:2, :], prob_one / gate_sum, prob_two / gate_sum, prob_one, prob_two, jnp.zeros((10, n_tokens), F32)], axis=0)


def gather_kernel(z_ref, rows_ref, src_ref, *outs, peers, per, scaled):
    step = pl.program_id(0)
    n_tokens = src_ref.shape[0]
    peer = sum(jnp.where(step // per == i, d, 0) for i, d in enumerate(peers))
    slot = (peer * per + step % per) * GATHER_TILE + lax.broadcasted_iota(jnp.int32, (GATHER_TILE, n_tokens), 0)
    slot = slot.astype(F32)
    hit_one = rows_ref[0:1, :] == slot
    hit_two = rows_ref[1:2, :] == slot
    pick = jnp.where(jnp.logical_or(hit_one, hit_two), 1.0, 0.0).astype(BF16)
    val = jnp.dot(pick, src_ref[...], preferred_element_type=F32)
    if scaled:
        gate = jnp.where(hit_one, rows_ref[2:3, :], 0.0) + jnp.where(hit_two, rows_ref[3:4, :], 0.0)
        val = jnp.sum(gate, axis=1, keepdims=True) * val
    val = val.astype(BF16)
    for i, out in enumerate(outs):
        @pl.when(step // per == i)
        def _(out=out):
            out[...] = val


def forward_own_kernel(z_ref, *refs, n_src, cols):
    xs = refs[:n_src]
    wa, wb, wc, gv_ref, sv_ref, h_ref, part_ref = refs[n_src:]
    cap = xs[0].shape[1]
    col = pl.ds(pl.multiple_of(z_ref[0] * cols, cols), cols)
    group = GROUP
    for first in range(0, n_src, group):
        x = jnp.concatenate([r[0] for r in xs[first:first + group]], axis=0)
        rows = slice(first * cap, (first + group) * cap)
        pre_a = jnp.dot(x, wa[0], preferred_element_type=F32)
        pre_b = jnp.dot(x, wb[0], preferred_element_type=F32)
        gelu_val, gelu_slope = gelu_parts(pre_a)
        hidden = (gelu_val * pre_b).astype(BF16)
        gv_ref[0, rows, :] = gelu_val
        sv_ref[0, rows, :] = pre_b * gelu_slope
        h_ref[0, rows, :] = hidden
        part_ref[0, rows, :] = jnp.dot(hidden, wc[0, :, col], preferred_element_type=F32).astype(BF16)


def forward_other_kernel(*refs, n_src, n_chunk):
    xs = refs[:n_src]
    part_ref, part2_ref, wa, wb, wc = refs[n_src:n_src + 5]
    outs = refs[n_src + 5:n_src + 5 + n_chunk * n_src]
    gv_ref, sv_ref = refs[n_src + 5 + n_chunk * n_src:]
    parts = jnp.concatenate([part_ref[0], part2_ref[0]], axis=0)
    cap = xs[0].shape[1]
    wide = outs[0].shape[2]
    group = GROUP
    for first in range(0, n_src, GROUP):
        x = jnp.concatenate([r[0] for r in xs[first:first + GROUP]], axis=0)
        rows = slice(first * cap, (first + GROUP) * cap)
        pre_a = jnp.dot(x, wa[0], preferred_element_type=F32)
        pre_b = jnp.dot(x, wb[0], preferred_element_type=F32)
        gelu_val, gelu_slope = gelu_parts(pre_a)
        hidden = (gelu_val * pre_b).astype(BF16)
        gv_ref[0, rows, :] = gelu_val
        sv_ref[0, rows, :] = pre_b * gelu_slope
        part = jnp.dot(hidden, wc[0], preferred_element_type=F32).astype(BF16).astype(F32)
        total = (parts[rows].astype(F32) + part).astype(BF16)
        for c in range(n_chunk):
            for i in range(group):
                outs[c * n_src + first + i][0] = total[i * cap:(i + 1) * cap, c * wide:(c + 1) * wide]


def put_rows(z, rows, ref, dest):
    if len(ref) == 1:
        dest[rows, :] = ref[0][0]
        return
    cols = ref[0].shape[2]
    dest[rows, pl.ds(pl.multiple_of(z * cols, cols), cols)] = ref[0][0]
    dest[rows, pl.ds(pl.multiple_of((1 - z) * cols, cols), cols)] = ref[1][0]


def group_refs(refs, widths):
    groups, at = [], 0
    for w in widths:
        groups.append(refs[at:at + w])
        at += w
    return groups, refs[at:]


def backward_kernel(z_ref, *refs, widths, saved_widths, cols, n_chunk):
    dos, refs = group_refs(refs, widths)
    n_src = len(widths)
    saved, refs = group_refs(refs, saved_widths)
    wa, wb, wc, wa2, wb2, wcz, wcn = refs[:7]
    outs = refs[7:7 + n_chunk * n_src]
    da_ref, db_ref, do_ref = refs[7 + n_chunk * n_src:]
    gv, sv, gv2, sv2 = [jnp.concatenate([r[0] for r in group], axis=0) if len(group) > 1 else group[0][0] for group in saved]
    cap = dos[0][0].shape[1]
    z = z_ref[0]
    near = pl.ds(pl.multiple_of(z * cols, cols), cols)
    far = pl.ds(pl.multiple_of((1 - z) * cols, cols), cols)
    wide = cols // n_chunk
    head = pl.ds(pl.multiple_of(z * cols, cols), wide)
    shared = (slice(wide, cols), slice(cols + wide, 2 * cols))
    group = GROUP
    for first in range(0, n_src, group):
        rows = slice(first * cap, (first + group) * cap)
        for i in range(first, first + group):
            put_rows(z, slice(i * cap, (i + 1) * cap), dos[i], do_ref)
        totals = [None, None]
        for k, (a_ref, b_ref, slope, gelu) in enumerate(((wa, wb, sv, gv), (wa2, wb2, sv2, gv2))):
            if k == 0:
                dhid = lax.dot_general(do_ref[rows, :], wc[0], NT, preferred_element_type=F32)
            else:
                dhid = lax.dot_general(do_ref[rows, near], wcz[0], NT, preferred_element_type=F32)
                dhid = dhid + lax.dot_general(do_ref[rows, far], wcn[0], NT, preferred_element_type=F32)
            grad_a = (dhid * slope[rows]).astype(BF16)
            grad_b = (dhid * gelu[rows]).astype(BF16)
            if k == 0:
                da_ref[0, rows, :] = grad_a
                db_ref[0, rows, :] = grad_b
            for c, picks in enumerate(((head,), shared)):
                parts = [lax.dot_general(grad_a, a_ref[0, p, :], NT, preferred_element_type=F32) + lax.dot_general(grad_b, b_ref[0, p, :], NT, preferred_element_type=F32) for p in picks]
                part = jnp.concatenate(parts, axis=1).astype(BF16).astype(F32)
                totals[c] = part if k == 0 else totals[c] + part
        for c in range(2):
            total = totals[c].astype(BF16)
            for i in range(group):
                outs[c * n_src + first + i][0] = total[i * cap:(i + 1) * cap]


def weight_grad_kernel(z_ref, *refs, n_src, widths):
    xs = refs[:n_src]
    dos, refs = group_refs(refs[n_src:], widths)
    h_ref, h2_ref, da_ref, da2_ref, db_ref, db2_ref, d0, d2, d4, d6, ga_ref, gb_ref, gc_ref, dw_ref, do_ref = refs
    dw_ref[...] = (d0[...] + d2[...]) + (d4[...] + d6[...])
    cap = xs[0].shape[1]
    for i, ref in enumerate(dos):
        put_rows(z_ref[0], slice(i * cap, (i + 1) * cap), ref, do_ref)
    x = jnp.concatenate([r[0] for r in xs], axis=0)
    grad_a = jnp.concatenate([da_ref[0], da2_ref[0]], axis=0)
    grad_b = jnp.concatenate([db_ref[0], db2_ref[0]], axis=0)
    ga_ref[0] = lax.dot_general(x, grad_a, TN, preferred_element_type=F32)
    gb_ref[0] = lax.dot_general(x, grad_b, TN, preferred_element_type=F32)
    gc_ref[0] = lax.dot_general(jnp.concatenate([h_ref[0], h2_ref[0]], axis=0), do_ref[...], TN, preferred_element_type=F32)


def slot_picks(cols_ref):
    lane = lax.broadcasted_iota(jnp.int32, (TOKEN_TILE, 128), 1).astype(F32)
    picks = []
    for k in range(2):
        slot = cols_ref[:, k:k + 1]
        blk = jnp.floor(slot * (1.0 / 128.0))
        hot = jnp.where(slot - 128.0 * blk == lane, 1.0, 0.0).astype(BF16)
        picks.append((jnp.broadcast_to(blk, (TOKEN_TILE, 128)).astype(BF16), hot))
    return picks


def add_rows(total, picks, srcs, peers):
    zero = jnp.zeros((TOKEN_TILE, 128), BF16)
    blocks = srcs[0].shape[0] // 128
    for d, src in zip(peers, srcs):
        pick = jnp.concatenate(
            [jnp.concatenate([jnp.where(blk == jnp.asarray(d * blocks + b, BF16), hot, zero) for b in range(blocks)], axis=1) for blk, hot in picks], axis=0)
        part = jnp.dot(pick, src[...], preferred_element_type=F32)
        total = part if total is None else total + part
    return total


def combine_first_kernel(z_ref, cols_ref, *refs, peers):
    both = add_rows(None, slot_picks(cols_ref), refs[:-2], peers)
    refs[-2][...] = both[:TOKEN_TILE]
    refs[-1][...] = both[TOKEN_TILE:]


def combine_out_kernel(z_ref, cols_ref, dy_ref, one_ref, two_ref, *refs, peers):
    y_ref, dg_ref, out_ref = refs[-3:]
    both = jnp.concatenate([one_ref[...], two_ref[...]], axis=0)
    both = add_rows(both, slot_picks(cols_ref), refs[:-3], peers)
    dy = dy_ref[...].astype(F32)
    one, two = both[:TOKEN_TILE], both[TOKEN_TILE:]
    out = (cols_ref[:, 2:3] * one + cols_ref[:, 3:4] * two).astype(BF16)
    y_ref[...] = out
    out_ref[...] = out
    dg_one = jnp.sum(dy * one, axis=1, keepdims=True)
    dg_two = jnp.sum(dy * two, axis=1, keepdims=True)
    wide = jnp.concatenate([dg_one, dg_two, jnp.zeros((TOKEN_TILE, 126), F32)], axis=1)
    dg_ref[...] = wide.T[:8, :]


def logit_grad_kernel(z_ref, rows_ref, prob_ref, one_ref, two_ref, x_ref, *refs):
    n_experts, n_tokens = prob_ref.shape
    dga_ref, dgb_ref, dl_ref, dw_ref = refs
    dgate = dga_ref[0:2, :] + dgb_ref[0:2, :]
    dg_one, dg_two = dgate[0:1], dgate[1:2]
    gate_one, gate_two = rows_ref[2:3, :], rows_ref[3:4, :]
    prob_one, prob_two = rows_ref[4:5, :], rows_ref[5:6, :]
    shared = dg_one * gate_one + dg_two * gate_two
    gate_sum = prob_one + prob_two
    dp_one = (dg_one - shared) / gate_sum
    dp_two = (dg_two - shared) / gate_sum
    centre = dp_one * prob_one + dp_two * prob_two
    expert = lax.broadcasted_iota(jnp.int32, (n_experts, n_tokens), 0)
    inner = jnp.where(one_ref[...] == expert, dp_one, 0.0) + jnp.where(two_ref[...] == expert, dp_two, 0.0) - centre
    high, mid, low = split3(prob_ref[...] * inner)
    dl_ref[...] = jnp.concatenate([high, high, mid, high, low, mid], axis=0)
    raw = jnp.dot(jnp.concatenate([high, mid, low], axis=0), x_ref[...], preferred_element_type=F32)
    dw_ref[...] = raw[:n_experts] + raw[n_experts:2 * n_experts] + raw[2 * n_experts:]


def combine_in_kernel(z_ref, cols_ref, dl_ref, *refs, n_src, last):
    n_w = 2 if last else 1
    wts, refs = refs[:n_w], refs[n_w:]
    srcs, refs = refs[:n_src], refs[n_src:]
    blocks = srcs[0].shape[0] // 128
    (blk_one, hot_one), (blk_two, hot_two) = slot_picks(cols_ref)
    zero = jnp.zeros((TOKEN_TILE, 128), BF16)
    acc = None
    for d in range(n_src):
        parts = []
        for b in range(blocks):
            this = jnp.asarray(d * blocks + b, BF16)
            parts.append(jnp.where(blk_one == this, hot_one, jnp.where(blk_two == this, hot_two, zero)))
        part = jnp.dot(jnp.concatenate(parts, axis=1), srcs[d][...], preferred_element_type=F32)
        acc = part if acc is None else acc + part
    high, mid, low = split3(jnp.concatenate([w[...] for w in wts], axis=1))
    weights = jnp.concatenate([high, mid, high, low, high, mid], axis=0)
    back = lax.dot_general(dl_ref[...], weights, TN, preferred_element_type=F32)
    res = (acc + back).astype(BF16)
    if not last:
        refs[0][...] = res
        return
    mine, other, near_ref, far_ref, dx_ref, dw_ref = refs
    wide = mine.shape[1]
    low_side = z_ref[0] == 0

    @pl.when(pl.program_id(0) == 0)
    def _():
        near, far = near_ref[...], far_ref[...]
        dw_ref[...] = jnp.concatenate([jnp.where(low_side, near, far), jnp.where(low_side, far, near)], axis=1)

    dx_ref[:, :wide] = jnp.where(low_side, mine[...], other[...])
    dx_ref[:, wide:2 * wide] = res[:, :wide]
    dx_ref[:, 2 * wide:3 * wide] = jnp.where(low_side, other[...], mine[...])
    dx_ref[:, 3 * wide:] = res[:, wide:]


def place_kernel(z_ref, kept_ref, piece_ref, own_core, pair_core, dw_ref, out_ref):
    out_ref[...] = piece_ref[...]
    dw_ref[...] = own_core[...] + pair_core[...]


def cost(flops, nbytes, trans=0):
    return pl.CostEstimate(flops=int(flops), bytes_accessed=int(nbytes), transcendentals=int(trans))


def solution(mesh):
    tp_size = mesh.shape["tp"]
    n_src = mesh.shape["ep"]
    n_chunk = 2
    all_vmem = pltpu.CompilerParams(vmem_limit_bytes=67043328)
    diag = [n_src - 2, n_src - 1]
    early = diag + [0, 1]
    late = [2, 4, 3, 5]
    src_order = early + late
    first_peer = 6
    out_early, out_late = [0, 1, 6], [4, 2, 7, 5, 3]

    def local_step(x_rows, w_router, first_ids, second_ids, w_gelu, w_lin, w_out, dy_rows):
        n_tokens, model = x_rows.shape
        n_experts = w_router.shape[1]
        own, width = w_gelu.shape[0], w_gelu.shape[2]
        slot_cap = 2 * n_tokens // n_experts
        block = own * slot_cap
        cols = model // tp_size
        wide = cols // n_chunk
        rows_all = n_src * slot_cap
        rows_early = len(early) * slot_cap
        rows_late = len(late) * slot_cap
        sds = jax.ShapeDtypeStruct
        me = lax.axis_index("ep").astype(jnp.int32).reshape(1)
        z = lax.axis_index("tp").astype(jnp.int32).reshape(1)
        swap = [(i, tp_size - 1 - i) for i in range(tp_size)]

        def across(val):
            return lax.ppermute(val, "tp", swap)

        def to_peer(val, d):
            if d == 0:
                return val
            return lax.ppermute(val, "ep", [(i, i ^ d) for i in range(n_src)])

        def call(kernel, grid, in_specs, out_specs, out_shape, estimate, args, scratch=()):
            return pl.pallas_call(
                kernel,
                grid_spec=pltpu.PrefetchScalarGridSpec(num_scalar_prefetch=1, grid=grid, in_specs=in_specs, out_specs=out_specs, scratch_shapes=list(scratch)),
                out_shape=out_shape, cost_estimate=estimate, compiler_params=all_vmem)(z, *args)

        wa2, wb2 = across(w_gelu), across(w_lin)
        wt = w_router.T
        id_one, id_two = first_ids.reshape(1, n_tokens), second_ids.reshape(1, n_tokens)
        in_vmem = pl.BlockSpec(memory_space=pltpu.VMEM)
        slots, first_x = pl.pallas_call(
            functools.partial(slots_kernel, slot_cap=slot_cap, own_experts=own, n_experts=n_experts, peer=first_peer),
            in_specs=[pl.BlockSpec(memory_space=pltpu.SMEM)] + [in_vmem] * 3,
            out_shape=(sds((8, n_tokens), F32), sds((block, model), BF16)),
            cost_estimate=cost(2 * block * n_tokens * model, 2 * n_tokens * model),
            compiler_params=all_vmem, name="k_slots",
        )(me, x_rows, id_one, id_two)
        rows, prob = pl.pallas_call(
            route_kernel,
            in_specs=[in_vmem] * 5,
            out_shape=(sds((16, n_tokens), F32), sds((n_experts, n_tokens), F32)),
            cost_estimate=cost(2 * 96 * n_tokens * model, 2 * n_tokens * model, n_experts * n_tokens),
            compiler_params=all_vmem, name="k_route",
        )(x_rows, wt, id_one, id_two, slots)
        token_cols = rows.T
        wcz = across(lax.dynamic_slice_in_dim(w_out, (1 - z[0]) * cols, cols, 2))
        wcn = across(lax.dynamic_slice_in_dim(w_out, z[0] * cols, cols, 2))

        per = block // GATHER_TILE

        def gather(src, peers, scaled, part=False):
            width_out = cols if part else model

            def out_map(g, z, i):
                return (jnp.clip(g - i * per, 0, per - 1), 0)

            def src_map(g, z):
                return (0, z[0] if part else 0)

            return call(
                functools.partial(gather_kernel, peers=peers, per=per, scaled=scaled), (len(peers) * per,),
                [pl.BlockSpec((16 if scaled else 8, n_tokens), lambda g, z: (0, 0)), pl.BlockSpec((n_tokens, width_out), src_map)],
                [pl.BlockSpec((GATHER_TILE, width_out), functools.partial(out_map, i=i)) for i in range(len(peers))],
                [sds((block, width_out), BF16)] * len(peers),
                cost(2 * len(peers) * block * n_tokens * width_out, 2 * (n_tokens + len(peers) * block) * width_out),
                (rows if scaled else slots, src))

        xs, dos = [None] * n_src, [None] * n_src
        xs[first_peer] = to_peer(first_x, first_peer).reshape(own, slot_cap, model)
        for peers in ([4, 2], [7, 1, 0], [5, 3]):
            for d, val in zip(peers, gather(x_rows, peers, False)):
                xs[d] = to_peer(val, d).reshape(own, slot_cap, model)
        for peers in (diag, [4, 2]):
            for d, val in zip(peers, gather(dy_rows, peers, True, part=True)):
                mine = to_peer(val, d)
                dos[d] = tuple(v.reshape(own, slot_cap, cols) for v in (mine, across(mine)))
        for peers in ([1, 0], [5, 3]):
            for d, val in zip(peers, gather(dy_rows, peers, True)):
                dos[d] = (to_peer(val, d).reshape(own, slot_cap, model),)
        xs = [xs[d] for d in src_order]

        def whole(a, b, at=0):
            return pl.BlockSpec((1, a, b), lambda e, *_: (e, at, 0))

        def forward_own(lo, hi):
            n_rows = (hi - lo) * slot_cap
            return call(
                functools.partial(forward_own_kernel, n_src=hi - lo, cols=cols), (own,),
                [whole(slot_cap, model)] * (hi - lo) + [whole(model, width)] * 2 + [whole(width, model)],
                [whole(n_rows, width)] * 3 + [whole(n_rows, cols)],
                [sds((own, n_rows, width), F32)] * 2 + [sds((own, n_rows, width), BF16), sds((own, n_rows, cols), BF16)],
                cost(2 * own * n_rows * width * (2 * model + cols), 8e3 * own * n_rows, own * n_rows * width),
                (*xs[lo:hi], w_gelu, w_lin, w_out))

        cuts = (0, n_src - 2, n_src)
        own_parts = [forward_own(cuts[i], cuts[i + 1]) for i in range(2)]
        part_rows = [(cuts[i + 1] - cuts[i]) * slot_cap for i in range(2)]
        fwd = pl.pallas_call(
            functools.partial(forward_other_kernel, n_src=n_src, n_chunk=1), grid=(own,),
            in_specs=[whole(slot_cap, model)] * n_src + [whole(r, cols) for r in part_rows] + [whole(model, width)] * 2 + [whole(width, cols)],
            out_specs=[whole(slot_cap, cols)] * n_src + [whole(rows_all, width)] * 2,
            out_shape=[sds((own, slot_cap, cols), BF16)] * n_src + [sds((own, rows_all, width), F32)] * 2,
            cost_estimate=cost(2 * own * rows_all * width * (2 * model + cols), 32e6, own * rows_all * width),
            compiler_params=all_vmem, name="k_fwd_other")(*xs, own_parts[0][3], own_parts[1][3], wa2, wb2, wcz)
        gv2, sv2 = fwd[n_src:]
        back_out = [None] * n_src
        for i, d in enumerate(src_order):
            back_out[d] = to_peer(fwd[i], d).reshape(block, cols)

        dx_widths = (wide, 2 * wide)

        def backward(peers, at):
            n_rows = len(peers) * slot_cap
            lo, hi = at * slot_cap, at * slot_cap + n_rows
            args = [v for d in peers for v in dos[d]]
            saved, specs, counts = [], [], []
            for source in ([p[0] for p in own_parts], [p[1] for p in own_parts], [gv2], [sv2]):
                base, n = 0, 0
                for arr in source:
                    rows_in = arr.shape[1]
                    a, b = max(lo, base), min(hi, base + rows_in)
                    if a < b:
                        step = b - a
                        saved.append(arr)
                        specs.append(whole(step, width, (a - base) // step))
                        n += 1
                    base += rows_in
                counts.append(n)
            return call(
                functools.partial(backward_kernel, widths=[len(dos[d]) for d in peers], saved_widths=counts, cols=cols, n_chunk=n_chunk), (own,),
                [whole(slot_cap, v.shape[2]) for v in args] + specs + [whole(model, width)] * 2 + [whole(width, model)] + [whole(model, width)] * 2 + [whole(width, cols)] * 2,
                [whole(slot_cap, w) for w in dx_widths for _ in peers] + [whole(n_rows, width)] * 2,
                [sds((own, slot_cap, w), BF16) for w in dx_widths for _ in peers] + [sds((own, n_rows, width), BF16)] * 2,
                cost(4 * own * n_rows * width * (model + 2 * cols), 6e3 * own * n_rows),
                (*args, *saved, w_gelu, w_lin, w_out, wa2, wb2, wcz, wcn),
                [pltpu.VMEM((n_rows, model), BF16)])

        bwd_a = backward(early, 0)
        bwd_b = backward(late, len(early))
        back_in = []
        for c in range(n_chunk):
            got = [None] * n_src
            for peers, vals in ((early, bwd_a), (late, bwd_b)):
                for i, d in enumerate(peers):
                    got[d] = to_peer(vals[c * len(peers) + i], d).reshape(block, dx_widths[c])
            back_in.append(got)

        def resident(a, b):
            return pl.BlockSpec((a, b), lambda i, *_: (0, 0))

        def tiles(b, col=None):
            return pl.BlockSpec((TOKEN_TILE, b), lambda i, z: (i, 0 if col is None else z[0] * n_chunk + col))

        n_tiles = (n_tokens // TOKEN_TILE,)
        any_spec = pl.BlockSpec(memory_space=pl.ANY)

        one, two = call(
            functools.partial(combine_first_kernel, peers=out_early), n_tiles,
            [tiles(16)] + [resident(block, cols)] * len(out_early), [tiles(cols)] * 2, [sds((n_tokens, cols), F32)] * 2,
            cost(4 * n_tokens * len(out_early) * block * cols, 12e6),
            (token_cols, *[back_out[d] for d in out_early]))
        y_mine, dg_mine, act_out = call(
            functools.partial(combine_out_kernel, peers=out_late), n_tiles,
            [tiles(16), pl.BlockSpec((TOKEN_TILE, cols), lambda i, z: (i, z[0]))] + [tiles(cols)] * 2 + [resident(block, cols)] * len(out_late),
            [tiles(cols), pl.BlockSpec((8, TOKEN_TILE), lambda i, z: (0, i)), pl.BlockSpec((TOKEN_TILE, cols), lambda i, z: (i, z[0]))],
            [sds((n_tokens, cols), BF16), sds((8, n_tokens), F32), sds((n_tokens, model), BF16)],
            cost(4 * n_tokens * len(out_late) * block * cols, 16e6),
            (token_cols, dy_rows, one, two, *[back_out[d] for d in out_late]))
        dg_other = across(dg_mine)
        y_other = across(y_mine)

        dl, dw = call(
            logit_grad_kernel, (1,),
            [resident(16, n_tokens), resident(n_experts, n_tokens), resident(1, n_tokens), resident(1, n_tokens), pl.BlockSpec((n_tokens, cols), lambda i, z: (0, z[0]))] + [resident(8, n_tokens)] * 2,
            [resident(6 * n_experts, n_tokens), resident(n_experts, cols)],
            [sds((6 * n_experts, n_tokens), BF16), sds((n_experts, cols), F32)],
            cost(2 * 96 * n_tokens * cols, 4e6),
            (rows, prob, id_one, id_two, x_rows, dg_mine, dg_other))

        all_dos = [v for d in src_order for v in dos[d]]
        grad_wa, grad_wb, grad_wc, dw_core = call(
            functools.partial(weight_grad_kernel, n_src=n_src, widths=[len(dos[d]) for d in src_order]), (own,),
            [whole(slot_cap, model)] * n_src + [whole(slot_cap, v.shape[2]) for v in all_dos] + [whole(r, width) for r in part_rows] + [whole(rows_early, width), whole(rows_late, width)] * 2 + [resident(n_experts, cols)] * 4,
            [whole(model, width), whole(model, width), whole(width, model), resident(n_experts, cols)],
            [sds((own, model, width), F32)] * 2 + [sds((own, width, model), F32), sds((n_experts, cols), F32)],
            cost(6 * own * rows_all * width * model, 40e6),
            (*xs, *all_dos, own_parts[0][2], own_parts[1][2], bwd_a[-2], bwd_b[-2], bwd_a[-1], bwd_b[-1], dw, to_peer(dw, 2), to_peer(dw, 4), to_peer(dw, 6)),
            [pltpu.VMEM((rows_all, model), BF16)])

        dw_near, act_out = pl.pallas_call(
            place_kernel,
            grid_spec=pltpu.PrefetchScalarGridSpec(
                num_scalar_prefetch=1, grid=n_tiles, in_specs=[pl.BlockSpec(memory_space=pl.ANY), tiles(cols)] + [resident(n_experts, cols)] * 2,
                out_specs=[resident(n_experts, cols), pl.BlockSpec((TOKEN_TILE, cols), lambda i, z: (i, 1 - z[0]))]),
            out_shape=[sds((n_experts, cols), F32), sds((n_tokens, model), BF16)], input_output_aliases={1: 1}, cost_estimate=cost(1e6, 4e6),
            compiler_params=all_vmem, name="k_place_y")(z, act_out, y_other, dw_core, to_peer(dw_core, 1))
        routers = (dw_near, across(dw_near))

        def combine_in(last, extra, srcs):
            quarters = [(lambda i, z: (0, 1)), (lambda i, z: (0, 3))] if last else [lambda i, z: (0, z[0] * n_chunk)]
            return call(
                functools.partial(combine_in_kernel, n_src=n_src, last=last), n_tiles,
                [tiles(16), pl.BlockSpec((6 * n_experts, TOKEN_TILE), lambda i, z: (0, i))] + [pl.BlockSpec((n_experts, wide), q) for q in quarters]
                + [resident(block, v.shape[1]) for v in srcs] + [tiles(wide)] * len(extra) + ([resident(n_experts, cols)] * len(routers) if last else []),
                [tiles(model), resident(n_experts, model)] if last else tiles(wide),
                [sds((n_tokens, model), BF16), sds((n_experts, model), F32)] if last else sds((n_tokens, wide), BF16),
                cost(2 * n_tokens * n_src * block * srcs[0].shape[1], 8e6),
                (token_cols, dl, *([wt] * len(quarters)), *srcs, *extra, *(routers if last else ())))

        dx_mine = combine_in(False, (), back_in[0])
        dx_other = across(dx_mine)
        grad_in, grad_router = combine_in(True, (dx_mine, dx_other), back_in[1])
        return act_out, grad_in, grad_wa, grad_wb, grad_wc, grad_router.T

    return jax.shard_map(local_step, mesh=mesh, in_specs=(P("ep", None), P(), P("ep"), P("ep"), P("ep", None, "tp"), P("ep", None, "tp"), P("ep", "tp", None), P("ep", None)), out_specs=(P("ep", None), P("ep", None), P("ep", None, "tp"), P("ep", None, "tp"), P("ep", "tp", None), P()), check_vma=False)
```

```python
import functools

import jax
import jax.numpy as jnp
from jax import lax
from jax.experimental import pallas as pl
from jax.experimental.pallas import tpu as pltpu
from jax.sharding import PartitionSpec as P


GELU_COEF = 0.7978845608028654
F32 = jnp.float32
BF16 = jnp.bfloat16
NT = (((1,), (1,)), ((), ()))
TN = (((0,), (0,)), ((), ()))
TILE = 256
GATHER_TILE = 256
GROUP = 2
TOKEN_TILE = 512
LANES = 128


def gelu_parts(pre_act):
    inner_arg = GELU_COEF * (pre_act + 0.044715 * pre_act * pre_act * pre_act)
    tanh_val = jnp.tanh(inner_arg)
    gelu_val = 0.5 * pre_act * (1.0 + tanh_val)
    gelu_slope = 0.5 * (1.0 + tanh_val) + 0.5 * pre_act * (1.0 - tanh_val * tanh_val) * GELU_COEF * (1.0 + 0.134145 * pre_act * pre_act)
    return gelu_val, gelu_slope


def split3(val):
    high = val.astype(BF16)
    rest = val - high.astype(F32)
    mid = rest.astype(BF16)
    return high, mid, (rest - mid.astype(F32)).astype(BF16)


def slots_kernel(me_ref, x_ref, one_ref, two_ref, slots_ref, first_ref, *, slot_cap, own_experts, n_experts, peer):
    n_tokens = x_ref.shape[0]
    expert = lax.broadcasted_iota(jnp.int32, (n_experts, n_tokens), 0)
    id_one, id_two = one_ref[...], two_ref[...]
    hot_one = jnp.where(id_one == expert, 1.0, 0.0)
    hot_two = jnp.where(id_two == expert, 1.0, 0.0)
    hots = jnp.concatenate([hot_one, hot_two], axis=0)
    before = lax.broadcasted_iota(jnp.int32, (TILE, TILE), 0) < lax.broadcasted_iota(jnp.int32, (TILE, TILE), 1)
    tri = jnp.where(before, 1.0, 0.0).astype(BF16)
    run = jnp.zeros((2 * n_experts, 1), F32)
    counts = []
    for b in range(n_tokens // TILE):
        part = hots[:, b * TILE:(b + 1) * TILE]
        counts.append(jnp.dot(part.astype(BF16), tri, preferred_element_type=F32) + run)
        run = run + jnp.sum(part, axis=1, keepdims=True)
    count = jnp.concatenate(counts, axis=1)
    pos_one = jnp.sum(count[:n_experts] * hot_one, axis=0, keepdims=True)
    pos_two = jnp.sum((count[n_experts:] + run[:n_experts]) * hot_two, axis=0, keepdims=True)
    turn = me_ref[0] * (own_experts * slot_cap)

    def slot_of(ids, pos):
        place = pos.astype(jnp.int32)
        slot = jnp.where(place < slot_cap, ids * slot_cap + place, n_experts * slot_cap)
        return jnp.bitwise_xor(slot, turn).astype(F32)

    slot_one, slot_two = slot_of(id_one, pos_one), slot_of(id_two, pos_two)
    slots_ref[...] = jnp.concatenate([slot_one, slot_two, jnp.zeros((6, n_tokens), F32)], axis=0)
    block = first_ref.shape[0]
    slot = (peer * block + lax.broadcasted_iota(jnp.int32, (block, n_tokens), 0)).astype(F32)
    hit = jnp.logical_or(slot_one == slot, slot_two == slot)
    first_ref[...] = jnp.dot(jnp.where(hit, 1.0, 0.0).astype(BF16), x_ref[...], preferred_element_type=F32).astype(BF16)


def route_kernel(x_ref, wt_ref, one_ref, two_ref, slots_ref, rows_ref, prob_ref):
    n_experts, n_tokens = prob_ref.shape
    pieces = jnp.concatenate(split3(wt_ref[...]), axis=0)
    raw = lax.dot_general(pieces, x_ref[...], NT, preferred_element_type=F32)
    logits = raw[:n_experts] + raw[n_experts:2 * n_experts] + raw[2 * n_experts:]
    expo = jnp.exp(logits - jnp.max(logits, axis=0, keepdims=True))
    prob = expo / jnp.sum(expo, axis=0, keepdims=True)
    prob_ref[...] = prob
    expert = lax.broadcasted_iota(jnp.int32, (n_experts, n_tokens), 0)
    prob_one = jnp.sum(jnp.where(one_ref[...] == expert, prob, 0.0), axis=0, keepdims=True)
    prob_two = jnp.sum(jnp.where(two_ref[...] == expert, prob, 0.0), axis=0, keepdims=True)
    gate_sum = prob_one + prob_two
    rows_ref[...] = jnp.concatenate(
        [slots_ref[0:2, :], prob_one / gate_sum, prob_two / gate_sum, prob_one, prob_two, jnp.zeros((10, n_tokens), F32)], axis=0)


def gather_kernel(z_ref, rows_ref, src_ref, *outs, peers, per, scaled):
    step = pl.program_id(0)
    n_tokens = src_ref.shape[0]
    peer = sum(jnp.where(step // per == i, d, 0) for i, d in enumerate(peers))
    slot = (peer * per + step % per) * GATHER_TILE + lax.broadcasted_iota(jnp.int32, (GATHER_TILE, n_tokens), 0)
    slot = slot.astype(F32)
    hit_one = rows_ref[0:1, :] == slot
    hit_two = rows_ref[1:2, :] == slot
    pick = jnp.where(jnp.logical_or(hit_one, hit_two), 1.0, 0.0).astype(BF16)
    val = jnp.dot(pick, src_ref[...], preferred_element_type=F32)
    if scaled:
        gate = jnp.where(hit_one, rows_ref[2:3, :], 0.0) + jnp.where(hit_two, rows_ref[3:4, :], 0.0)
        val = jnp.sum(gate, axis=1, keepdims=True) * val
    val = val.astype(BF16)
    for i, out in enumerate(outs):
        @pl.when(step // per == i)
        def _(out=out):
            out[...] = val


def forward_own_kernel(z_ref, *refs, n_src, cols):
    xs = refs[:n_src]
    wa, wb, wc, gv_ref, sv_ref, h_ref, part_ref = refs[n_src:]
    cap = xs[0].shape[1]
    col = pl.ds(pl.multiple_of(z_ref[0] * cols, cols), cols)
    group = GROUP
    for first in range(0, n_src, group):
        x = jnp.concatenate([r[0] for r in xs[first:first + group]], axis=0)
        rows = slice(first * cap, (first + group) * cap)
        pre_a = jnp.dot(x, wa[0], preferred_element_type=F32)
        pre_b = jnp.dot(x, wb[0], preferred_element_type=F32)
        gelu_val, gelu_slope = gelu_parts(pre_a)
        hidden = (gelu_val * pre_b).astype(BF16)
        gv_ref[0, rows, :] = gelu_val
        sv_ref[0, rows, :] = pre_b * gelu_slope
        h_ref[0, rows, :] = hidden
        part_ref[0, rows, :] = jnp.dot(hidden, wc[0, :, col], preferred_element_type=F32).astype(BF16)


def forward_other_kernel(*refs, n_src, n_chunk):
    xs = refs[:n_src]
    part_ref, part2_ref, wa, wb, wc = refs[n_src:n_src + 5]
    outs = refs[n_src + 5:n_src + 5 + n_chunk * n_src]
    gv_ref, sv_ref = refs[n_src + 5 + n_chunk * n_src:]
    parts = jnp.concatenate([part_ref[0], part2_ref[0]], axis=0)
    cap = xs[0].shape[1]
    wide = outs[0].shape[2]
    group = GROUP
    for first in range(0, n_src, GROUP):
        x = jnp.concatenate([r[0] for r in xs[first:first + GROUP]], axis=0)
        rows = slice(first * cap, (first + GROUP) * cap)
        pre_a = jnp.dot(x, wa[0], preferred_element_type=F32)
        pre_b = jnp.dot(x, wb[0], preferred_element_type=F32)
        gelu_val, gelu_slope = gelu_parts(pre_a)
        hidden = (gelu_val * pre_b).astype(BF16)
        gv_ref[0, rows, :] = gelu_val
        sv_ref[0, rows, :] = pre_b * gelu_slope
        part = jnp.dot(hidden, wc[0], preferred_element_type=F32).astype(BF16).astype(F32)
        total = (parts[rows].astype(F32) + part).astype(BF16)
        for c in range(n_chunk):
            for i in range(group):
                outs[c * n_src + first + i][0] = total[i * cap:(i + 1) * cap, c * wide:(c + 1) * wide]


def put_rows(z, rows, ref, dest):
    if len(ref) == 1:
        dest[rows, :] = ref[0][0]
        return
    cols = ref[0].shape[2]
    dest[rows, pl.ds(pl.multiple_of(z * cols, cols), cols)] = ref[0][0]
    dest[rows, pl.ds(pl.multiple_of((1 - z) * cols, cols), cols)] = ref[1][0]


def group_refs(refs, widths):
    groups, at = [], 0
    for w in widths:
        groups.append(refs[at:at + w])
        at += w
    return groups, refs[at:]


def backward_kernel(z_ref, *refs, widths, saved_widths, cols, n_chunk):
    dos, refs = group_refs(refs, widths)
    n_src = len(widths)
    saved, refs = group_refs(refs, saved_widths)
    wa, wb, wc, wa2, wb2, wcz, wcn = refs[:7]
    outs = refs[7:7 + n_chunk * n_src]
    da_ref, db_ref, do_ref = refs[7 + n_chunk * n_src:]
    gv, sv, gv2, sv2 = [jnp.concatenate([r[0] for r in group], axis=0) if len(group) > 1 else group[0][0] for group in saved]
    cap = dos[0][0].shape[1]
    z = z_ref[0]
    near = pl.ds(pl.multiple_of(z * cols, cols), cols)
    far = pl.ds(pl.multiple_of((1 - z) * cols, cols), cols)
    wide = cols // n_chunk
    head = pl.ds(pl.multiple_of(z * cols, cols), wide)
    shared = (slice(wide, cols), slice(cols + wide, 2 * cols))
    group = GROUP
    for first in range(0, n_src, group):
        rows = slice(first * cap, (first + group) * cap)
        for i in range(first, first + group):
            put_rows(z, slice(i * cap, (i + 1) * cap), dos[i], do_ref)
        totals = [None, None]
        for k, (a_ref, b_ref, slope, gelu) in enumerate(((wa, wb, sv, gv), (wa2, wb2, sv2, gv2))):
            if k == 0:
                dhid = lax.dot_general(do_ref[rows, :], wc[0], NT, preferred_element_type=F32)
            else:
                dhid = lax.dot_general(do_ref[rows, near], wcz[0], NT, preferred_element_type=F32)
                dhid = dhid + lax.dot_general(do_ref[rows, far], wcn[0], NT, preferred_element_type=F32)
            grad_a = (dhid * slope[rows]).astype(BF16)
            grad_b = (dhid * gelu[rows]).astype(BF16)
            if k == 0:
                da_ref[0, rows, :] = grad_a
                db_ref[0, rows, :] = grad_b
            for c, picks in enumerate(((head,), shared)):
                parts = [lax.dot_general(grad_a, a_ref[0, p, :], NT, preferred_element_type=F32) + lax.dot_general(grad_b, b_ref[0, p, :], NT, preferred_element_type=F32) for p in picks]
                part = jnp.concatenate(parts, axis=1).astype(BF16).astype(F32)
                totals[c] = part if k == 0 else totals[c] + part
        for c in range(2):
            total = totals[c].astype(BF16)
            for i in range(group):
                outs[c * n_src + first + i][0] = total[i * cap:(i + 1) * cap]


def weight_grad_kernel(z_ref, kept_ref, piece_ref, *refs, n_src, widths):
    xs = refs[:n_src]
    dos, refs = group_refs(refs[n_src:], widths)
    h_ref, h2_ref, da_ref, da2_ref, db_ref, db2_ref, d0, d2, d4, d6, ga_ref, gb_ref, gc_ref, dw_ref, out_ref, do_ref = refs
    out_ref[...] = piece_ref[...]
    dw_ref[...] = (d0[...] + d2[...]) + (d4[...] + d6[...])
    cap = xs[0].shape[1]
    for i, ref in enumerate(dos):
        put_rows(z_ref[0], slice(i * cap, (i + 1) * cap), ref, do_ref)
    x = jnp.concatenate([r[0] for r in xs], axis=0)
    grad_a = jnp.concatenate([da_ref[0], da2_ref[0]], axis=0)
    grad_b = jnp.concatenate([db_ref[0], db2_ref[0]], axis=0)
    ga_ref[0] = lax.dot_general(x, grad_a, TN, preferred_element_type=F32)
    gb_ref[0] = lax.dot_general(x, grad_b, TN, preferred_element_type=F32)
    gc_ref[0] = lax.dot_general(jnp.concatenate([h_ref[0], h2_ref[0]], axis=0), do_ref[...], TN, preferred_element_type=F32)


def slot_picks(cols_ref):
    lane = lax.broadcasted_iota(jnp.int32, (TOKEN_TILE, 128), 1).astype(F32)
    picks = []
    for k in range(2):
        slot = cols_ref[:, k:k + 1]
        blk = jnp.floor(slot * (1.0 / 128.0))
        hot = jnp.where(slot - 128.0 * blk == lane, 1.0, 0.0).astype(BF16)
        picks.append((jnp.broadcast_to(blk, (TOKEN_TILE, 128)).astype(BF16), hot))
    return picks


def add_rows(total, picks, srcs, peers):
    zero = jnp.zeros((TOKEN_TILE, 128), BF16)
    blocks = srcs[0].shape[0] // 128
    for d, src in zip(peers, srcs):
        pick = jnp.concatenate(
            [jnp.concatenate([jnp.where(blk == jnp.asarray(d * blocks + b, BF16), hot, zero) for b in range(blocks)], axis=1) for blk, hot in picks], axis=0)
        part = jnp.dot(pick, src[...], preferred_element_type=F32)
        total = part if total is None else total + part
    return total


def combine_first_kernel(z_ref, cols_ref, *refs, peers):
    both = add_rows(None, slot_picks(cols_ref), refs[:-2], peers)
    refs[-2][...] = both[:TOKEN_TILE]
    refs[-1][...] = both[TOKEN_TILE:]


def combine_out_kernel(z_ref, cols_ref, dy_ref, one_ref, two_ref, *refs, peers):
    y_ref, dg_ref, out_ref = refs[-3:]
    both = jnp.concatenate([one_ref[...], two_ref[...]], axis=0)
    both = add_rows(both, slot_picks(cols_ref), refs[:-3], peers)
    dy = dy_ref[...].astype(F32)
    one, two = both[:TOKEN_TILE], both[TOKEN_TILE:]
    out = (cols_ref[:, 2:3] * one + cols_ref[:, 3:4] * two).astype(BF16)
    y_ref[...] = out
    out_ref[...] = out
    dg_one = jnp.sum(dy * one, axis=1, keepdims=True)
    dg_two = jnp.sum(dy * two, axis=1, keepdims=True)
    wide = jnp.concatenate([dg_one, dg_two, jnp.zeros((TOKEN_TILE, 126), F32)], axis=1)
    dg_ref[...] = wide.T[:8, :]


def logit_grad_kernel(z_ref, rows_ref, prob_ref, one_ref, two_ref, x_ref, *refs):
    n_experts, n_tokens = prob_ref.shape
    dga_ref, dgb_ref, dl_ref, dw_ref = refs
    dgate = dga_ref[0:2, :] + dgb_ref[0:2, :]
    dg_one, dg_two = dgate[0:1], dgate[1:2]
    gate_one, gate_two = rows_ref[2:3, :], rows_ref[3:4, :]
    prob_one, prob_two = rows_ref[4:5, :], rows_ref[5:6, :]
    shared = dg_one * gate_one + dg_two * gate_two
    gate_sum = prob_one + prob_two
    dp_one = (dg_one - shared) / gate_sum
    dp_two = (dg_two - shared) / gate_sum
    centre = dp_one * prob_one + dp_two * prob_two
    expert = lax.broadcasted_iota(jnp.int32, (n_experts, n_tokens), 0)
    inner = jnp.where(one_ref[...] == expert, dp_one, 0.0) + jnp.where(two_ref[...] == expert, dp_two, 0.0) - centre
    high, mid, low = split3(prob_ref[...] * inner)
    dl_ref[...] = jnp.concatenate([high, high, mid, high, low, mid], axis=0)
    raw = jnp.dot(jnp.concatenate([high, mid, low], axis=0), x_ref[...], preferred_element_type=F32)
    dw_ref[...] = raw[:n_experts] + raw[n_experts:2 * n_experts] + raw[2 * n_experts:]


def add_token_rows(total, cols_ref, srcs, peers):
    (blk_one, hot_one), (blk_two, hot_two) = slot_picks(cols_ref)
    zero = jnp.zeros((TOKEN_TILE, LANES), BF16)
    blocks = srcs[0].shape[0] // LANES
    for d, src in zip(peers, srcs):
        parts = []
        for b in range(blocks):
            this = jnp.asarray(d * blocks + b, BF16)
            parts.append(jnp.where(blk_one == this, hot_one, jnp.where(blk_two == this, hot_two, zero)))
        total = total + jnp.dot(jnp.concatenate(parts, axis=1), src[...], preferred_element_type=F32)
    return total


def combine_in_kernel(z_ref, cols_ref, dl_ref, *refs, peers):
    srcs, wts, out_ref = refs[:len(peers)], refs[len(peers):-1], refs[-1]
    high, mid, low = split3(jnp.concatenate([w[...] for w in wts], axis=1))
    weights = jnp.concatenate([high, mid, high, low, high, mid], axis=0)
    back = lax.dot_general(dl_ref[...], weights, TN, preferred_element_type=F32)
    out_ref[...] = add_token_rows(back, cols_ref, srcs, peers).astype(out_ref.dtype)


def combine_last_kernel(z_ref, cols_ref, acc_ref, *refs, peers):
    srcs = refs[:len(peers)]
    mine, other, own_core, pair_core, own_far, pair_far, dx_ref, dw_ref = refs[len(peers):]
    res = add_token_rows(acc_ref[...], cols_ref, srcs, peers).astype(BF16)
    low_side = z_ref[0] == 0

    @pl.when(pl.program_id(0) == 0)
    def _():
        near, far = own_core[...] + pair_core[...], own_far[...] + pair_far[...]
        dw_ref[...] = jnp.concatenate([jnp.where(low_side, near, far), jnp.where(low_side, far, near)], axis=1)

    wide = mine.shape[1]
    first, third = jnp.where(low_side, mine[...], other[...]), jnp.where(low_side, other[...], mine[...])
    dx_ref[...] = jnp.concatenate([first, res[:, :wide], third, res[:, wide:]], axis=1)


def cost(flops, nbytes, trans=0):
    return pl.CostEstimate(flops=int(flops), bytes_accessed=int(nbytes), transcendentals=int(trans))


def peers_of(digits):
    return [int(c) for c in digits]


def solution(mesh):
    tp_size = mesh.shape["tp"]
    n_src = mesh.shape["ep"]
    n_chunk = 2
    all_vmem = pltpu.CompilerParams(vmem_limit_bytes=67043328)
    early, late = peers_of("6701"), peers_of("2435")
    src_order = early + late
    first_peer = 6
    out_early, out_late = peers_of("016"), peers_of("42753")
    in_early, in_late = peers_of("01624"), peers_of("357")

    def local_step(x_rows, w_router, first_ids, second_ids, w_gelu, w_lin, w_out, dy_rows):
        n_tokens, model = x_rows.shape
        n_experts = w_router.shape[1]
        own, width = w_gelu.shape[0], w_gelu.shape[2]
        slot_cap = 2 * n_tokens // n_experts
        block = own * slot_cap
        cols = model // tp_size
        wide = cols // n_chunk
        rows_all = n_src * slot_cap
        rows_early = len(early) * slot_cap
        rows_late = len(late) * slot_cap
        sds = jax.ShapeDtypeStruct
        me = lax.axis_index("ep").astype(jnp.int32).reshape(1)
        z = lax.axis_index("tp").astype(jnp.int32).reshape(1)
        swap = [(i, tp_size - 1 - i) for i in range(tp_size)]

        def across(val):
            return lax.ppermute(val, "tp", swap)

        def to_peer(val, d):
            if d == 0:
                return val
            return lax.ppermute(val, "ep", [(i, i ^ d) for i in range(n_src)])

        def call(kernel, grid, in_specs, out_specs, out_shape, estimate, args, scratch=(), aliases={}):
            return pl.pallas_call(
                kernel,
                grid_spec=pltpu.PrefetchScalarGridSpec(num_scalar_prefetch=1, grid=grid, in_specs=in_specs, out_specs=out_specs, scratch_shapes=list(scratch)),
                out_shape=out_shape, cost_estimate=estimate, compiler_params=all_vmem, input_output_aliases=aliases)(z, *args)

        wa2, wb2 = across(w_gelu), across(w_lin)
        wt = w_router.T
        id_one, id_two = first_ids.reshape(1, n_tokens), second_ids.reshape(1, n_tokens)
        in_vmem = pl.BlockSpec(memory_space=pltpu.VMEM)
        slots, first_x = pl.pallas_call(
            functools.partial(slots_kernel, slot_cap=slot_cap, own_experts=own, n_experts=n_experts, peer=first_peer),
            in_specs=[pl.BlockSpec(memory_space=pltpu.SMEM)] + [in_vmem] * 3,
            out_shape=(sds((8, n_tokens), F32), sds((block, model), BF16)),
            cost_estimate=cost(2 * block * n_tokens * model, 2 * n_tokens * model),
            compiler_params=all_vmem, name="k_slots",
        )(me, x_rows, id_one, id_two)
        rows, prob = pl.pallas_call(
            route_kernel,
            in_specs=[in_vmem] * 5,
            out_shape=(sds((16, n_tokens), F32), sds((n_experts, n_tokens), F32)),
            cost_estimate=cost(2 * 96 * n_tokens * model, 2 * n_tokens * model, n_experts * n_tokens),
            compiler_params=all_vmem, name="k_route",
        )(x_rows, wt, id_one, id_two, slots)
        token_cols = rows.T
        wcz = across(lax.dynamic_slice_in_dim(w_out, (1 - z[0]) * cols, cols, 2))
        wcn = across(lax.dynamic_slice_in_dim(w_out, z[0] * cols, cols, 2))

        per = block // GATHER_TILE

        def gather(src, peers, scaled, part=False):
            width_out = cols if part else model

            def out_map(g, z, i):
                return (jnp.clip(g - i * per, 0, per - 1), 0)

            def src_map(g, z):
                return (0, z[0] if part else 0)

            return call(
                functools.partial(gather_kernel, peers=peers, per=per, scaled=scaled), (len(peers) * per,),
                [pl.BlockSpec((16 if scaled else 8, n_tokens), lambda g, z: (0, 0)), pl.BlockSpec((n_tokens, width_out), src_map)],
                [pl.BlockSpec((GATHER_TILE, width_out), functools.partial(out_map, i=i)) for i in range(len(peers))],
                [sds((block, width_out), BF16)] * len(peers),
                cost(2 * len(peers) * block * n_tokens * width_out, 2 * (n_tokens + len(peers) * block) * width_out),
                (rows if scaled else slots, src))

        xs, dos = [None] * n_src, [None] * n_src
        xs[first_peer] = to_peer(first_x, first_peer).reshape(own, slot_cap, model)
        for peers in map(peers_of, ("42", "710", "53")):
            for d, val in zip(peers, gather(x_rows, peers, False)):
                xs[d] = to_peer(val, d).reshape(own, slot_cap, model)
        for peers in map(peers_of, ("67", "42")):
            for d, val in zip(peers, gather(dy_rows, peers, True, part=True)):
                mine = to_peer(val, d)
                dos[d] = tuple(v.reshape(own, slot_cap, cols) for v in (mine, across(mine)))
        for peers in map(peers_of, ("10", "53")):
            for d, val in zip(peers, gather(dy_rows, peers, True)):
                dos[d] = (to_peer(val, d).reshape(own, slot_cap, model),)
        xs = [xs[d] for d in src_order]

        def whole(a, b, at=0):
            return pl.BlockSpec((1, a, b), lambda e, *_: (e, at, 0))

        def forward_own(lo, hi):
            n_rows = (hi - lo) * slot_cap
            return call(
                functools.partial(forward_own_kernel, n_src=hi - lo, cols=cols), (own,),
                [whole(slot_cap, model)] * (hi - lo) + [whole(model, width)] * 2 + [whole(width, model)],
                [whole(n_rows, width)] * 3 + [whole(n_rows, cols)],
                [sds((own, n_rows, width), F32)] * 2 + [sds((own, n_rows, width), BF16), sds((own, n_rows, cols), BF16)],
                cost(2 * own * n_rows * width * (2 * model + cols), 8e3 * own * n_rows, own * n_rows * width),
                (*xs[lo:hi], w_gelu, w_lin, w_out))

        cuts = (0, n_src - 2, n_src)
        own_parts = [forward_own(cuts[i], cuts[i + 1]) for i in range(2)]
        part_rows = [(cuts[i + 1] - cuts[i]) * slot_cap for i in range(2)]
        fwd = pl.pallas_call(
            functools.partial(forward_other_kernel, n_src=n_src, n_chunk=1), grid=(own,),
            in_specs=[whole(slot_cap, model)] * n_src + [whole(r, cols) for r in part_rows] + [whole(model, width)] * 2 + [whole(width, cols)],
            out_specs=[whole(slot_cap, cols)] * n_src + [whole(rows_all, width)] * 2,
            out_shape=[sds((own, slot_cap, cols), BF16)] * n_src + [sds((own, rows_all, width), F32)] * 2,
            cost_estimate=cost(2 * own * rows_all * width * (2 * model + cols), 32e6, own * rows_all * width),
            compiler_params=all_vmem, name="k_fwd_other")(*xs, own_parts[0][3], own_parts[1][3], wa2, wb2, wcz)
        gv2, sv2 = fwd[n_src:]
        back_out = [None] * n_src
        for i, d in enumerate(src_order):
            back_out[d] = to_peer(fwd[i], d).reshape(block, cols)

        dx_widths = (wide, 2 * wide)

        def backward(peers, at):
            n_rows = len(peers) * slot_cap
            lo, hi = at * slot_cap, at * slot_cap + n_rows
            args = [v for d in peers for v in dos[d]]
            saved, specs, counts = [], [], []
            for source in ([p[0] for p in own_parts], [p[1] for p in own_parts], [gv2], [sv2]):
                base, n = 0, 0
                for arr in source:
                    rows_in = arr.shape[1]
                    a, b = max(lo, base), min(hi, base + rows_in)
                    if a < b:
                        step = b - a
                        saved.append(arr)
                        specs.append(whole(step, width, (a - base) // step))
                        n += 1
                    base += rows_in
                counts.append(n)
            return call(
                functools.partial(backward_kernel, widths=[len(dos[d]) for d in peers], saved_widths=counts, cols=cols, n_chunk=n_chunk), (own,),
                [whole(slot_cap, v.shape[2]) for v in args] + specs + [whole(model, width)] * 2 + [whole(width, model)] + [whole(model, width)] * 2 + [whole(width, cols)] * 2,
                [whole(slot_cap, w) for w in dx_widths for _ in peers] + [whole(n_rows, width)] * 2,
                [sds((own, slot_cap, w), BF16) for w in dx_widths for _ in peers] + [sds((own, n_rows, width), BF16)] * 2,
                cost(4 * own * n_rows * width * (model + 2 * cols), 6e3 * own * n_rows),
                (*args, *saved, w_gelu, w_lin, w_out, wa2, wb2, wcz, wcn),
                [pltpu.VMEM((n_rows, model), BF16)])

        bwd_a = backward(early, 0)
        bwd_b = backward(late, len(early))
        back_in = []
        for c in range(n_chunk):
            got = [None] * n_src
            for peers, vals in ((early, bwd_a), (late, bwd_b)):
                for i, d in enumerate(peers):
                    got[d] = to_peer(vals[c * len(peers) + i], d).reshape(block, dx_widths[c])
            back_in.append(got)

        def resident(a, b):
            return pl.BlockSpec((a, b), lambda i, *_: (0, 0))

        def tiles(b, col=None):
            return pl.BlockSpec((TOKEN_TILE, b), lambda i, z: (i, 0 if col is None else z[0] * n_chunk + col))

        n_tiles = (n_tokens // TOKEN_TILE,)
        one, two = call(
            functools.partial(combine_first_kernel, peers=out_early), n_tiles,
            [tiles(16)] + [resident(block, cols)] * len(out_early), [tiles(cols)] * 2, [sds((n_tokens, cols), F32)] * 2,
            cost(4 * n_tokens * len(out_early) * block * cols, 12e6),
            (token_cols, *[back_out[d] for d in out_early]))
        y_mine, dg_mine, act_out = call(
            functools.partial(combine_out_kernel, peers=out_late), n_tiles,
            [tiles(16), pl.BlockSpec((TOKEN_TILE, cols), lambda i, z: (i, z[0]))] + [tiles(cols)] * 2 + [resident(block, cols)] * len(out_late),
            [tiles(cols), pl.BlockSpec((8, TOKEN_TILE), lambda i, z: (0, i)), pl.BlockSpec((TOKEN_TILE, cols), lambda i, z: (i, z[0]))],
            [sds((n_tokens, cols), BF16), sds((8, n_tokens), F32), sds((n_tokens, model), BF16)],
            cost(4 * n_tokens * len(out_late) * block * cols, 16e6),
            (token_cols, dy_rows, one, two, *[back_out[d] for d in out_late]))
        dg_other = across(dg_mine)
        y_other = across(y_mine)

        dl, dw = call(
            logit_grad_kernel, (1,),
            [resident(16, n_tokens), resident(n_experts, n_tokens), resident(1, n_tokens), resident(1, n_tokens), pl.BlockSpec((n_tokens, cols), lambda i, z: (0, z[0]))] + [resident(8, n_tokens)] * 2,
            [resident(6 * n_experts, n_tokens), resident(n_experts, cols)],
            [sds((6 * n_experts, n_tokens), BF16), sds((n_experts, cols), F32)],
            cost(2 * 96 * n_tokens * cols, 4e6),
            (rows, prob, id_one, id_two, x_rows, dg_mine, dg_other))

        all_dos = [v for d in src_order for v in dos[d]]
        assert n_tokens // TOKEN_TILE == own
        grad_wa, grad_wb, grad_wc, dw_core, act_out = call(
            functools.partial(weight_grad_kernel, n_src=n_src, widths=[len(dos[d]) for d in src_order]), (own,),
            [pl.BlockSpec(memory_space=pl.ANY), tiles(cols)] + [whole(slot_cap, model)] * n_src + [whole(slot_cap, v.shape[2]) for v in all_dos] + [whole(r, width) for r in part_rows] + [whole(rows_early, width), whole(rows_late, width)] * 2 + [resident(n_experts, cols)] * 4,
            [whole(model, width), whole(model, width), whole(width, model), resident(n_experts, cols), pl.BlockSpec((TOKEN_TILE, cols), lambda e, z: (e, 1 - z[0]))],
            [sds((own, model, width), F32)] * 2 + [sds((own, width, model), F32), sds((n_experts, cols), F32), sds((n_tokens, model), BF16)],
            cost(6 * own * rows_all * width * model, 40e6),
            (act_out, y_other, *xs, *all_dos, own_parts[0][2], own_parts[1][2], bwd_a[-2], bwd_b[-2], bwd_a[-1], bwd_b[-1], dw, to_peer(dw, 2), to_peer(dw, 4), to_peer(dw, 6)),
            [pltpu.VMEM((rows_all, model), BF16)], {1: 4})
        far_pair = lax.ppermute(dw_core, ("tp", "ep"), [(i, i ^ (n_src + 1)) for i in range(tp_size * n_src)])
        routers = (dw_core, to_peer(dw_core, 1), across(dw_core), far_pair)

        def combine_in(peers, srcs, quarters, dtype):
            width_out = srcs[0].shape[1]
            return call(
                functools.partial(combine_in_kernel, peers=peers), n_tiles,
                [tiles(16), pl.BlockSpec((6 * n_experts, TOKEN_TILE), lambda i, z: (0, i))] + [resident(block, width_out)] * len(peers) + [pl.BlockSpec((n_experts, wide), q) for q in quarters],
                tiles(width_out), sds((n_tokens, width_out), dtype),
                cost(2 * n_tokens * len(peers) * block * width_out, 8e6),
                (token_cols, dl, *[srcs[d] for d in peers], *([wt] * len(quarters))))

        dx_mine = combine_in(tuple(range(n_src)), back_in[0], [lambda i, z: (0, z[0] * n_chunk)], BF16)
        dx_other = across(dx_mine)
        shared_part = combine_in(in_early, back_in[1], [lambda i, z: (0, 1), lambda i, z: (0, 3)], F32)
        grad_in, grad_router = call(
            functools.partial(combine_last_kernel, peers=in_late), n_tiles,
            [tiles(16), tiles(2 * wide)] + [resident(block, 2 * wide)] * len(in_late) + [tiles(wide)] * 2 + [resident(n_experts, cols)] * len(routers),
            [tiles(model), resident(n_experts, model)], [sds((n_tokens, model), BF16), sds((n_experts, model), F32)],
            cost(2 * n_tokens * len(in_late) * block * 2 * wide, 12e6),
            (token_cols, shared_part, *[back_in[1][d] for d in in_late], dx_mine, dx_other, *routers))
        return act_out, grad_in, grad_wa, grad_wb, grad_wc, grad_router.T

    return jax.shard_map(local_step, mesh=mesh, in_specs=(P("ep", None), P(), P("ep"), P("ep"), P("ep", None, "tp"), P("ep", None, "tp"), P("ep", "tp", None), P("ep", None)), out_specs=(P("ep", None), P("ep", None), P("ep", None, "tp"), P("ep", None, "tp"), P("ep", "tp", None), P()), check_vma=False)
```

```python
import functools

import jax
import jax.numpy as jnp
from jax import lax
from jax.experimental import pallas as pl
from jax.experimental.pallas import tpu as pltpu
from jax.sharding import PartitionSpec as P


GELU_COEF = 0.7978845608028654
F32 = jnp.float32
BF16 = jnp.bfloat16
NT = (((1,), (1,)), ((), ()))
TN = (((0,), (0,)), ((), ()))
TILE = 256
GATHER_TILE = 256
GROUP = 4
TOKEN_TILE = 512
IN_TILE = 1024
LANES = 128


def gelu_parts(pre_act):
    inner_arg = GELU_COEF * (pre_act + 0.044715 * pre_act * pre_act * pre_act)
    tanh_val = jnp.tanh(inner_arg)
    gelu_val = 0.5 * pre_act * (1.0 + tanh_val)
    gelu_slope = 0.5 * (1.0 + tanh_val) + 0.5 * pre_act * (1.0 - tanh_val * tanh_val) * GELU_COEF * (1.0 + 0.134145 * pre_act * pre_act)
    return gelu_val, gelu_slope


def split3(val):
    high = val.astype(BF16)
    rest = val - high.astype(F32)
    mid = rest.astype(BF16)
    return high, mid, (rest - mid.astype(F32)).astype(BF16)


def slots_kernel(me_ref, x_ref, one_ref, two_ref, slots_ref, first_ref, *, slot_cap, own_experts, n_experts, peer):
    n_tokens = x_ref.shape[0]
    expert = lax.broadcasted_iota(jnp.int32, (n_experts, n_tokens), 0)
    id_one, id_two = one_ref[...], two_ref[...]
    hot_one = jnp.where(id_one == expert, 1.0, 0.0)
    hot_two = jnp.where(id_two == expert, 1.0, 0.0)
    hots = jnp.concatenate([hot_one, hot_two], axis=0)
    before = lax.broadcasted_iota(jnp.int32, (TILE, TILE), 0) < lax.broadcasted_iota(jnp.int32, (TILE, TILE), 1)
    tri = jnp.where(before, 1.0, 0.0).astype(BF16)
    run = jnp.zeros((2 * n_experts, 1), F32)
    counts = []
    for b in range(n_tokens // TILE):
        part = hots[:, b * TILE:(b + 1) * TILE]
        counts.append(jnp.dot(part.astype(BF16), tri, preferred_element_type=F32) + run)
        run = run + jnp.sum(part, axis=1, keepdims=True)
    count = jnp.concatenate(counts, axis=1)
    pos_one = jnp.sum(count[:n_experts] * hot_one, axis=0, keepdims=True)
    pos_two = jnp.sum((count[n_experts:] + run[:n_experts]) * hot_two, axis=0, keepdims=True)
    turn = me_ref[0] * (own_experts * slot_cap)

    def slot_of(ids, pos):
        place = pos.astype(jnp.int32)
        slot = jnp.where(place < slot_cap, ids * slot_cap + place, n_experts * slot_cap)
        return jnp.bitwise_xor(slot, turn).astype(F32)

    slot_one, slot_two = slot_of(id_one, pos_one), slot_of(id_two, pos_two)
    slots_ref[...] = jnp.concatenate([slot_one, slot_two, jnp.zeros((6, n_tokens), F32)], axis=0)
    block = first_ref.shape[0]
    slot = (peer * block + lax.broadcasted_iota(jnp.int32, (block, n_tokens), 0)).astype(F32)
    hit = jnp.logical_or(slot_one == slot, slot_two == slot)
    first_ref[...] = jnp.dot(jnp.where(hit, 1.0, 0.0).astype(BF16), x_ref[...], preferred_element_type=F32).astype(BF16)


def route_kernel(x_ref, wt_ref, one_ref, two_ref, slots_ref, rows_ref, prob_ref):
    n_experts, n_tokens = prob_ref.shape
    pieces = jnp.concatenate(split3(wt_ref[...]), axis=0)
    raw = lax.dot_general(pieces, x_ref[...], NT, preferred_element_type=F32)
    logits = raw[:n_experts] + raw[n_experts:2 * n_experts] + raw[2 * n_experts:]
    expo = jnp.exp(logits - jnp.max(logits, axis=0, keepdims=True))
    prob = expo / jnp.sum(expo, axis=0, keepdims=True)
    prob_ref[...] = prob
    expert = lax.broadcasted_iota(jnp.int32, (n_experts, n_tokens), 0)
    prob_one = jnp.sum(jnp.where(one_ref[...] == expert, prob, 0.0), axis=0, keepdims=True)
    prob_two = jnp.sum(jnp.where(two_ref[...] == expert, prob, 0.0), axis=0, keepdims=True)
    gate_sum = prob_one + prob_two
    rows_ref[...] = jnp.concatenate(
        [slots_ref[0:2, :], prob_one / gate_sum, prob_two / gate_sum, prob_one, prob_two, jnp.zeros((10, n_tokens), F32)], axis=0)


def gather_kernel(z_ref, rows_ref, src_ref, *outs, peers, per, scaled):
    step = pl.program_id(0)
    n_tokens = src_ref.shape[0]
    peer = sum(jnp.where(step // per == i, d, 0) for i, d in enumerate(peers))
    slot = (peer * per + step % per) * GATHER_TILE + lax.broadcasted_iota(jnp.int32, (GATHER_TILE, n_tokens), 0)
    slot = slot.astype(F32)
    hit_one = rows_ref[0:1, :] == slot
    hit_two = rows_ref[1:2, :] == slot
    pick = jnp.where(jnp.logical_or(hit_one, hit_two), 1.0, 0.0).astype(BF16)
    val = jnp.dot(pick, src_ref[...], preferred_element_type=F32)
    if scaled:
        gate = jnp.where(hit_one, rows_ref[2:3, :], 0.0) + jnp.where(hit_two, rows_ref[3:4, :], 0.0)
        val = jnp.sum(gate, axis=1, keepdims=True) * val
    val = val.astype(BF16)
    for i, out in enumerate(outs):
        @pl.when(step // per == i)
        def _(out=out):
            out[...] = val


def forward_own_kernel(z_ref, *refs, n_src, cols):
    xs = refs[:n_src]
    wa, wb, wc, gv_ref, sv_ref, h_ref, part_ref = refs[n_src:]
    cap = xs[0].shape[1]
    col = pl.ds(pl.multiple_of(z_ref[0] * cols, cols), cols)
    group = GROUP
    for first in range(0, n_src, group):
        x = jnp.concatenate([r[0] for r in xs[first:first + group]], axis=0)
        rows = slice(first * cap, (first + group) * cap)
        pre_a = jnp.dot(x, wa[0], preferred_element_type=F32)
        pre_b = jnp.dot(x, wb[0], preferred_element_type=F32)
        gelu_val, gelu_slope = gelu_parts(pre_a)
        hidden = (gelu_val * pre_b).astype(BF16)
        gv_ref[0, rows, :] = gelu_val
        sv_ref[0, rows, :] = pre_b * gelu_slope
        h_ref[0, rows, :] = hidden
        part_ref[0, rows, :] = jnp.dot(hidden, wc[0, :, col], preferred_element_type=F32).astype(BF16)


def forward_other_kernel(*refs, n_src, n_chunk):
    xs = refs[:n_src]
    part_ref, part2_ref, wa, wb, wc = refs[n_src:n_src + 5]
    outs = refs[n_src + 5:n_src + 5 + n_chunk * n_src]
    gv_ref, sv_ref = refs[n_src + 5 + n_chunk * n_src:]
    parts = jnp.concatenate([part_ref[0], part2_ref[0]], axis=0)
    cap = xs[0].shape[1]
    wide = outs[0].shape[2]
    group = GROUP
    for first in range(0, n_src, GROUP):
        x = jnp.concatenate([r[0] for r in xs[first:first + GROUP]], axis=0)
        rows = slice(first * cap, (first + GROUP) * cap)
        pre_a = jnp.dot(x, wa[0], preferred_element_type=F32)
        pre_b = jnp.dot(x, wb[0], preferred_element_type=F32)
        gelu_val, gelu_slope = gelu_parts(pre_a)
        hidden = (gelu_val * pre_b).astype(BF16)
        gv_ref[0, rows, :] = gelu_val
        sv_ref[0, rows, :] = pre_b * gelu_slope
        part = jnp.dot(hidden, wc[0], preferred_element_type=F32).astype(BF16).astype(F32)
        total = (parts[rows].astype(F32) + part).astype(BF16)
        for c in range(n_chunk):
            for i in range(group):
                outs[c * n_src + first + i][0] = total[i * cap:(i + 1) * cap, c * wide:(c + 1) * wide]


def put_rows(z, rows, ref, dest):
    if len(ref) == 1:
        dest[rows, :] = ref[0][0]
        return
    cols = ref[0].shape[2]
    dest[rows, pl.ds(pl.multiple_of(z * cols, cols), cols)] = ref[0][0]
    dest[rows, pl.ds(pl.multiple_of((1 - z) * cols, cols), cols)] = ref[1][0]


def group_refs(refs, widths):
    groups, at = [], 0
    for w in widths:
        groups.append(refs[at:at + w])
        at += w
    return groups, refs[at:]


def backward_kernel(z_ref, *refs, widths, saved_widths, cols, n_chunk):
    dos, refs = group_refs(refs, widths)
    n_src = len(widths)
    saved, refs = group_refs(refs, saved_widths)
    wa, wb, wc, wa2, wb2, wcz, wcn = refs[:7]
    outs = refs[7:7 + n_chunk * n_src]
    da_ref, db_ref, do_ref = refs[7 + n_chunk * n_src:]
    gv, sv, gv2, sv2 = [jnp.concatenate([r[0] for r in group], axis=0) if len(group) > 1 else group[0][0] for group in saved]
    cap = dos[0][0].shape[1]
    z = z_ref[0]
    near = pl.ds(pl.multiple_of(z * cols, cols), cols)
    far = pl.ds(pl.multiple_of((1 - z) * cols, cols), cols)
    wide = cols // n_chunk
    head = pl.ds(pl.multiple_of(z * cols, cols), wide)
    shared = (slice(wide, cols), slice(cols + wide, 2 * cols))
    group = GROUP
    for first in range(0, n_src, group):
        rows = slice(first * cap, (first + group) * cap)
        for i in range(first, first + group):
            put_rows(z, slice(i * cap, (i + 1) * cap), dos[i], do_ref)
        totals = [None, None]
        for k, (a_ref, b_ref, slope, gelu) in enumerate(((wa, wb, sv, gv), (wa2, wb2, sv2, gv2))):
            if k == 0:
                dhid = lax.dot_general(do_ref[rows, :], wc[0], NT, preferred_element_type=F32)
            else:
                dhid = lax.dot_general(do_ref[rows, near], wcz[0], NT, preferred_element_type=F32)
                dhid = dhid + lax.dot_general(do_ref[rows, far], wcn[0], NT, preferred_element_type=F32)
            grad_a = (dhid * slope[rows]).astype(BF16)
            grad_b = (dhid * gelu[rows]).astype(BF16)
            if k == 0:
                da_ref[0, rows, :] = grad_a
                db_ref[0, rows, :] = grad_b
            for c, picks in enumerate(((head,), shared)):
                parts = [lax.dot_general(grad_a, a_ref[0, p, :], NT, preferred_element_type=F32) + lax.dot_general(grad_b, b_ref[0, p, :], NT, preferred_element_type=F32) for p in picks]
                part = jnp.concatenate(parts, axis=1).astype(BF16).astype(F32)
                totals[c] = part if k == 0 else totals[c] + part
        for c in range(2):
            total = totals[c].astype(BF16)
            for i in range(group):
                outs[c * n_src + first + i][0] = total[i * cap:(i + 1) * cap]


def weight_grad_kernel(z_ref, *refs, n_src, widths):
    xs = refs[:n_src]
    dos, refs = group_refs(refs[n_src:], widths)
    h_ref, h2_ref, da_ref, da2_ref, db_ref, db2_ref, d0, d2, d4, d6, ga_ref, gb_ref, gc_ref, dw_ref, do_ref = refs
    dw_ref[...] = (d0[...] + d2[...]) + (d4[...] + d6[...])
    cap = xs[0].shape[1]
    for i, ref in enumerate(dos):
        put_rows(z_ref[0], slice(i * cap, (i + 1) * cap), ref, do_ref)
    x = jnp.concatenate([r[0] for r in xs], axis=0)
    grad_a = jnp.concatenate([da_ref[0], da2_ref[0]], axis=0)
    grad_b = jnp.concatenate([db_ref[0], db2_ref[0]], axis=0)
    ga_ref[0] = lax.dot_general(x, grad_a, TN, preferred_element_type=F32)
    gb_ref[0] = lax.dot_general(x, grad_b, TN, preferred_element_type=F32)
    gc_ref[0] = lax.dot_general(jnp.concatenate([h_ref[0], h2_ref[0]], axis=0), do_ref[...], TN, preferred_element_type=F32)


def slot_picks(cols_ref):
    lane = lax.broadcasted_iota(jnp.int32, (cols_ref.shape[0], 128), 1).astype(F32)
    picks = []
    for k in range(2):
        slot = cols_ref[:, k:k + 1]
        blk = jnp.floor(slot * (1.0 / 128.0))
        hot = jnp.where(slot - 128.0 * blk == lane, 1.0, 0.0).astype(BF16)
        picks.append((jnp.broadcast_to(blk, (cols_ref.shape[0], 128)).astype(BF16), hot))
    return picks


def add_rows(total, picks, srcs, peers):
    zero = jnp.zeros((TOKEN_TILE, 128), BF16)
    blocks = srcs[0].shape[0] // 128
    for d, src in zip(peers, srcs):
        pick = jnp.concatenate(
            [jnp.concatenate([jnp.where(blk == jnp.asarray(d * blocks + b, BF16), hot, zero) for b in range(blocks)], axis=1) for blk, hot in picks], axis=0)
        part = jnp.dot(pick, src[...], preferred_element_type=F32)
        total = part if total is None else total + part
    return total


def combine_first_kernel(z_ref, cols_ref, *refs, peers):
    both = add_rows(None, slot_picks(cols_ref), refs[:-2], peers)
    refs[-2][...] = both[:TOKEN_TILE]
    refs[-1][...] = both[TOKEN_TILE:]


def combine_out_kernel(z_ref, cols_ref, dy_ref, one_ref, two_ref, *refs, peers):
    y_ref, dg_ref, out_ref = refs[-3:]
    both = jnp.concatenate([one_ref[...], two_ref[...]], axis=0)
    both = add_rows(both, slot_picks(cols_ref), refs[:-3], peers)
    dy = dy_ref[...].astype(F32)
    one, two = both[:TOKEN_TILE], both[TOKEN_TILE:]
    out = (cols_ref[:, 2:3] * one + cols_ref[:, 3:4] * two).astype(BF16)
    y_ref[...] = out
    out_ref[...] = out
    dg_one = jnp.sum(dy * one, axis=1, keepdims=True)
    dg_two = jnp.sum(dy * two, axis=1, keepdims=True)
    wide = jnp.concatenate([dg_one, dg_two, jnp.zeros((TOKEN_TILE, 126), F32)], axis=1)
    dg_ref[...] = wide.T[:8, :]


def logit_grad_kernel(z_ref, rows_ref, prob_ref, one_ref, two_ref, x_ref, *refs):
    n_experts, n_tokens = prob_ref.shape
    dga_ref, dgb_ref, dl_ref, dw_ref = refs
    dgate = dga_ref[0:2, :] + dgb_ref[0:2, :]
    dg_one, dg_two = dgate[0:1], dgate[1:2]
    gate_one, gate_two = rows_ref[2:3, :], rows_ref[3:4, :]
    prob_one, prob_two = rows_ref[4:5, :], rows_ref[5:6, :]
    shared = dg_one * gate_one + dg_two * gate_two
    gate_sum = prob_one + prob_two
    dp_one = (dg_one - shared) / gate_sum
    dp_two = (dg_two - shared) / gate_sum
    centre = dp_one * prob_one + dp_two * prob_two
    expert = lax.broadcasted_iota(jnp.int32, (n_experts, n_tokens), 0)
    inner = jnp.where(one_ref[...] == expert, dp_one, 0.0) + jnp.where(two_ref[...] == expert, dp_two, 0.0) - centre
    high, mid, low = split3(prob_ref[...] * inner)
    dl_ref[...] = jnp.concatenate([high, high, mid, high, low, mid], axis=0)
    raw = jnp.dot(jnp.concatenate([high, mid, low], axis=0), x_ref[...], preferred_element_type=F32)
    dw_ref[...] = raw[:n_experts] + raw[n_experts:2 * n_experts] + raw[2 * n_experts:]


def add_token_rows(total, cols_ref, srcs, peers):
    (blk_one, hot_one), (blk_two, hot_two) = slot_picks(cols_ref)
    zero = jnp.zeros_like(hot_one)
    blocks = srcs[0].shape[0] // LANES
    for d, src in zip(peers, srcs):
        parts = []
        for b in range(blocks):
            this = jnp.asarray(d * blocks + b, BF16)
            parts.append(jnp.where(blk_one == this, hot_one, jnp.where(blk_two == this, hot_two, zero)))
        total = total + jnp.dot(jnp.concatenate(parts, axis=1), src[...], preferred_element_type=F32)
    return total


def combine_in_kernel(z_ref, cols_ref, dl_ref, *refs, peers):
    srcs, wts, out_ref = refs[:len(peers)], refs[len(peers):-1], refs[-1]
    high, mid, low = split3(jnp.concatenate([w[...] for w in wts], axis=1))
    weights = jnp.concatenate([high, mid, high, low, high, mid], axis=0)
    back = lax.dot_general(dl_ref[...], weights, TN, preferred_element_type=F32)
    out_ref[...] = add_token_rows(back, cols_ref, srcs, peers).astype(out_ref.dtype)


def combine_place_kernel(z_ref, kept_ref, piece_ref, *refs, peers):
    refs[-1][...] = piece_ref[...]
    combine_in_kernel(z_ref, *refs[:-1], peers=peers)


def combine_last_kernel(z_ref, cols_ref, acc_ref, *refs, peers):
    srcs = refs[:len(peers)]
    mine, other, own_core, pair_core, own_far, pair_far, dx_ref, dw_ref = refs[len(peers):]
    res = add_token_rows(acc_ref[...], cols_ref, srcs, peers).astype(BF16)
    low_side = z_ref[0] == 0

    @pl.when(pl.program_id(0) == 0)
    def _():
        near, far = own_core[...] + pair_core[...], own_far[...] + pair_far[...]
        dw_ref[...] = jnp.concatenate([jnp.where(low_side, near, far), jnp.where(low_side, far, near)], axis=1)

    wide = mine.shape[1]
    first, third = jnp.where(low_side, mine[...], other[...]), jnp.where(low_side, other[...], mine[...])
    dx_ref[...] = jnp.concatenate([first, res[:, :wide], third, res[:, wide:]], axis=1)


def cost(flops, nbytes, trans=0):
    return pl.CostEstimate(flops=int(flops), bytes_accessed=int(nbytes), transcendentals=int(trans))


def peers_of(digits):
    return [int(c) for c in digits]


def solution(mesh):
    tp_size = mesh.shape["tp"]
    n_src = mesh.shape["ep"]
    n_chunk = 2
    all_vmem = pltpu.CompilerParams(vmem_limit_bytes=67043328)
    early, late = peers_of("6701"), peers_of("2435")
    src_order = early + late
    first_peer = 6
    out_early, out_late = peers_of("016"), peers_of("42753")
    in_early, in_late = peers_of("01624"), peers_of("357")

    def local_step(x_rows, w_router, first_ids, second_ids, w_gelu, w_lin, w_out, dy_rows):
        n_tokens, model = x_rows.shape
        n_experts = w_router.shape[1]
        own, width = w_gelu.shape[0], w_gelu.shape[2]
        slot_cap = 2 * n_tokens // n_experts
        block = own * slot_cap
        cols = model // tp_size
        wide = cols // n_chunk
        rows_all = n_src * slot_cap
        rows_early = len(early) * slot_cap
        rows_late = len(late) * slot_cap
        sds = jax.ShapeDtypeStruct
        me = lax.axis_index("ep").astype(jnp.int32).reshape(1)
        z = lax.axis_index("tp").astype(jnp.int32).reshape(1)
        swap = [(i, tp_size - 1 - i) for i in range(tp_size)]

        def across(val):
            return lax.ppermute(val, "tp", swap)

        def to_peer(val, d):
            if d == 0:
                return val
            return lax.ppermute(val, "ep", [(i, i ^ d) for i in range(n_src)])

        def call(kernel, grid, in_specs, out_specs, out_shape, estimate, args, scratch=(), aliases={}):
            return pl.pallas_call(
                kernel,
                grid_spec=pltpu.PrefetchScalarGridSpec(num_scalar_prefetch=1, grid=grid, in_specs=in_specs, out_specs=out_specs, scratch_shapes=list(scratch)),
                out_shape=out_shape, cost_estimate=estimate, compiler_params=all_vmem, input_output_aliases=aliases)(z, *args)

        wa2, wb2 = across(w_gelu), across(w_lin)
        wt = w_router.T
        id_one, id_two = first_ids.reshape(1, n_tokens), second_ids.reshape(1, n_tokens)
        in_vmem = pl.BlockSpec(memory_space=pltpu.VMEM)
        slots, first_x = pl.pallas_call(
            functools.partial(slots_kernel, slot_cap=slot_cap, own_experts=own, n_experts=n_experts, peer=first_peer),
            in_specs=[pl.BlockSpec(memory_space=pltpu.SMEM)] + [in_vmem] * 3,
            out_shape=(sds((8, n_tokens), F32), sds((block, model), BF16)),
            cost_estimate=cost(2 * block * n_tokens * model, 2 * n_tokens * model),
            compiler_params=all_vmem, name="k_slots",
        )(me, x_rows, id_one, id_two)
        rows, prob = pl.pallas_call(
            route_kernel,
            in_specs=[in_vmem] * 5,
            out_shape=(sds((16, n_tokens), F32), sds((n_experts, n_tokens), F32)),
            cost_estimate=cost(2 * 96 * n_tokens * model, 2 * n_tokens * model, n_experts * n_tokens),
            compiler_params=all_vmem, name="k_route",
        )(x_rows, wt, id_one, id_two, slots)
        token_cols = rows.T
        wcz = across(lax.dynamic_slice_in_dim(w_out, (1 - z[0]) * cols, cols, 2))
        wcn = across(lax.dynamic_slice_in_dim(w_out, z[0] * cols, cols, 2))

        per = block // GATHER_TILE

        def gather(src, peers, scaled, part=False):
            width_out = cols if part else model

            def out_map(g, z, i):
                return (jnp.clip(g - i * per, 0, per - 1), 0)

            def src_map(g, z):
                return (0, z[0] if part else 0)

            return call(
                functools.partial(gather_kernel, peers=peers, per=per, scaled=scaled), (len(peers) * per,),
                [pl.BlockSpec((16 if scaled else 8, n_tokens), lambda g, z: (0, 0)), pl.BlockSpec((n_tokens, width_out), src_map)],
                [pl.BlockSpec((GATHER_TILE, width_out), functools.partial(out_map, i=i)) for i in range(len(peers))],
                [sds((block, width_out), BF16)] * len(peers),
                cost(2 * len(peers) * block * n_tokens * width_out, 2 * (n_tokens + len(peers) * block) * width_out),
                (rows if scaled else slots, src))

        xs, dos = [None] * n_src, [None] * n_src
        xs[first_peer] = to_peer(first_x, first_peer).reshape(own, slot_cap, model)
        for peers in map(peers_of, ("42", "710", "53")):
            for d, val in zip(peers, gather(x_rows, peers, False)):
                xs[d] = to_peer(val, d).reshape(own, slot_cap, model)
        for peers in map(peers_of, ("67", "42")):
            for d, val in zip(peers, gather(dy_rows, peers, True, part=True)):
                mine = to_peer(val, d)
                dos[d] = tuple(v.reshape(own, slot_cap, cols) for v in (mine, across(mine)))
        for peers in map(peers_of, ("10", "53")):
            for d, val in zip(peers, gather(dy_rows, peers, True)):
                dos[d] = (to_peer(val, d).reshape(own, slot_cap, model),)
        xs = [xs[d] for d in src_order]

        def whole(a, b, at=0):
            return pl.BlockSpec((1, a, b), lambda e, *_: (e, at, 0))

        def forward_own(lo, hi):
            n_rows = (hi - lo) * slot_cap
            return call(
                functools.partial(forward_own_kernel, n_src=hi - lo, cols=cols), (own,),
                [whole(slot_cap, model)] * (hi - lo) + [whole(model, width)] * 2 + [whole(width, model)],
                [whole(n_rows, width)] * 3 + [whole(n_rows, cols)],
                [sds((own, n_rows, width), F32)] * 2 + [sds((own, n_rows, width), BF16), sds((own, n_rows, cols), BF16)],
                cost(2 * own * n_rows * width * (2 * model + cols), 8e3 * own * n_rows, own * n_rows * width),
                (*xs[lo:hi], w_gelu, w_lin, w_out))

        cuts = (0, n_src - 2, n_src)
        own_parts = [forward_own(cuts[i], cuts[i + 1]) for i in range(2)]
        part_rows = [(cuts[i + 1] - cuts[i]) * slot_cap for i in range(2)]
        fwd = pl.pallas_call(
            functools.partial(forward_other_kernel, n_src=n_src, n_chunk=1), grid=(own,),
            in_specs=[whole(slot_cap, model)] * n_src + [whole(r, cols) for r in part_rows] + [whole(model, width)] * 2 + [whole(width, cols)],
            out_specs=[whole(slot_cap, cols)] * n_src + [whole(rows_all, width)] * 2,
            out_shape=[sds((own, slot_cap, cols), BF16)] * n_src + [sds((own, rows_all, width), F32)] * 2,
            cost_estimate=cost(2 * own * rows_all * width * (2 * model + cols), 32e6, own * rows_all * width),
            compiler_params=all_vmem, name="k_fwd_other")(*xs, own_parts[0][3], own_parts[1][3], wa2, wb2, wcz)
        gv2, sv2 = fwd[n_src:]
        back_out = [None] * n_src
        for i, d in enumerate(src_order):
            back_out[d] = to_peer(fwd[i], d).reshape(block, cols)

        dx_widths = (wide, 2 * wide)

        def backward(peers, at):
            n_rows = len(peers) * slot_cap
            lo, hi = at * slot_cap, at * slot_cap + n_rows
            args = [v for d in peers for v in dos[d]]
            saved, specs, counts = [], [], []
            for source in ([p[0] for p in own_parts], [p[1] for p in own_parts], [gv2], [sv2]):
                base, n = 0, 0
                for arr in source:
                    rows_in = arr.shape[1]
                    a, b = max(lo, base), min(hi, base + rows_in)
                    if a < b:
                        step = b - a
                        saved.append(arr)
                        specs.append(whole(step, width, (a - base) // step))
                        n += 1
                    base += rows_in
                counts.append(n)
            return call(
                functools.partial(backward_kernel, widths=[len(dos[d]) for d in peers], saved_widths=counts, cols=cols, n_chunk=n_chunk), (own,),
                [whole(slot_cap, v.shape[2]) for v in args] + specs + [whole(model, width)] * 2 + [whole(width, model)] + [whole(model, width)] * 2 + [whole(width, cols)] * 2,
                [whole(slot_cap, w) for w in dx_widths for _ in peers] + [whole(n_rows, width)] * 2,
                [sds((own, slot_cap, w), BF16) for w in dx_widths for _ in peers] + [sds((own, n_rows, width), BF16)] * 2,
                cost(4 * own * n_rows * width * (model + 2 * cols), 6e3 * own * n_rows),
                (*args, *saved, w_gelu, w_lin, w_out, wa2, wb2, wcz, wcn),
                [pltpu.VMEM((n_rows, model), BF16)])

        bwd_a = backward(early, 0)
        bwd_b = backward(late, len(early))
        back_in = []
        for c in range(n_chunk):
            got = [None] * n_src
            for peers, vals in ((early, bwd_a), (late, bwd_b)):
                for i, d in enumerate(peers):
                    got[d] = to_peer(vals[c * len(peers) + i], d).reshape(block, dx_widths[c])
            back_in.append(got)

        def resident(a, b):
            return pl.BlockSpec((a, b), lambda i, *_: (0, 0))

        def tiles(b, col=None):
            return pl.BlockSpec((TOKEN_TILE, b), lambda i, z: (i, 0 if col is None else z[0] * n_chunk + col))

        n_tiles = (n_tokens // TOKEN_TILE,)
        one, two = call(
            functools.partial(combine_first_kernel, peers=out_early), n_tiles,
            [tiles(16)] + [resident(block, cols)] * len(out_early), [tiles(cols)] * 2, [sds((n_tokens, cols), F32)] * 2,
            cost(4 * n_tokens * len(out_early) * block * cols, 12e6),
            (token_cols, *[back_out[d] for d in out_early]))
        y_mine, dg_mine, act_out = call(
            functools.partial(combine_out_kernel, peers=out_late), n_tiles,
            [tiles(16), pl.BlockSpec((TOKEN_TILE, cols), lambda i, z: (i, z[0]))] + [tiles(cols)] * 2 + [resident(block, cols)] * len(out_late),
            [tiles(cols), pl.BlockSpec((8, TOKEN_TILE), lambda i, z: (0, i)), pl.BlockSpec((TOKEN_TILE, cols), lambda i, z: (i, z[0]))],
            [sds((n_tokens, cols), BF16), sds((8, n_tokens), F32), sds((n_tokens, model), BF16)],
            cost(4 * n_tokens * len(out_late) * block * cols, 16e6),
            (token_cols, dy_rows, one, two, *[back_out[d] for d in out_late]))
        dg_other = across(dg_mine)
        y_other = across(y_mine)

        dl, dw = call(
            logit_grad_kernel, (1,),
            [resident(16, n_tokens), resident(n_experts, n_tokens), resident(1, n_tokens), resident(1, n_tokens), pl.BlockSpec((n_tokens, cols), lambda i, z: (0, z[0]))] + [resident(8, n_tokens)] * 2,
            [resident(6 * n_experts, n_tokens), resident(n_experts, cols)],
            [sds((6 * n_experts, n_tokens), BF16), sds((n_experts, cols), F32)],
            cost(2 * 96 * n_tokens * cols, 4e6),
            (rows, prob, id_one, id_two, x_rows, dg_mine, dg_other))

        all_dos = [v for d in src_order for v in dos[d]]
        grad_wa, grad_wb, grad_wc, dw_core = call(
            functools.partial(weight_grad_kernel, n_src=n_src, widths=[len(dos[d]) for d in src_order]), (own,),
            [whole(slot_cap, model)] * n_src + [whole(slot_cap, v.shape[2]) for v in all_dos] + [whole(r, width) for r in part_rows] + [whole(rows_early, width), whole(rows_late, width)] * 2 + [resident(n_experts, cols)] * 4,
            [whole(model, width), whole(model, width), whole(width, model), resident(n_experts, cols)],
            [sds((own, model, width), F32)] * 2 + [sds((own, width, model), F32), sds((n_experts, cols), F32)],
            cost(6 * own * rows_all * width * model, 40e6),
            (*xs, *all_dos, own_parts[0][2], own_parts[1][2], bwd_a[-2], bwd_b[-2], bwd_a[-1], bwd_b[-1], dw, to_peer(dw, 2), to_peer(dw, 4), to_peer(dw, 6)),
            [pltpu.VMEM((rows_all, model), BF16)])
        far_pair = lax.ppermute(dw_core, ("tp", "ep"), [(i, i ^ (n_src + 1)) for i in range(tp_size * n_src)])
        routers = (dw_core, to_peer(dw_core, 1), across(dw_core), far_pair)

        def in_tiles(b):
            return pl.BlockSpec((IN_TILE, b), lambda i, z: (i, 0))

        def combine_in(peers, srcs, quarters, dtype, place=None):
            width_out = srcs[0].shape[1]
            in_specs = [in_tiles(16), pl.BlockSpec((6 * n_experts, IN_TILE), lambda i, z: (0, i))] + [resident(block, width_out)] * len(peers) + [pl.BlockSpec((n_experts, wide), q) for q in quarters]
            out_spec, out_shape = in_tiles(width_out), sds((n_tokens, width_out), dtype)
            estimate = cost(2 * n_tokens * len(peers) * block * width_out, 8e6)
            args = (token_cols, dl, *[srcs[d] for d in peers], *([wt] * len(quarters)))
            grid = (n_tokens // IN_TILE,)
            if place is None:
                return call(functools.partial(combine_in_kernel, peers=peers), grid, in_specs, out_spec, out_shape, estimate, args)
            kept, piece = place
            far_half = pl.BlockSpec((IN_TILE, cols), lambda i, z: (i, 1 - z[0]))
            return call(
                functools.partial(combine_place_kernel, peers=peers), grid, [pl.BlockSpec(memory_space=pl.ANY), in_tiles(cols)] + in_specs,
                [out_spec, far_half], [out_shape, sds(kept.shape, BF16)], estimate, (kept, piece, *args), aliases={1: 1})

        dx_mine = combine_in(tuple(range(n_src)), back_in[0], [lambda i, z: (0, z[0] * n_chunk)], BF16)
        dx_other = across(dx_mine)
        shared_part, act_out = combine_in(in_early, back_in[1], [lambda i, z: (0, 1), lambda i, z: (0, 3)], F32, (act_out, y_other))
        grad_in, grad_router = call(
            functools.partial(combine_last_kernel, peers=in_late), (n_tokens // IN_TILE,),
            [in_tiles(16), in_tiles(2 * wide)] + [resident(block, 2 * wide)] * len(in_late) + [in_tiles(wide)] * 2 + [resident(n_experts, cols)] * len(routers),
            [in_tiles(model), resident(n_experts, model)], [sds((n_tokens, model), BF16), sds((n_experts, model), F32)],
            cost(2 * n_tokens * len(in_late) * block * 2 * wide, 12e6),
            (token_cols, shared_part, *[back_in[1][d] for d in in_late], dx_mine, dx_other, *routers))
        return act_out, grad_in, grad_wa, grad_wb, grad_wc, grad_router.T

    return jax.shard_map(local_step, mesh=mesh, in_specs=(P("ep", None), P(), P("ep"), P("ep"), P("ep", None, "tp"), P("ep", None, "tp"), P("ep", "tp", None), P("ep", None)), out_specs=(P("ep", None), P("ep", None), P("ep", None, "tp"), P("ep", None, "tp"), P("ep", "tp", None), P()), check_vma=False)
```
